128 devices in a mesh: space: 64 (over x_lo, z, y, core), peer: 2 (over x_hi).
Axes of the slice: x: 4 (x_hi: 2, x_lo: 2; x = x_hi * 2 + x_lo), y: 4, z: 4, core: 2. Of those that a mesh axis runs over, the one named last changes fastest.
Arguments:
- wavefield: float32 [2, 9, 512, 64, 128], P('peer', None, 'space'), may hold values from -100 to 100
- buoyancy: float32 [512, 64, 128], P('space'), may hold values from 0.2 to 0.5
- lame_lambda: float32 [512, 64, 128], P('space'), may hold values from 0.06 to 0.12
- shear_modulus: float32 [512, 64, 128], P('space'), may hold values from 0.05 to 0.1
- scale_exponents: int32 [9, 64, 8, 16], P(None, 'space'), may hold values from -2 to 2
- source_cells: int32 [2, 8], replicated, may hold values from 0 to 4194303
- wavelet: float32 [2, 3, 8], replicated, may hold values from -18 to 18
Outputs:
- final_field: float32 [2, 9, 512, 64, 128], P('peer', None, 'space')
- stored: bfloat16 [2, 3, 9, 512, 64, 128], P('peer', None, None, 'space')
- statistics: float32 [2, 3, 2], P('peer')
The draws below stay inside these ranges and needn't reach their ends.
All inputs are finite; a program needn't handle non-finite values.
Results may differ from the reference program's by a relative error of at most 0.0045.
Values may be sent and summed in bfloat16 or wider, within the bound.
A program may use at most 64 MiB of HBM per device.

```python
import math
import jax
import jax.numpy as jnp
from jax import lax

NX = 128
NY = 64
BLOCK = 8
STEPS = 3
SRC = 8
SHOTS = 2
NZ = 512


def draw_wavefield(key, part):
    row_key, column_key, value_key = jax.random.split(key, 3)
    depth = jnp.arange(NZ, dtype=jnp.float32) / (NZ - 1)
    shape = (SHOTS, 9, NZ, NY, NX)
    ramp = 0.4 * jnp.exp(jnp.log(5.0) * depth)
    row_scale = jnp.exp(jax.random.uniform(row_key, (SHOTS, 1, 1, NY, 1), minval=jnp.log(0.32), maxval=jnp.log(3.2)))
    column_scale = jnp.exp(jax.random.uniform(column_key, (SHOTS, 1, 1, 1, NX), minval=jnp.log(0.32), maxval=jnp.log(3.2)))
    values = jax.random.truncated_normal(value_key, -4.0, 4.0, shape)
    return (values * ramp[None, None, :, None, None] * row_scale * column_scale).astype(jnp.float32)


def set_ends(drawn, stream_key, least, top_value):
    place = [jax.random.randint(jax.random.fold_in(stream_key, axis), (), 0, length) for axis, length in enumerate(drawn.shape)]
    longest = drawn.shape.index(max(drawn.shape))
    neighbour = place[:longest] + [(place[longest] + 1) % drawn.shape[longest]] + place[longest + 1:]
    return drawn.at[tuple(place)].set(least).at[tuple(neighbour)].set(top_value)


def block_scale(key, shape, shards, least, top_value):
    level = 1.0
    for dim, parts in shards:
        steps = jax.random.uniform(jax.random.fold_in(jax.random.fold_in(key, 6), dim), (parts,), jnp.float32, least / len(shards), top_value / len(shards))
        level = level * jnp.repeat(jnp.exp(steps), shape[dim] // parts).reshape((-1,) + (1,) * (len(shape) - 1 - dim))
    return level


def centred(rng, extent, spread, bound, kind=jnp.bfloat16):
    entries = spread * jax.random.normal(rng, extent, jnp.float32)
    return jnp.clip(entries, min=-bound, max=bound).astype(kind)


def setup_inputs(seed: int = 0) -> dict:
    key_list = jax.random.split(jax.random.key(seed), 8)
    wavefield = draw_wavefield(jax.random.fold_in(key_list[7], 71), 0)
    buoyancy = jnp.clip(jnp.exp(math.log(0.5) - 0.9162907 * jax.random.uniform(key_list[1], (NZ, NY, NX), jnp.float32) ** block_scale(key_list[1], (NZ, NY, NX), ((0, 64),), -0.2, 0.2)), 0.2, 0.5)
    lame_lambda = jnp.clip(jnp.exp(math.log(0.12) - 0.6931472 * jax.random.uniform(key_list[2], (NZ, NY, NX), jnp.float32) ** block_scale(key_list[2], (NZ, NY, NX), ((0, 64),), -0.2, 0.2)), 0.06, 0.12)
    shear_modulus = jnp.clip(jnp.exp(math.log(0.1) - 0.6931472 * jax.random.uniform(key_list[3], (NZ, NY, NX), jnp.float32) ** block_scale(key_list[3], (NZ, NY, NX), ((0, 64),), -0.2, 0.2)), 0.05, 0.1)
    scale_exponents = set_ends(jax.random.randint(key_list[4], (9, NZ // BLOCK, NY // BLOCK, NX // BLOCK), -2, 3), jax.random.fold_in(key_list[4], 1), -2, 2).astype(jnp.int32)
    source_cells = set_ends(jax.random.randint(key_list[5], (SHOTS, SRC), 0, NZ * NY * NX), jax.random.fold_in(key_list[5], 1), 0, (NZ * NY * NX) - 1).astype(jnp.int32)
    wavelet = centred(key_list[6], (SHOTS, STEPS, SRC), 3.0, 18.0, jnp.float32)
    return {"wavefield": wavefield, "buoyancy": buoyancy, "lame_lambda": lame_lambda, "shear_modulus": shear_modulus, "scale_exponents": scale_exponents, "source_cells": source_cells, "wavelet": wavelet}


stencil_reach = 2
stencil_weights = (9.0 / 8.0, -1.0 / 24.0)
clip_level = 4.0
energy_floor = 1e-06

def pad_along(values, dimension):
    widths = [(0, 0)] * values.ndim
    widths[dimension] = (stencil_reach, stencil_reach)
    return jnp.pad(values, widths)

def derivative(padded, dimension, forward):
    length = padded.shape[dimension] - 2 * stencil_reach
    summed = None
    for offset in range(1, stencil_reach + 1):
        weight = stencil_weights[offset - 1]
        if forward:
            above_at = stencil_reach + offset
            below_at = stencil_reach + 1 - offset
        else:
            above_at = stencil_reach + offset - 1
            below_at = stencil_reach - offset
        portion = weight * (lax.slice_in_dim(padded, above_at, above_at + length, axis=dimension) - lax.slice_in_dim(padded, below_at, below_at + length, axis=dimension))
        summed = portion if summed is None else summed + portion
    return summed

def differ(values, dimension, forward):
    return derivative(pad_along(values, dimension), dimension, forward)

def pad_depth(stack):
    return pad_along(stack, 2)

def advance(current, buoyancy, lame_lambda, shear_modulus, images, stress_padder, velocity_padder):
    velocity = [current[:, component] for component in range(3)]
    stress = [current[:, component] for component in range(3, 9)]
    depth_rims = stress_padder(current[:, 6:9])
    velocity[0] = velocity[0] + buoyancy * (differ(stress[0], 3, True) + differ(stress[2], 2, False) + derivative(depth_rims[:, 1], 1, False))
    velocity[1] = velocity[1] + buoyancy * (differ(stress[2], 3, False) + differ(stress[1], 2, True) + derivative(depth_rims[:, 2], 1, False))
    velocity[2] = velocity[2] + buoyancy * (differ(stress[4], 3, False) + differ(stress[5], 2, False) + derivative(depth_rims[:, 0], 1, True))
    depth_rims = velocity_padder(jnp.stack(velocity, axis=1))
    strain = [differ(velocity[0], 3, False), differ(velocity[1], 2, False), derivative(depth_rims[:, 2], 1, False)]
    dilation = strain[0] + strain[1] + strain[2]
    pressure = lame_lambda * dilation + images
    stress[0] = stress[0] + pressure + 2.0 * shear_modulus * strain[0]
    stress[1] = stress[1] + pressure + 2.0 * shear_modulus * strain[1]
    stress[3] = stress[3] + pressure + 2.0 * shear_modulus * strain[2]
    stress[2] = stress[2] + shear_modulus * (differ(velocity[0], 2, True) + differ(velocity[1], 3, True))
    stress[4] = stress[4] + shear_modulus * (derivative(depth_rims[:, 0], 1, True) + differ(velocity[2], 3, True))
    stress[5] = stress[5] + shear_modulus * (derivative(depth_rims[:, 1], 1, True) + differ(velocity[2], 2, True))
    return jnp.stack(velocity + stress, axis=1)

def scale_tables(exponents):
    expanded = jnp.repeat(jnp.repeat(jnp.repeat(exponents, BLOCK, axis=1), BLOCK, axis=2), BLOCK, axis=3)
    upscale = jnp.zeros(expanded.shape, jnp.float32)
    downscale = jnp.zeros(expanded.shape, jnp.float32)
    for exponent in range(-2, 3):
        chosen = expanded == exponent
        upscale = jnp.where(chosen, jnp.float32(2.0 ** exponent), upscale)
        downscale = jnp.where(chosen, jnp.float32(2.0 ** (-exponent)), downscale)
    return (upscale, downscale)

def compress(current, upscale, downscale):
    payload = jnp.clip(current * downscale, -clip_level, clip_level).astype(jnp.bfloat16)
    levels = lax.optimization_barrier(payload).astype(jnp.float32)
    return (payload, levels, levels * upscale)

def finish(sums, cell_count):
    mean_size = sums[..., 0] / cell_count
    relative = sums[..., 1] / cell_count / (sums[..., 2] / cell_count + energy_floor)
    return jnp.stack([mean_size, jnp.sqrt(relative)], axis=-1)

def place_sources(cell_index, amounts):
    flat = jnp.zeros((NZ * NY * NX,), jnp.float32).at[cell_index].add(amounts)
    return flat.reshape(NZ, NY, NX)

def reference(wavefield, buoyancy, lame_lambda, shear_modulus, scale_exponents, source_cells, wavelet):
    upscale, downscale = scale_tables(scale_exponents)
    cell_count = 9 * NZ * NY * NX
    current = wavefield
    stored_list = []
    sums_list = []
    for instant in range(STEPS):
        images = jnp.stack([place_sources(source_cells[shot_index], wavelet[shot_index, instant]) for shot_index in range(SHOTS)], axis=0)
        current = advance(current, buoyancy, lame_lambda, shear_modulus, images, pad_depth, pad_depth)
        payload, levels, restored = compress(current, upscale, downscale)
        stored_list.append(payload[::-1])
        misfit = current - restored
        sums_list.append(jnp.stack([lax.optimization_barrier(jnp.sum(jnp.abs(levels), axis=(1, 2, 3, 4))), lax.optimization_barrier(jnp.sum(misfit * misfit, axis=(1, 2, 3, 4))), lax.optimization_barrier(jnp.sum(current * current, axis=(1, 2, 3, 4)))], axis=-1))
    stored = jnp.stack(stored_list, axis=1)
    statistics = finish(jnp.stack(sums_list, axis=1), cell_count)
    return (current, stored, statistics)
```

```python
import functools

import jax
import jax.numpy as jnp
from jax import lax
from jax.experimental import pallas as pl
from jax.experimental.pallas import tpu as pltpu
from jax.sharding import PartitionSpec as P

MESH = pl.DeviceIdType.MESH
F32 = jnp.float32
BF16 = jnp.bfloat16

BLOCK = 8
STEPS = 3
SOURCES = 8
DEPTH, ROWS, COLS = 8, 64, 128
PAD = 8
YB = 16
OWN = 3
FAR = 6
BUO, MOD = 5, 3
LOW = 8
ROW_CUTS = (0, 32, 48, 64)
VX, VY, VZ, SXX, SYY, SXY, SZZ, SXZ, SYZ = range(9)
clip_level = 4.0
energy_floor = 1e-06


def lanes(shape):
    return lax.broadcasted_iota(jnp.int32, shape, 1)


class Slab:
    def __init__(self, ref, lead, buoyancy, lame, shear):
        self.ref, self.lead = ref, lead
        self.buoyancy, self.lame, self.shear = buoyancy, lame, shear
        self.lane = lanes((YB, COLS))

    def at(self, part, z, y, shift=0):
        if shift == 0:
            return self.ref[part, z + self.lead, pl.ds(y + PAD, YB), :]
        window = self.ref[part, z + self.lead, pl.ds(y, YB + 2 * PAD), :]
        return window[PAD + shift : PAD + shift + YB]

    def put(self, part, z, y, value, rows):
        lo, hi = rows
        if lo > y or hi < y + YB:
            row = lax.broadcasted_iota(jnp.int32, (YB, COLS), 0) + y
            value = jnp.where((row >= lo) & (row < hi), value, self.at(part, z, y))
        self.ref[part, z + self.lead, pl.ds(y + PAD, YB), :] = value

    def along_x(self, f, forward):
        after = jnp.where(self.lane < COLS - 1, pltpu.roll(f, COLS - 1, 1), 0.0)
        before = jnp.where(self.lane >= 1, pltpu.roll(f, 1, 1), 0.0)
        if forward:
            far = jnp.where(self.lane < COLS - 2, pltpu.roll(f, COLS - 2, 1), 0.0)
            return after - f, far - before
        far = jnp.where(self.lane >= 2, pltpu.roll(f, 2, 1), 0.0)
        return f - before, after - far

    def dx(self, part, z, y, forward):
        return self.along_x(self.at(part, z, y), forward)

    def dy(self, part, z, y, forward):
        window = self.ref[part, z + self.lead, pl.ds(y, YB + 2 * PAD), :]
        get = lambda shift: window[PAD + shift : PAD + shift + YB]
        if forward:
            return get(1) - get(0), get(2) - get(-1)
        return get(0) - get(-1), get(1) - get(-2)

    def dz(self, part, z, y, forward):
        get = lambda shift: self.at(part, z + shift, y)
        if forward:
            return get(1) - get(0), get(2) - get(-1)
        return get(0) - get(-1), get(1) - get(-2)

    def mat(self, table, lead, z, y, factor):
        return table[z + lead, pl.ds(y, YB), :] * factor

    def velocity(self, part, z, y, rows):
        if part == VX:
            terms = (self.dx(SXX, z, y, True), self.dy(SXY, z, y, False), self.dz(SXZ, z, y, False))
        elif part == VY:
            terms = (self.dx(SXY, z, y, False), self.dy(SYY, z, y, True), self.dz(SYZ, z, y, False))
        else:
            terms = (self.dx(SXZ, z, y, False), self.dy(SYZ, z, y, False), self.dz(SZZ, z, y, True))
        near = terms[0][0] + terms[1][0] + terms[2][0]
        far = terms[0][1] + terms[1][1] + terms[2][1]
        change = self.mat(self.buoyancy, BUO, z, y, 1.0 / 24.0) * (27.0 * near - far)
        self.put(part, z, y, self.at(part, z, y) + change, rows)

    def shears(self, part, z, y, rows):
        if part == SXY:
            terms = (self.dy(VX, z, y, True), self.dx(VY, z, y, True))
        elif part == SXZ:
            terms = (self.dz(VX, z, y, True), self.dx(VZ, z, y, True))
        else:
            terms = (self.dz(VY, z, y, True), self.dy(VZ, z, y, True))
        near = terms[0][0] + terms[1][0]
        far = terms[0][1] + terms[1][1]
        change = self.mat(self.shear, MOD, z, y, 1.0 / 24.0) * (27.0 * near - far)
        self.put(part, z, y, self.at(part, z, y) + change, rows)

    def normals(self, z, y, rows, image):
        strain = []
        for near, far in (
            self.dx(VX, z, y, False),
            self.dy(VY, z, y, False),
            self.dz(VZ, z, y, False),
        ):
            strain.append(27.0 * near - far)
        pressure = (
            self.mat(self.lame, MOD, z, y, 1.0 / 24.0) * (strain[0] + strain[1] + strain[2])
            + image(z, y)
        )
        double = self.mat(self.shear, MOD, z, y, 2.0 / 24.0)
        for part, value in zip((SXX, SYY, SZZ), strain):
            self.put(part, z, y, self.at(part, z, y) + (pressure + double * value), rows)


def layers(count, place, rows, body):
    first = rows[0] // YB * YB

    @pl.loop(0, count)
    def _(i):
        z = place(i)
        for y in range(first, rows[1], YB):
            body(z, y)


def run_velocity(slab, count, place, deep_place, rows):
    for part in (VX, VY):
        layers(count, place, rows, lambda z, y, part=part: slab.velocity(part, z, y, rows))
    layers(count, deep_place, rows, lambda z, y: slab.velocity(VZ, z, y, rows))


def run_stress(slab, deep, plain, rows, image):
    layers(*deep, rows, lambda z, y: slab.normals(z, y, rows, image))
    layers(*plain, rows, lambda z, y: slab.shears(SXY, z, y, rows))
    layers(*deep, rows, lambda z, y: slab.shears(SXZ, z, y, rows))
    layers(*deep, rows, lambda z, y: slab.shears(SYZ, z, y, rows))


def kernel(
    slabs,
    wave_hbm, buo_hbm, lame_hbm, shear_hbm, exps, cells, wavelet,
    final_hbm, stored_hbm, stats_out,
    own, other, mirror, low_a, low_b, high_a, high_b, buo, lame, shear, got, packed,
    up_rows, down_rows, exp_rows, sums, stat_src, stat_rx,
    in_sem, out_sem, halo_send, halo_recv, mat_send, mat_recv,
    x_send, x_recv, fwd_send, fwd_recv, stat_send, stat_recv,
):
    me, peer = lax.axis_index("space"), lax.axis_index("peer")
    has_down, has_up = me > 0, me < slabs - 1
    up, down = (me + 1, peer), (me - 1, peer)
    partner = (me, 1 - peer)
    groups = slabs // LOW
    block, lane_of = me // LOW, lax.rem(me, LOW)
    near_peers = [(block * LOW + lax.rem(lane_of + k, LOW), peer) for k in range(1, LOW)]
    wide_peers = [(lax.rem(block + k, groups) * LOW + lane_of, peer) for k in range(1, groups)]

    barrier = pltpu.get_barrier_semaphore()
    for device in [partner] + near_peers + wide_peers:
        pl.semaphore_signal(barrier, inc=1, device_id=device, device_id_type=MESH)

    @pl.when(has_up)
    def _():
        pl.semaphore_signal(barrier, inc=1, device_id=up, device_id_type=MESH)

    @pl.when(has_down)
    def _():
        pl.semaphore_signal(barrier, inc=1, device_id=down, device_id_type=MESH)

    def remote(source, target, send, recv, device):
        return pltpu.make_async_remote_copy(
            src_ref=source, dst_ref=target, send_sem=send, recv_sem=recv,
            device_id=device, device_id_type=MESH,
        )

    inner = pl.ds(PAD, ROWS)
    loads = [
        pltpu.make_async_copy(
            wave_hbm.at[0, part], own.at[part, pl.ds(OWN, DEPTH), inner, :], in_sem.at[part]
        )
        for part in range(9)
    ]
    tables = ((buo_hbm, buo, BUO), (lame_hbm, lame, MOD), (shear_hbm, shear, MOD))
    mat_loads = [
        pltpu.make_async_copy(source, target.at[pl.ds(lead, DEPTH)], in_sem.at[9 + k])
        for k, (source, target, lead) in enumerate(tables)
    ]
    for copy in loads + mat_loads:
        copy.start()

    zero = jnp.zeros((PAD, COLS), F32)
    plane = jnp.zeros((ROWS, COLS), F32)

    @pl.loop(0, 9)
    def _(part):
        for z in range(DEPTH + 2 * OWN):
            own[part, z, pl.ds(0, PAD), :] = zero
            own[part, z, pl.ds(PAD + ROWS, PAD), :] = zero
        for z in range(DEPTH + 2 * FAR):
            other[part, z, pl.ds(0, PAD), :] = zero
            other[part, z, pl.ds(PAD + ROWS, PAD), :] = zero
        for z in list(range(OWN)) + list(range(OWN + DEPTH, DEPTH + 2 * OWN)):
            own[part, z, inner, :] = plane

    def clear(base_mat, base_own):
        for _, target, lead in tables:
            for z in range(lead):
                target[z + (lead + DEPTH if base_mat else 0)] = plane

        @pl.loop(0, 9)
        def _(part):
            for z in range(FAR):
                got[part, z + base_own] = jnp.zeros((ROWS, COLS), BF16)

    @pl.when(jnp.logical_not(has_down))
    def _():
        clear(0, 0)

    @pl.when(jnp.logical_not(has_up))
    def _():
        clear(1, FAR + DEPTH)

    spread = (
        lax.broadcasted_iota(jnp.int32, (COLS // BLOCK, COLS), 0)
        == lanes((COLS // BLOCK, COLS)) // BLOCK
    ).astype(F32)
    exp_rows[...] = jnp.dot(
        exps[...].astype(F32), spread, preferred_element_type=F32, precision=lax.Precision.HIGHEST
    )

    @pl.loop(0, 9 * ROWS // BLOCK)
    def _(i):
        level = jnp.broadcast_to(exp_rows[pl.ds(i, 1), :], (BLOCK, COLS))
        upscale = jnp.ones((BLOCK, COLS), F32)
        downscale = upscale
        for exponent in (-2, -1, 1, 2):
            chosen = jnp.abs(level - exponent) < 0.5
            upscale = jnp.where(chosen, 2.0**exponent, upscale)
            downscale = jnp.where(chosen, 2.0**-exponent, downscale)
        up_rows[pl.ds(pl.multiple_of(i * BLOCK, BLOCK), BLOCK), :] = upscale
        down_rows[pl.ds(pl.multiple_of(i * BLOCK, BLOCK), BLOCK), :] = downscale

    sums[...] = jnp.zeros_like(sums)

    for copy in loads:
        copy.wait()

    @pl.loop(0, 9)
    def _(part):
        for z in (0, 1, 2, 5, 6, 7):
            mirror[0, part, z] = own[part, z + OWN, inner, :].astype(BF16)

    pl.semaphore_wait(
        barrier, 1 + len(near_peers) + len(wide_peers) + has_up.astype(jnp.int32) + has_down.astype(jnp.int32)
    )

    def halo_up(step):
        return [
            remote(mirror.at[step, pl.ds(0, 6), pl.ds(6, 2)], low_a.at[step],
                   halo_send.at[step, 0, 0], halo_recv.at[step, 0, 0], up),
            remote(mirror.at[step, pl.ds(6, 3), pl.ds(5, 3)], low_b.at[step],
                   halo_send.at[step, 0, 1], halo_recv.at[step, 0, 1], up),
        ]

    def halo_down(step):
        return [
            remote(mirror.at[step, pl.ds(0, 6), pl.ds(0, 2)], high_a.at[step],
                   halo_send.at[step, 1, 0], halo_recv.at[step, 1, 0], down),
            remote(mirror.at[step, pl.ds(6, 3), pl.ds(0, 3)], high_b.at[step],
                   halo_send.at[step, 1, 1], halo_recv.at[step, 1, 1], down),
        ]

    def mat_up():
        return [
            remote(target.at[pl.ds(DEPTH, lead)], target.at[pl.ds(0, lead)],
                   mat_send.at[k, 0], mat_recv.at[k, 0], up)
            for k, (_, target, lead) in enumerate(tables)
        ]

    def mat_down():
        return [
            remote(target.at[pl.ds(lead, lead)], target.at[pl.ds(lead + DEPTH, lead)],
                   mat_send.at[k, 1], mat_recv.at[k, 1], down)
            for k, (_, target, lead) in enumerate(tables)
        ]

    def send_halos(step):
        @pl.when(has_up)
        def _():
            for copy in halo_up(step):
                copy.start()

        @pl.when(has_down)
        def _():
            for copy in halo_down(step):
                copy.start()

    send_halos(0)
    for copy in mat_loads:
        copy.wait()

    @pl.when(has_up)
    def _():
        for copy in mat_up():
            copy.start()

    @pl.when(has_down)
    def _():
        for copy in mat_down():
            copy.start()

    row_parts = list(zip(ROW_CUTS[:-1], ROW_CUTS[1:]))

    def across(index):
        if index == 0:
            layer, count, lo, hi = 3, 2, 0, ROWS
        else:
            lo, hi = row_parts[(index - 1) // 2]
            layer, count = (0, 3) if index % 2 else (5, 3)
        return remote(
            mirror.at[1, :, pl.ds(layer, count), pl.ds(lo, hi - lo)],
            got.at[:, pl.ds(FAR + layer, count), pl.ds(lo, hi - lo)],
            x_send.at[index], x_recv.at[index], partner,
        )

    across_count = 1 + 2 * len(row_parts)

    def forward_up(index):
        if index == 0:
            return [remote(got.at[:, pl.ds(FAR + 3, 2)], got.at[:, pl.ds(1, 2)],
                           fwd_send.at[0, 0, 0], fwd_recv.at[0, 0, 0], up)]
        lo, hi = row_parts[index - 1]
        rows = pl.ds(lo, hi - lo)
        return [
            remote(got.at[:, pl.ds(FAR + 5, 3), rows], got.at[:, pl.ds(3, 3), rows],
                   fwd_send.at[index, 0, 0], fwd_recv.at[index, 0, 0], up),
            remote(got.at[pl.ds(6, 3), pl.ds(FAR + 2, 1), rows], got.at[pl.ds(6, 3), pl.ds(0, 1), rows],
                   fwd_send.at[index, 0, 1], fwd_recv.at[index, 0, 1], up),
        ]

    def forward_down(index):
        base = FAR + DEPTH
        if index == 0:
            return [remote(got.at[:, pl.ds(FAR + 3, 2)], got.at[:, pl.ds(base + 3, 2)],
                           fwd_send.at[0, 1, 0], fwd_recv.at[0, 1, 0], down)]
        lo, hi = row_parts[index - 1]
        rows = pl.ds(lo, hi - lo)
        return [
            remote(got.at[:, pl.ds(FAR, 3), rows], got.at[:, pl.ds(base, 3), rows],
                   fwd_send.at[index, 1, 0], fwd_recv.at[index, 1, 0], down),
            remote(got.at[pl.ds(6, 3), pl.ds(FAR + 5, 1), rows], got.at[pl.ds(6, 3), pl.ds(base + 5, 1), rows],
                   fwd_send.at[index, 1, 1], fwd_recv.at[index, 1, 1], down),
        ]

    def pass_on(index):
        if index == 0:
            across(0).wait_recv()
        else:
            across(2 * index - 1).wait_recv()
            across(2 * index).wait_recv()

        @pl.when(has_up)
        def _():
            for copy in forward_up(index):
                copy.start()

        @pl.when(has_down)
        def _():
            for copy in forward_down(index):
                copy.start()

    def image_of(shot, step):
        def image(z, y):
            cell = (
                ((me * DEPTH + z) * ROWS + y) * COLS
                + lax.broadcasted_iota(jnp.int32, (YB, COLS), 0) * COLS
                + lanes((YB, COLS))
            )
            total = jnp.zeros((YB, COLS), F32)
            for j in range(SOURCES):
                total = total + jnp.where(cell == cells[shot, j], wavelet[shot, step, j], 0.0)
            return total

        return image

    mine = Slab(own, OWN, buo, lame, shear)
    every = (0, ROWS)

    def record(step, count, place):
        def body(k, carry):
            part, z = k // count, place(lax.rem(k, count))
            sizes, misfits, squares = carry
            for y in range(0, ROWS, YB):
                value = mine.at(part, z, y)
                rounded = value.astype(BF16)
                mirror[step + 1, part, z, pl.ds(y, YB), :] = rounded
                at = pl.ds(pl.multiple_of(part * ROWS + y, YB), YB)
                level = jnp.clip(rounded.astype(F32) * down_rows[at, :], -clip_level, clip_level)
                misfit = value - level * up_rows[at, :]
                sizes = sizes + jnp.abs(level)
                misfits = misfits + misfit * misfit
                squares = squares + value * value
            return sizes, misfits, squares

        start = tuple(sums[step, k] for k in range(3))
        for k, total in enumerate(lax.fori_loop(0, 9 * count, body, start)):
            sums[step, k] = total

    edges = lambda first, gap: (lambda i: first + i + (i // 3) * gap)

    @pl.loop(0, STEPS)
    def _(step):
        @pl.when(step > 0)
        def _():
            send_halos(step)

        @pl.when(step == 2)
        def _():
            pass_on(0)

        image = image_of(peer, step)
        run_velocity(mine, 5, lambda i: i + 2, lambda i: i + 1, every)
        middle = (2, lambda i: i + 3)
        run_stress(mine, middle, middle, every, image)
        record(step, *middle)

        @pl.when(step == 0)
        def _():
            across(0).start()

        @pl.when(has_down)
        def _():
            for copy in halo_up(step):
                copy.wait_recv()

            @pl.when(step == 0)
            def _():
                for copy in mat_up():
                    copy.wait_recv()

            @pl.loop(0, 6)
            def _(part):
                for z in range(2):
                    own[part, OWN - 2 + z, inner, :] = low_a[step, part, z].astype(F32)

            @pl.loop(0, 3)
            def _(part):
                for z in range(3):
                    own[part + 6, OWN - 3 + z, inner, :] = low_b[step, part, z].astype(F32)

        @pl.when(has_up)
        def _():
            for copy in halo_down(step):
                copy.wait_recv()

            @pl.when(step == 0)
            def _():
                for copy in mat_down():
                    copy.wait_recv()

            @pl.loop(0, 6)
            def _(part):
                for z in range(2):
                    own[part, OWN + DEPTH + z, inner, :] = high_a[step, part, z].astype(F32)

            @pl.loop(0, 3)
            def _(part):
                for z in range(3):
                    own[part + 6, OWN + DEPTH + z, inner, :] = high_b[step, part, z].astype(F32)

        run_velocity(mine, 6, edges(-1, 5), edges(-2, 5), every)
        outer = (6, edges(0, 2))
        run_stress(mine, outer, outer, every, image)
        record(step, *outer)

        @pl.when(step == 0)
        def _():
            for index in range(1, across_count):
                across(index).start()

    store_final = pltpu.make_async_copy(
        own.at[:, pl.ds(OWN, DEPTH), inner, :], final_hbm.at[0], out_sem.at[0]
    )
    store_final.start()

    row8 = lax.broadcasted_iota(jnp.int32, (8, COLS), 0)
    lane8 = lanes((8, COLS))
    tile = jnp.zeros((8, COLS), F32)
    for step in range(STEPS):
        for k in range(3):
            tile = tile + jnp.where((row8 == step) & (lane8 == k), jnp.sum(sums[step, k]), 0.0)

    def gather(phase, peers, mine_at, size, tile):
        stat_src[phase] = tile
        copies = [
            remote(stat_src.at[phase], stat_rx.at[phase, mine_at],
                   stat_send.at[phase, k], stat_recv.at[phase, k], device)
            for k, device in enumerate(peers)
        ]
        for copy in copies:
            copy.start()
        stat_rx[phase, mine_at] = tile
        for copy in copies:
            copy.wait()
        total = stat_rx[phase, 0]
        for k in range(1, size):
            total = total + stat_rx[phase, k]
        return total

    tile = gather(0, near_peers, lane_of, LOW, tile)
    tile = gather(1, wide_peers, block, groups, tile)
    scaled = tile * (1.0 / (9 * slabs * DEPTH * ROWS * COLS))
    ratio = pltpu.roll(scaled, COLS - 1, 1) / (pltpu.roll(scaled, COLS - 2, 1) + energy_floor)
    table = jnp.where(lane8 == 0, scaled, pltpu.roll(jnp.sqrt(ratio), 1, 1))
    stats_out[...] = table[:STEPS, :2]

    theirs = Slab(other, FAR, buo, lame, shear)

    def widen(rows):
        lo, hi = rows

        @pl.loop(0, 9)
        def _(part):
            @pl.loop(1, DEPTH + 2 * FAR - 1)
            def _(z):
                other[part, z, pl.ds(PAD + lo, hi - lo), :] = got[part, z, pl.ds(lo, hi - lo), :].astype(F32)

        @pl.loop(6, 9)
        def _(part):
            for z in (0, DEPTH + 2 * FAR - 1):
                other[part, z, pl.ds(PAD + lo, hi - lo), :] = got[part, z, pl.ds(lo, hi - lo), :].astype(F32)

    def compress(step, rows):
        lo, hi = rows

        @pl.loop(0, 9)
        def _(part):
            @pl.loop(0, DEPTH)
            def _(z):
                for y in range(lo // YB * YB, hi, YB):
                    at = pl.ds(pl.multiple_of(part * ROWS + y, YB), YB)
                    level = jnp.clip(theirs.at(part, z, y) * down_rows[at, :], -clip_level, clip_level)
                    if lo > y or hi < y + YB:
                        row = lax.broadcasted_iota(jnp.int32, (YB, COLS), 0) + y
                        before = packed[step, part, z, pl.ds(y, YB), :].astype(F32)
                        level = jnp.where((row >= lo) & (row < hi), level, before)
                    packed[step, part, z, pl.ds(y, YB), :] = level.astype(BF16)

    stores = []

    def store_payload(step, index, rows):
        lo, hi = (bound // YB * YB for bound in rows)
        if lo < hi:
            stores.append(
                pltpu.make_async_copy(
                    packed.at[step, :, :, pl.ds(lo, hi - lo)],
                    stored_hbm.at[0, step, :, :, pl.ds(lo, hi - lo)],
                    out_sem.at[1 + step * len(row_parts) + index],
                )
            )
            stores[-1].start()

    for index in range(1, len(row_parts) + 1):
        pass_on(index)

    last = len(row_parts) - 1
    done = [0, 0, 0, 0]
    for index, (lo, hi) in enumerate(row_parts):
        @pl.when(has_down)
        def _():
            for copy in (forward_up(0) if index == 0 else []) + forward_up(index + 1):
                copy.wait_recv()

        @pl.when(has_up)
        def _():
            for copy in (forward_down(0) if index == 0 else []) + forward_down(index + 1):
                copy.wait_recv()

        widen((lo, hi))
        compress(0, (lo, hi))
        store_payload(0, index, (lo, hi))
        ends = [ROWS if index == last else hi - 2 * (k + 1) for k in range(4)]
        spans = list(zip(done, ends))
        run_velocity(theirs, 17, lambda i: i - 4, lambda i: i - 5, spans[0])
        run_stress(theirs, (14, lambda i: i - 3), (11, lambda i: i - 1), spans[1], image_of(1 - peer, 1))
        compress(1, spans[1])
        store_payload(1, index, spans[1])
        run_velocity(theirs, 11, lambda i: i - 1, lambda i: i - 2, spans[2])
        plain = (DEPTH, lambda i: i)
        run_stress(theirs, plain, plain, spans[3], image_of(1 - peer, 2))
        compress(2, spans[3])
        store_payload(2, index, spans[3])
        done = ends

    for index in range(across_count):
        across(index).wait_send()

    @pl.when(has_up)
    def _():
        for copy in mat_up():
            copy.wait_send()
        for step in range(STEPS):
            for copy in halo_up(step):
                copy.wait_send()
        for index in range(len(row_parts) + 1):
            for copy in forward_up(index):
                copy.wait_send()

    @pl.when(has_down)
    def _():
        for copy in mat_down():
            copy.wait_send()
        for step in range(STEPS):
            for copy in halo_down(step):
                copy.wait_send()
        for index in range(len(row_parts) + 1):
            for copy in forward_down(index):
                copy.wait_send()

    store_final.wait()
    for copy in stores:
        copy.wait()


def per_device(slabs, wavefield, buoyancy, lame_lambda, shear_modulus, scale_exponents, source_cells, wavelet):
    hbm = pl.BlockSpec(memory_space=pl.ANY)
    vmem = pl.BlockSpec(memory_space=pltpu.VMEM)
    smem = pl.BlockSpec(memory_space=pltpu.SMEM)
    parts = len(ROW_CUTS) - 1
    dma = pltpu.SemaphoreType.DMA
    final, stored, statistics = pl.pallas_call(
        functools.partial(kernel, slabs),
        out_shape=(
            jax.ShapeDtypeStruct(wavefield.shape, F32),
            jax.ShapeDtypeStruct((1, STEPS, 9, DEPTH, ROWS, COLS), BF16),
            jax.ShapeDtypeStruct((STEPS, 2), F32),
        ),
        in_specs=[hbm, hbm, hbm, hbm, vmem, smem, smem],
        out_specs=(hbm, hbm, vmem),
        scratch_shapes=[
            pltpu.VMEM((9, DEPTH + 2 * OWN, ROWS + 2 * PAD, COLS), F32),
            pltpu.VMEM((9, DEPTH + 2 * FAR, ROWS + 2 * PAD, COLS), F32),
            pltpu.VMEM((STEPS + 1, 9, DEPTH, ROWS, COLS), BF16),
            pltpu.VMEM((STEPS, 6, 2, ROWS, COLS), BF16),
            pltpu.VMEM((STEPS, 3, 3, ROWS, COLS), BF16),
            pltpu.VMEM((STEPS, 6, 2, ROWS, COLS), BF16),
            pltpu.VMEM((STEPS, 3, 3, ROWS, COLS), BF16),
            pltpu.VMEM((DEPTH + 2 * BUO, ROWS, COLS), F32),
            pltpu.VMEM((DEPTH + 2 * MOD, ROWS, COLS), F32),
            pltpu.VMEM((DEPTH + 2 * MOD, ROWS, COLS), F32),
            pltpu.VMEM((9, DEPTH + 2 * FAR, ROWS, COLS), BF16),
            pltpu.VMEM((STEPS, 9, DEPTH, ROWS, COLS), BF16),
            pltpu.VMEM((9 * ROWS, COLS), F32),
            pltpu.VMEM((9 * ROWS, COLS), F32),
            pltpu.VMEM((9 * ROWS // BLOCK, COLS), F32),
            pltpu.VMEM((STEPS, 3, YB, COLS), F32),
            pltpu.VMEM((2, 8, COLS), F32),
            pltpu.VMEM((2, max(LOW, slabs // LOW), 8, COLS), F32),
            dma((12,)),
            dma((1 + STEPS * parts,)),
            dma((STEPS, 2, 2)),
            dma((STEPS, 2, 2)),
            dma((3, 2)),
            dma((3, 2)),
            dma((1 + 2 * parts,)),
            dma((1 + 2 * parts,)),
            dma((1 + parts, 2, 2)),
            dma((1 + parts, 2, 2)),
            dma((2, max(LOW, slabs // LOW))),
            dma((2, max(LOW, slabs // LOW))),
        ],
        compiler_params=pltpu.CompilerParams(
            collective_id=0, has_side_effects=True, vmem_limit_bytes=60 * 1024 * 1024
        ),
        name="elastic_steps",
    )(
        wavefield, buoyancy, lame_lambda, shear_modulus,
        scale_exponents.reshape(9 * ROWS // BLOCK, COLS // BLOCK), source_cells, wavelet,
    )
    return final, stored, statistics[None]


def solution(mesh):
    return jax.shard_map(
        functools.partial(per_device, mesh.shape["space"]),
        mesh=mesh,
        in_specs=(
            P("peer", None, "space", None, None),
            P("space", None, None),
            P("space", None, None),
            P("space", None, None),
            P(None, "space", None, None),
            P(),
            P(),
        ),
        out_specs=(
            P("peer", None, "space", None, None),
            P("peer", None, None, "space", None, None),
            P("peer", None, None),
        ),
        check_vma=False,
    )
```

```python
import functools

import jax
import jax.numpy as jnp
from jax import lax
from jax.experimental import pallas as pl
from jax.experimental.pallas import tpu as pltpu
from jax.sharding import PartitionSpec as P

MESH = pl.DeviceIdType.MESH
F32 = jnp.float32
BF16 = jnp.bfloat16

BLOCK = 8
STEPS = 3
SOURCES = 8
DEPTH, ROWS, COLS = 8, 64, 128
PAD = 8
YB = 16
GROUP = 2
MATMUL_X = False
OWN = 3
FAR = 6
BUO, MOD = 5, 3
LOW = 8
ROW_CUTS = (0, 32, 48, 64)
VX, VY, VZ, SXX, SYY, SXY, SZZ, SXZ, SYZ = range(9)
clip_level = 4.0
energy_floor = 1e-06


def lanes(shape):
    return lax.broadcasted_iota(jnp.int32, shape, 1)


class Slab:
    def __init__(self, ref, lead, buoyancy, lame, shear, band):
        self.ref, self.lead = ref, lead
        self.buoyancy, self.lame, self.shear, self.band = buoyancy, lame, shear, band

    def rows(self, rows):
        self.lo, self.hi = rows
        self.y = self.lo // BLOCK * BLOCK
        self.n = -(-self.hi // BLOCK) * BLOCK - self.y
        return self

    def at(self, part, z):
        return self.ref[part, z + self.lead, pl.ds(self.y + PAD, self.n), :]

    def put(self, part, z, value):
        ref, n = self.ref, self.n
        head = BLOCK if self.lo % BLOCK else 0
        tail = BLOCK if self.hi % BLOCK else 0
        row = lax.broadcasted_iota(jnp.int32, (BLOCK, COLS), 0)
        if head:
            at = pl.ds(self.y + PAD, BLOCK)
            keep = row >= self.lo % BLOCK
            if n == BLOCK and tail:
                keep = keep & (row < self.hi % BLOCK)
                tail = 0
            ref[part, z + self.lead, at, :] = jnp.where(keep, value[:BLOCK], ref[part, z + self.lead, at, :])
        if tail:
            at = pl.ds(self.y + PAD + n - BLOCK, BLOCK)
            keep = row < self.hi % BLOCK
            ref[part, z + self.lead, at, :] = jnp.where(
                keep, value[n - BLOCK :], ref[part, z + self.lead, at, :]
            )
        if n - head - tail:
            ref[part, z + self.lead, pl.ds(self.y + PAD + head, n - head - tail), :] = value[head : n - tail]


    def dx(self, part, z, forward):
        f = self.at(part, z)
        if self.band is not None:
            top = f.astype(BF16)
            rest = (f - top.astype(F32)).astype(BF16)
            return jnp.dot(
                jnp.concatenate([top, rest], axis=1), self.band[int(forward)], preferred_element_type=F32
            )
        lane = lanes((1, COLS))
        after = jnp.where(lane < COLS - 1, pltpu.roll(f, COLS - 1, 1), 0.0)
        before = jnp.where(lane >= 1, pltpu.roll(f, 1, 1), 0.0)
        if forward:
            far = jnp.where(lane < COLS - 2, pltpu.roll(f, COLS - 2, 1), 0.0)
            return 27.0 * (after - f) - (far - before)
        far = jnp.where(lane >= 2, pltpu.roll(f, 2, 1), 0.0)
        return 27.0 * (f - before) - (after - far)

    def dy(self, part, z, forward):
        window = self.ref[part, z + self.lead, pl.ds(self.y, self.n + 2 * PAD), :]
        get = lambda shift: window[PAD + shift : PAD + shift + self.n]
        if forward:
            return get(1) - get(0), get(2) - get(-1)
        return get(0) - get(-1), get(1) - get(-2)

    def dz(self, part, z, forward):
        get = lambda shift: self.at(part, z + shift)
        if forward:
            return get(1) - get(0), get(2) - get(-1)
        return get(0) - get(-1), get(1) - get(-2)

    def mat(self, table, lead, z, factor):
        return table[z + lead, pl.ds(self.y, self.n), :] * factor

    def velocity(self, zs):
        results = []
        for z in zs:
            for part, along_x, along_y, along_z, at in (
                (VX, (SXX, True), (SXY, False), (SXZ, False), z),
                (VY, (SXY, False), (SYY, True), (SYZ, False), z),
                (VZ, (SXZ, False), (SYZ, False), (SZZ, True), z - 1),
            ):
                x = self.dx(along_x[0], at, along_x[1])
                y = self.dy(along_y[0], at, along_y[1])
                d = self.dz(along_z[0], at, along_z[1])
                change = 27.0 * (y[0] + d[0]) - (y[1] + d[1]) + x
                value = self.at(part, at) + self.mat(self.buoyancy, BUO, at, 1.0 / 24.0) * change
                results.append((part, at, value))
        for part, at, value in results:
            self.put(part, at, value)

    def stress(self, zs, image, plane_shear=True):
        results = []
        for z in zs:
            join = lambda pair: 27.0 * pair[0] - pair[1]
            strain = (
                self.dx(VX, z, False), join(self.dy(VY, z, False)), join(self.dz(VZ, z, False)),
            )
            shear = self.mat(self.shear, MOD, z, 1.0 / 24.0)
            pressure = self.mat(self.lame, MOD, z, 1.0 / 24.0) * (
                strain[0] + strain[1] + strain[2]
            ) + image(z, self.y, self.n)
            double = shear + shear
            for part, value in zip((SXX, SYY, SZZ), strain):
                results.append((part, z, self.at(part, z) + (pressure + double * value)))
            if plane_shear:
                change = join(self.dy(VX, z, True)) + self.dx(VY, z, True)
                results.append((SXY, z, self.at(SXY, z) + shear * change))
            change = join(self.dz(VX, z, True)) + self.dx(VZ, z, True)
            results.append((SXZ, z, self.at(SXZ, z) + shear * change))
            y, d = self.dy(VZ, z, True), self.dz(VY, z, True)
            change = 27.0 * (y[0] + d[0]) - (y[1] + d[1])
            results.append((SYZ, z, self.at(SYZ, z) + shear * change))
        for part, at, value in results:
            self.put(part, at, value)


def over(count, place, group, body):
    @pl.loop(0, count // group)
    def _(i):
        body([place(i * group + k) for k in range(group)])

    if count % group:
        body([place(i) for i in range(count // group * group, count)])


def kernel(
    slabs,
    wave_hbm, buo_hbm, lame_hbm, shear_hbm, exps, cells, wavelet,
    final_hbm, stored_hbm, stats_out,
    own, other, mirror, low_a, low_b, high_a, high_b, buo, lame, shear, got, packed,
    up_rows, down_rows, exp_rows, sums, stat_src, stat_rx,
    in_sem, out_sem, halo_send, halo_recv, mat_send, mat_recv,
    x_send, x_recv, fwd_send, fwd_recv, stat_send, stat_recv, *extra,
):
    me, peer = lax.axis_index("space"), lax.axis_index("peer")
    has_down, has_up = me > 0, me < slabs - 1
    up, down = (me + 1, peer), (me - 1, peer)
    partner = (me, 1 - peer)
    half = slabs // 2
    below_cross, above_cross = me == half - 1, me == half
    cross_up, cross_down = (me + 1, 1 - peer), (me - 1, 1 - peer)
    groups = slabs // LOW
    block, lane_of = me // LOW, lax.rem(me, LOW)
    near_peers = [(block * LOW + lax.rem(lane_of + k, LOW), peer) for k in range(1, LOW)]
    wide_peers = [(lax.rem(block + k, groups) * LOW + lane_of, peer) for k in range(1, groups)]

    barrier = pltpu.get_barrier_semaphore()
    for device in [partner] + near_peers + wide_peers:
        pl.semaphore_signal(barrier, inc=1, device_id=device, device_id_type=MESH)

    @pl.when(has_up)
    def _():
        pl.semaphore_signal(barrier, inc=1, device_id=up, device_id_type=MESH)

    @pl.when(has_down)
    def _():
        pl.semaphore_signal(barrier, inc=1, device_id=down, device_id_type=MESH)

    @pl.when(below_cross)
    def _():
        pl.semaphore_signal(barrier, inc=1, device_id=cross_up, device_id_type=MESH)

    @pl.when(above_cross)
    def _():
        pl.semaphore_signal(barrier, inc=1, device_id=cross_down, device_id_type=MESH)

    def remote(source, target, send, recv, device):
        return pltpu.make_async_remote_copy(
            src_ref=source, dst_ref=target, send_sem=send, recv_sem=recv,
            device_id=device, device_id_type=MESH,
        )

    inner = pl.ds(PAD, ROWS)
    loads = [
        pltpu.make_async_copy(
            wave_hbm.at[0, part], own.at[part, pl.ds(OWN, DEPTH), inner, :], in_sem.at[part]
        )
        for part in range(9)
    ]
    tables = ((buo_hbm, buo, BUO), (lame_hbm, lame, MOD), (shear_hbm, shear, MOD))
    mat_loads = [
        pltpu.make_async_copy(source, target.at[pl.ds(lead, DEPTH)], in_sem.at[9 + k])
        for k, (source, target, lead) in enumerate(tables)
    ]
    for copy in loads + mat_loads:
        copy.start()

    zero = jnp.zeros((PAD, COLS), F32)
    plane = jnp.zeros((ROWS, COLS), F32)

    @pl.loop(0, 9)
    def _(part):
        for z in range(DEPTH + 2 * OWN):
            own[part, z, pl.ds(0, PAD), :] = zero
            own[part, z, pl.ds(PAD + ROWS, PAD), :] = zero
        for z in list(range(OWN)) + list(range(OWN + DEPTH, DEPTH + 2 * OWN)):
            own[part, z, inner, :] = plane

    def clear(base_mat, base_own):
        for _, target, lead in tables:
            for z in range(lead):
                target[z + (lead + DEPTH if base_mat else 0)] = plane

        @pl.loop(0, 9)
        def _(part):
            for z in range(FAR):
                got[part, z + base_own] = jnp.zeros((ROWS, COLS), BF16)

    @pl.when(jnp.logical_not(has_down))
    def _():
        clear(0, 0)

    @pl.when(jnp.logical_not(has_up))
    def _():
        clear(1, FAR + DEPTH)

    sums[...] = jnp.zeros_like(sums)

    for copy in loads:
        copy.wait()

    @pl.loop(0, 9)
    def _(part):
        for z in (0, 1, 2, 5, 6, 7):
            mirror[0, part, z] = own[part, z + OWN, inner, :].astype(BF16)

    greeted = [flag.astype(jnp.int32) for flag in (has_up, has_down, below_cross, above_cross)]
    pl.semaphore_wait(barrier, 1 + len(near_peers) + len(wide_peers) + sum(greeted))

    def halo_up(step):
        return [
            remote(mirror.at[step, pl.ds(0, 6), pl.ds(6, 2)], low_a.at[step],
                   halo_send.at[step, 0, 0], halo_recv.at[step, 0, 0], up),
            remote(mirror.at[step, pl.ds(6, 3), pl.ds(5, 3)], low_b.at[step],
                   halo_send.at[step, 0, 1], halo_recv.at[step, 0, 1], up),
        ]

    def halo_down(step):
        return [
            remote(mirror.at[step, pl.ds(0, 6), pl.ds(0, 2)], high_a.at[step],
                   halo_send.at[step, 1, 0], halo_recv.at[step, 1, 0], down),
            remote(mirror.at[step, pl.ds(6, 3), pl.ds(0, 3)], high_b.at[step],
                   halo_send.at[step, 1, 1], halo_recv.at[step, 1, 1], down),
        ]

    def mat_up():
        return [
            remote(target.at[pl.ds(DEPTH, lead)], target.at[pl.ds(0, lead)],
                   mat_send.at[k, 0], mat_recv.at[k, 0], up)
            for k, (_, target, lead) in enumerate(tables)
        ]

    def mat_down():
        return [
            remote(target.at[pl.ds(lead, lead)], target.at[pl.ds(lead + DEPTH, lead)],
                   mat_send.at[k, 1], mat_recv.at[k, 1], down)
            for k, (_, target, lead) in enumerate(tables)
        ]

    def send_halos(step):
        @pl.when(has_up)
        def _():
            for copy in halo_up(step):
                copy.start()

        @pl.when(has_down)
        def _():
            for copy in halo_down(step):
                copy.start()

    send_halos(0)
    for copy in mat_loads:
        copy.wait()

    @pl.when(has_up)
    def _():
        for copy in mat_up():
            copy.start()

    @pl.when(has_down)
    def _():
        for copy in mat_down():
            copy.start()

    spread = (
        lax.broadcasted_iota(jnp.int32, (COLS // BLOCK, COLS), 0)
        == lanes((COLS // BLOCK, COLS)) // BLOCK
    ).astype(F32)
    exp_rows[...] = jnp.dot(
        exps[...].astype(F32), spread, preferred_element_type=F32, precision=lax.Precision.HIGHEST
    )

    @pl.loop(0, 9 * ROWS // BLOCK)
    def _(i):
        level = jnp.broadcast_to(exp_rows[pl.ds(i, 1), :], (BLOCK, COLS))
        upscale = jnp.ones((BLOCK, COLS), F32)
        downscale = upscale
        for exponent in (-2, -1, 1, 2):
            chosen = jnp.abs(level - exponent) < 0.5
            upscale = jnp.where(chosen, 2.0**exponent, upscale)
            downscale = jnp.where(chosen, 2.0**-exponent, downscale)
        up_rows[pl.ds(pl.multiple_of(i * BLOCK, BLOCK), BLOCK), :] = upscale
        down_rows[pl.ds(pl.multiple_of(i * BLOCK, BLOCK), BLOCK), :] = downscale

    @pl.loop(0, 9)
    def _(part):
        for z in range(DEPTH + 2 * FAR):
            other[part, z, pl.ds(0, PAD), :] = zero
            other[part, z, pl.ds(PAD + ROWS, PAD), :] = zero

    band = extra[0] if MATMUL_X else None
    if MATMUL_X:
        row = lax.broadcasted_iota(jnp.int32, (2 * COLS, COLS), 0)
        offset = lax.rem(row, COLS) - lanes((2 * COLS, COLS))
        for k, sign in ((0, -1), (1, 1)):
            weight = jnp.where(offset == 0, -27.0 * sign, 0.0)
            weight = jnp.where(offset == sign, 27.0 * sign, weight)
            weight = jnp.where(offset == -sign, 1.0 * sign, weight)
            weight = jnp.where(offset == 2 * sign, -1.0 * sign, weight)
            band[k] = weight.astype(BF16)

    row_parts = list(zip(ROW_CUTS[:-1], ROW_CUTS[1:]))

    def across(index):
        if index == 0:
            layer, count, lo, hi = 3, 2, 0, ROWS
        else:
            lo, hi = row_parts[(index - 1) // 2]
            layer, count = (0, 3) if index % 2 else (5, 3)
        return remote(
            mirror.at[1, :, pl.ds(layer, count), pl.ds(lo, hi - lo)],
            got.at[:, pl.ds(FAR + layer, count), pl.ds(lo, hi - lo)],
            x_send.at[index], x_recv.at[index], partner,
        )

    across_count = 1 + 2 * len(row_parts)

    def forward(index, source, lead, upward, device):
        side, base = (0, 0) if upward else (1, FAR + DEPTH)
        if index == 0:
            return [
                remote(source.at[:, pl.ds(lead + 3, 2)], got.at[:, pl.ds(base + (1 if upward else 3), 2)],
                       fwd_send.at[0, side, 0], fwd_recv.at[0, side, 0], device)
            ]
        lo, hi = row_parts[index - 1]
        rows, deep = pl.ds(lo, hi - lo), pl.ds(6, 3)
        first, single = (5, 2) if upward else (0, 5)
        return [
            remote(source.at[:, pl.ds(lead + first, 3), rows],
                   got.at[:, pl.ds(base + (3 if upward else 0), 3), rows],
                   fwd_send.at[index, side, 0], fwd_recv.at[index, side, 0], device),
            remote(source.at[deep, pl.ds(lead + single, 1), rows],
                   got.at[deep, pl.ds(base + (0 if upward else 5), 1), rows],
                   fwd_send.at[index, side, 1], fwd_recv.at[index, side, 1], device),
        ]

    def forward_up(index):
        return forward(index, got, FAR, True, up)

    def forward_down(index):
        return forward(index, got, FAR, False, down)

    def straight_up(index):
        return forward(index, mirror.at[1], 0, True, cross_up)

    def straight_down(index):
        return forward(index, mirror.at[1], 0, False, cross_down)

    def each(flag, copies, act):
        @pl.when(flag)
        def _():
            for copy in copies():
                act(copy)

    begin, sent = (lambda copy: copy.start()), (lambda copy: copy.wait_send())
    passes_up = has_up & jnp.logical_not(below_cross)
    passes_down = has_down & jnp.logical_not(above_cross)

    def pass_on(index):
        if index == 0:
            across(0).wait_recv()
        else:
            across(2 * index - 1).wait_recv()
            across(2 * index).wait_recv()
        each(passes_up, lambda: forward_up(index), begin)
        each(passes_down, lambda: forward_down(index), begin)

    def send_across(index):
        if index == 0:
            across(0).start()
        else:
            across(2 * index - 1).start()
            across(2 * index).start()
        each(below_cross, lambda: straight_up(index), begin)
        each(above_cross, lambda: straight_down(index), begin)

    def image_of(shot, step):
        def image(z, y, n):
            first = ((me * DEPTH + z) * ROWS + y) * COLS
            place = lax.broadcasted_iota(jnp.int32, (n, COLS), 0) * COLS + lanes((n, COLS))
            total = jnp.zeros((n, COLS), F32)
            for j in range(SOURCES):
                total = total + jnp.where(place == cells[shot, j] - first, wavelet[step, shot, j], 0.0)
            return total

        return image

    mine = Slab(own, OWN, buo, lame, shear, band).rows((0, ROWS))

    def record(step, count, place):
        def body(k, carry):
            part = k // (count // 2)
            down = down_rows[pl.ds(pl.multiple_of(part * ROWS, ROWS), ROWS), :]
            up_scale = up_rows[pl.ds(pl.multiple_of(part * ROWS, ROWS), ROWS), :]
            sizes, misfits, squares = carry
            for half in range(2):
                z = place(lax.rem(k, count // 2) * 2 + half)
                value = mine.at(part, z)
                rounded = value.astype(BF16)
                mirror[step + 1, part, z] = rounded
                level = jnp.clip(rounded.astype(F32) * down, -clip_level, clip_level)
                misfit = value - level * up_scale
                for y in range(0, ROWS, YB):
                    at = slice(y, y + YB)
                    sizes = sizes + jnp.abs(level[at])
                    misfits = misfits + misfit[at] * misfit[at]
                    squares = squares + value[at] * value[at]
            return sizes, misfits, squares

        start = tuple(sums[step, k] for k in range(3))
        for k, total in enumerate(lax.fori_loop(0, 9 * (count // 2), body, start)):
            sums[step, k] = total

    edges = lambda first, gap: (lambda i: first + i + (i // 3) * gap)

    @pl.loop(0, STEPS)
    def _(step):
        @pl.when(step == 2)
        def _():
            pass_on(0)

        image = image_of(peer, step)
        over(5, lambda i: i + 2, GROUP, mine.velocity)
        middle = (2, lambda i: i + 3)
        over(*middle, GROUP, lambda zs: mine.stress(zs, image))
        record(step, *middle)

        @pl.when(step == 0)
        def _():
            send_across(0)

        @pl.when(has_down)
        def _():
            for copy in halo_up(step):
                copy.wait_recv()

            @pl.when(step == 0)
            def _():
                for copy in mat_up():
                    copy.wait_recv()

            @pl.loop(0, 6)
            def _(part):
                for z in range(2):
                    own[part, OWN - 2 + z, inner, :] = low_a[step, part, z].astype(F32)

            @pl.loop(0, 3)
            def _(part):
                for z in range(3):
                    own[part + 6, OWN - 3 + z, inner, :] = low_b[step, part, z].astype(F32)

        @pl.when(has_up)
        def _():
            for copy in halo_down(step):
                copy.wait_recv()

            @pl.when(step == 0)
            def _():
                for copy in mat_down():
                    copy.wait_recv()

            @pl.loop(0, 6)
            def _(part):
                for z in range(2):
                    own[part, OWN + DEPTH + z, inner, :] = high_a[step, part, z].astype(F32)

            @pl.loop(0, 3)
            def _(part):
                for z in range(3):
                    own[part + 6, OWN + DEPTH + z, inner, :] = high_b[step, part, z].astype(F32)

        over(6, edges(-1, 5), GROUP, mine.velocity)
        outer = (6, edges(0, 2))
        over(*outer, GROUP, lambda zs: mine.stress(zs, image))
        record(step, *outer)

        @pl.when(step < STEPS - 1)
        def _():
            send_halos(step + 1)

        @pl.when(step == 0)
        def _():
            send_across(1)

        @pl.when(step == 1)
        def _():
            for index in range(2, len(row_parts) + 1):
                send_across(index)

    store_final = pltpu.make_async_copy(
        own.at[:, pl.ds(OWN, DEPTH), inner, :], final_hbm.at[0], out_sem.at[0]
    )
    store_final.start()

    row8 = lax.broadcasted_iota(jnp.int32, (8, COLS), 0)
    lane8 = lanes((8, COLS))
    tile = jnp.zeros((8, COLS), F32)
    for step in range(STEPS):
        for k in range(3):
            tile = tile + jnp.where((row8 == k) & (lane8 == step), jnp.sum(sums[step, k]), 0.0)

    def gather(phase, peers, mine_at, size, tile):
        stat_src[phase] = tile
        copies = [
            remote(stat_src.at[phase], stat_rx.at[phase, mine_at],
                   stat_send.at[phase, k], stat_recv.at[phase, k], device)
            for k, device in enumerate(peers)
        ]
        for copy in copies:
            copy.start()
        stat_rx[phase, mine_at] = tile
        for copy in copies:
            copy.wait()
        total = stat_rx[phase, 0]
        for k in range(1, size):
            total = total + stat_rx[phase, k]
        return total

    tile = gather(0, near_peers, lane_of, LOW, tile)
    tile = gather(1, wide_peers, block, groups, tile)
    scaled = tile * (1.0 / (9 * slabs * DEPTH * ROWS * COLS))
    ratio = scaled[1:2] / (scaled[2:3] + energy_floor)
    stats_out[0:1, :] = scaled[0:1, :STEPS]
    stats_out[1:2, :] = jnp.sqrt(ratio)[:, :STEPS]

    theirs = Slab(other, FAR, buo, lame, shear, band)

    def widen(rows):
        lo, hi = rows

        def move(part, z):
            other[part, z, pl.ds(PAD + lo, hi - lo), :] = got[part, z, pl.ds(lo, hi - lo), :].astype(F32)

        @pl.loop(0, 9)
        def _(part):
            for z in range(1, DEPTH + 2 * FAR - 1):
                move(part, z)

        for part in range(6, 9):
            for z in (0, DEPTH + 2 * FAR - 1):
                move(part, z)

    def compress(step, rows):
        lo, hi = rows

        @pl.loop(0, 9)
        def _(part):
            for y in range(lo // YB * YB, hi, YB):
                row = lax.broadcasted_iota(jnp.int32, (YB, COLS), 0) + y
                down = down_rows[pl.ds(pl.multiple_of(part * ROWS + y, YB), YB), :]
                for z in range(DEPTH):
                    value = other[part, z + FAR, pl.ds(PAD + y, YB), :]
                    level = jnp.clip(value * down, -clip_level, clip_level)
                    if lo > y or hi < y + YB:
                        before = packed[step, part, z, pl.ds(y, YB), :].astype(F32)
                        level = jnp.where((row >= lo) & (row < hi), level, before)
                    packed[step, part, z, pl.ds(y, YB), :] = level.astype(BF16)

    stores = []

    def store_payload(step, index, rows):
        lo, hi = (bound // YB * YB for bound in rows)
        if lo < hi:
            stores.append(
                pltpu.make_async_copy(
                    packed.at[step, :, :, pl.ds(lo, hi - lo)],
                    stored_hbm.at[0, step, :, :, pl.ds(lo, hi - lo)],
                    out_sem.at[1 + step * len(row_parts) + index],
                )
            )
            stores[-1].start()

    for index in range(1, len(row_parts) + 1):
        pass_on(index)

    last = len(row_parts) - 1
    done = [0, 0, 0, 0]
    for index, (lo, hi) in enumerate(row_parts):
        @pl.when(has_down)
        def _():
            for copy in (forward_up(0) if index == 0 else []) + forward_up(index + 1):
                copy.wait_recv()

        @pl.when(has_up)
        def _():
            for copy in (forward_down(0) if index == 0 else []) + forward_down(index + 1):
                copy.wait_recv()

        widen((lo, hi))
        compress(0, (lo, hi))
        store_payload(0, index, (lo, hi))
        ends = [ROWS if index == last else hi - 2 * (k + 1) for k in range(4)]
        wide_group = GROUP * (1 if hi - lo > 32 else 2)
        span = [(first, end) for first, end in zip(done, ends)]
        theirs.rows(span[0])
        over(17, lambda i: i - 4, wide_group, theirs.velocity)
        theirs.rows(span[1])
        image = image_of(1 - peer, 1)
        over(14, lambda i: i - 3, wide_group, lambda zs: theirs.stress(zs, image))
        compress(1, span[1])
        store_payload(1, index, span[1])
        theirs.rows(span[2])
        over(11, lambda i: i - 1, wide_group, theirs.velocity)
        theirs.rows(span[3])
        image = image_of(1 - peer, 2)
        over(DEPTH, lambda i: i, wide_group, lambda zs: theirs.stress(zs, image))
        compress(2, span[3])
        store_payload(2, index, span[3])
        done = ends

    for index in range(across_count):
        across(index).wait_send()

    @pl.when(has_up)
    def _():
        for copy in mat_up():
            copy.wait_send()
        for step in range(STEPS):
            for copy in halo_up(step):
                copy.wait_send()

    @pl.when(has_down)
    def _():
        for copy in mat_down():
            copy.wait_send()
        for step in range(STEPS):
            for copy in halo_down(step):
                copy.wait_send()

    for index in range(len(row_parts) + 1):
        each(passes_up, lambda: forward_up(index), sent)
        each(passes_down, lambda: forward_down(index), sent)
        each(below_cross, lambda: straight_up(index), sent)
        each(above_cross, lambda: straight_down(index), sent)

    store_final.wait()
    for copy in stores:
        copy.wait()


def per_device(slabs, wavefield, buoyancy, lame_lambda, shear_modulus, scale_exponents, source_cells, wavelet):
    hbm = pl.BlockSpec(memory_space=pl.ANY)
    vmem = pl.BlockSpec(memory_space=pltpu.VMEM)
    smem = pl.BlockSpec(memory_space=pltpu.SMEM)
    parts = len(ROW_CUTS) - 1
    dma = pltpu.SemaphoreType.DMA
    final, stored, statistics = pl.pallas_call(
        functools.partial(kernel, slabs),
        out_shape=(
            jax.ShapeDtypeStruct(wavefield.shape, F32),
            jax.ShapeDtypeStruct((1, STEPS, 9, DEPTH, ROWS, COLS), BF16),
            jax.ShapeDtypeStruct((2, STEPS), F32),
        ),
        in_specs=[hbm, hbm, hbm, hbm, vmem, smem, smem],
        out_specs=(hbm, hbm, vmem),
        scratch_shapes=[
            pltpu.VMEM((9, DEPTH + 2 * OWN, ROWS + 2 * PAD, COLS), F32),
            pltpu.VMEM((9, DEPTH + 2 * FAR, ROWS + 2 * PAD, COLS), F32),
            pltpu.VMEM((STEPS + 1, 9, DEPTH, ROWS, COLS), BF16),
            pltpu.VMEM((STEPS, 6, 2, ROWS, COLS), BF16),
            pltpu.VMEM((STEPS, 3, 3, ROWS, COLS), BF16),
            pltpu.VMEM((STEPS, 6, 2, ROWS, COLS), BF16),
            pltpu.VMEM((STEPS, 3, 3, ROWS, COLS), BF16),
            pltpu.VMEM((DEPTH + 2 * BUO, ROWS, COLS), F32),
            pltpu.VMEM((DEPTH + 2 * MOD, ROWS, COLS), F32),
            pltpu.VMEM((DEPTH + 2 * MOD, ROWS, COLS), F32),
            pltpu.VMEM((9, DEPTH + 2 * FAR, ROWS, COLS), BF16),
            pltpu.VMEM((STEPS, 9, DEPTH, ROWS, COLS), BF16),
            pltpu.VMEM((9 * ROWS, COLS), F32),
            pltpu.VMEM((9 * ROWS, COLS), F32),
            pltpu.VMEM((9 * ROWS // BLOCK, COLS), F32),
            pltpu.VMEM((STEPS, 3, YB, COLS), F32),
            pltpu.VMEM((2, 8, COLS), F32),
            pltpu.VMEM((2, max(LOW, slabs // LOW), 8, COLS), F32),
            dma((12,)),
            dma((1 + STEPS * parts,)),
            dma((STEPS, 2, 2)),
            dma((STEPS, 2, 2)),
            dma((3, 2)),
            dma((3, 2)),
            dma((1 + 2 * parts,)),
            dma((1 + 2 * parts,)),
            dma((1 + parts, 2, 2)),
            dma((1 + parts, 2, 2)),
            dma((2, max(LOW, slabs // LOW))),
            dma((2, max(LOW, slabs // LOW))),
        ]
        + ([pltpu.VMEM((2, 2 * COLS, COLS), BF16)] if MATMUL_X else []),
        compiler_params=pltpu.CompilerParams(
            collective_id=0, has_side_effects=True, vmem_limit_bytes=60 * 1024 * 1024
        ),
        name="elastic_steps",
    )(
        wavefield, buoyancy, lame_lambda, shear_modulus,
        scale_exponents.reshape(9 * ROWS // BLOCK, COLS // BLOCK), source_cells,
        wavelet.transpose(1, 0, 2),
    )
    return final, stored, statistics.T[None]


def solution(mesh):
    return jax.shard_map(
        functools.partial(per_device, mesh.shape["space"]),
        mesh=mesh,
        in_specs=(
            P("peer", None, "space", None, None),
            P("space", None, None),
            P("space", None, None),
            P("space", None, None),
            P(None, "space", None, None),
            P(),
            P(),
        ),
        out_specs=(
            P("peer", None, "space", None, None),
            P("peer", None, None, "space", None, None),
            P("peer", None, None),
        ),
        check_vma=False,
    )
```

```python
import functools

import jax
import jax.numpy as jnp
from jax import lax
from jax.experimental import pallas as pl
from jax.experimental.pallas import tpu as pltpu
from jax.sharding import PartitionSpec as P

MESH = pl.DeviceIdType.MESH
F32 = jnp.float32
BF16 = jnp.bfloat16

BLOCK = 8
STEPS = 3
SOURCES = 8
DEPTH, ROWS, COLS = 8, 64, 128
PAD = 8
YB = 16
GROUP = 2
MATMUL_X = False
OWN = 3
FAR = 6
BUO, MOD = 5, 3
LOW = 8
ROW_CUTS = (0, 32, 48, 64)
VX, VY, VZ, SXX, SYY, SXY, SZZ, SXZ, SYZ = range(9)
clip_level = 4.0
energy_floor = 1e-06


def lanes(shape):
    return lax.broadcasted_iota(jnp.int32, shape, 1)


class Slab:
    def __init__(self, ref, lead, buoyancy, lame, shear, band):
        self.ref, self.lead = ref, lead
        self.buoyancy, self.lame, self.shear, self.band = buoyancy, lame, shear, band

    def rows(self, rows):
        self.lo, self.hi = rows
        self.y = self.lo // BLOCK * BLOCK
        self.n = -(-self.hi // BLOCK) * BLOCK - self.y
        return self

    def at(self, part, z):
        return self.ref[part, z + self.lead, pl.ds(self.y + PAD, self.n), :]

    def put(self, part, z, value):
        ref, n = self.ref, self.n
        head = BLOCK if self.lo % BLOCK else 0
        tail = BLOCK if self.hi % BLOCK else 0
        row = lax.broadcasted_iota(jnp.int32, (BLOCK, COLS), 0)
        if head:
            at = pl.ds(self.y + PAD, BLOCK)
            keep = row >= self.lo % BLOCK
            if n == BLOCK and tail:
                keep = keep & (row < self.hi % BLOCK)
                tail = 0
            ref[part, z + self.lead, at, :] = jnp.where(keep, value[:BLOCK], ref[part, z + self.lead, at, :])
        if tail:
            at = pl.ds(self.y + PAD + n - BLOCK, BLOCK)
            keep = row < self.hi % BLOCK
            ref[part, z + self.lead, at, :] = jnp.where(
                keep, value[n - BLOCK :], ref[part, z + self.lead, at, :]
            )
        if n - head - tail:
            ref[part, z + self.lead, pl.ds(self.y + PAD + head, n - head - tail), :] = value[head : n - tail]


    def dx(self, part, z, forward):
        f = self.at(part, z)
        if self.band is not None:
            top = f.astype(BF16)
            rest = (f - top.astype(F32)).astype(BF16)
            return jnp.dot(
                jnp.concatenate([top, rest], axis=1), self.band[int(forward)], preferred_element_type=F32
            )
        lane = lanes((1, COLS))
        after = jnp.where(lane < COLS - 1, pltpu.roll(f, COLS - 1, 1), 0.0)
        before = jnp.where(lane >= 1, pltpu.roll(f, 1, 1), 0.0)
        if forward:
            far = jnp.where(lane < COLS - 2, pltpu.roll(f, COLS - 2, 1), 0.0)
            return 27.0 * (after - f) - (far - before)
        far = jnp.where(lane >= 2, pltpu.roll(f, 2, 1), 0.0)
        return 27.0 * (f - before) - (after - far)

    def dy(self, part, z, forward):
        get = lambda shift: self.ref[part, z + self.lead, pl.ds(self.y + PAD + shift, self.n), :]
        if forward:
            return get(1) - get(0), get(2) - get(-1)
        return get(0) - get(-1), get(1) - get(-2)

    def dz(self, part, z, forward):
        get = lambda shift: self.at(part, z + shift)
        if forward:
            return get(1) - get(0), get(2) - get(-1)
        return get(0) - get(-1), get(1) - get(-2)

    def mat(self, table, lead, z, factor):
        return table[z + lead, pl.ds(self.y, self.n), :] * factor

    def velocity(self, zs):
        results = []
        for z in zs:
            for part, along_x, along_y, along_z, at in (
                (VX, (SXX, True), (SXY, False), (SXZ, False), z),
                (VY, (SXY, False), (SYY, True), (SYZ, False), z),
                (VZ, (SXZ, False), (SYZ, False), (SZZ, True), z - 1),
            ):
                x = self.dx(along_x[0], at, along_x[1])
                y = self.dy(along_y[0], at, along_y[1])
                d = self.dz(along_z[0], at, along_z[1])
                change = 27.0 * (y[0] + d[0]) - (y[1] + d[1]) + x
                value = self.at(part, at) + self.mat(self.buoyancy, BUO, at, 1.0 / 24.0) * change
                results.append((part, at, value))
        for part, at, value in results:
            self.put(part, at, value)

    def stress(self, zs, image, plane_shear=True):
        results = []
        for z in zs:
            join = lambda pair: 27.0 * pair[0] - pair[1]
            strain = (
                self.dx(VX, z, False), join(self.dy(VY, z, False)), join(self.dz(VZ, z, False)),
            )
            shear = self.mat(self.shear, MOD, z, 1.0 / 24.0)
            pressure = self.mat(self.lame, MOD, z, 1.0 / 24.0) * (
                strain[0] + strain[1] + strain[2]
            ) + image(z, self.y, self.n)
            double = shear + shear
            for part, value in zip((SXX, SYY, SZZ), strain):
                results.append((part, z, self.at(part, z) + (pressure + double * value)))
            if plane_shear:
                change = join(self.dy(VX, z, True)) + self.dx(VY, z, True)
                results.append((SXY, z, self.at(SXY, z) + shear * change))
            change = join(self.dz(VX, z, True)) + self.dx(VZ, z, True)
            results.append((SXZ, z, self.at(SXZ, z) + shear * change))
            y, d = self.dy(VZ, z, True), self.dz(VY, z, True)
            change = 27.0 * (y[0] + d[0]) - (y[1] + d[1])
            results.append((SYZ, z, self.at(SYZ, z) + shear * change))
        for part, at, value in results:
            self.put(part, at, value)


def over(count, place, group, body):
    @pl.loop(0, count // group)
    def _(i):
        body([place(i * group + k) for k in range(group)])

    if count % group:
        body([place(i) for i in range(count // group * group, count)])


def kernel(
    slabs,
    wave_hbm, buo_hbm, lame_hbm, shear_hbm, exps, cells, wavelet,
    final_hbm, stored_hbm, stats_out,
    own, other, mirror, low_a, low_b, high_a, high_b, buo, lame, shear, mat_out, mat_in, got, packed,
    up_rows, down_rows, exp_rows, sums, stat_src, stat_rx, image_own, image_far,
    in_sem, out_sem, halo_send, halo_recv, mat_send, mat_recv,
    x_send, x_recv, fwd_send, fwd_recv, stat_send, stat_recv, *extra,
):
    me, peer = lax.axis_index("space"), lax.axis_index("peer")
    has_down, has_up = me > 0, me < slabs - 1
    up, down = (me + 1, peer), (me - 1, peer)
    partner = (me, 1 - peer)
    half = slabs // 2
    below_cross, above_cross = me == half - 1, me == half
    cross_up, cross_down = (me + 1, 1 - peer), (me - 1, 1 - peer)
    groups = slabs // LOW
    block, lane_of = me // LOW, lax.rem(me, LOW)
    near_peers = [(block * LOW + lax.rem(lane_of + k, LOW), peer) for k in range(1, LOW)]
    wide_peers = [(lax.rem(block + k, groups) * LOW + lane_of, peer) for k in range(1, groups)]

    barrier = pltpu.get_barrier_semaphore()
    for device in [partner] + near_peers + wide_peers:
        pl.semaphore_signal(barrier, inc=1, device_id=device, device_id_type=MESH)

    @pl.when(has_up)
    def _():
        pl.semaphore_signal(barrier, inc=1, device_id=up, device_id_type=MESH)

    @pl.when(has_down)
    def _():
        pl.semaphore_signal(barrier, inc=1, device_id=down, device_id_type=MESH)

    @pl.when(below_cross)
    def _():
        pl.semaphore_signal(barrier, inc=1, device_id=cross_up, device_id_type=MESH)

    @pl.when(above_cross)
    def _():
        pl.semaphore_signal(barrier, inc=1, device_id=cross_down, device_id_type=MESH)

    def remote(source, target, send, recv, device):
        return pltpu.make_async_remote_copy(
            src_ref=source, dst_ref=target, send_sem=send, recv_sem=recv,
            device_id=device, device_id_type=MESH,
        )

    inner = pl.ds(PAD, ROWS)
    loads = [
        pltpu.make_async_copy(
            wave_hbm.at[0, part], own.at[part, pl.ds(OWN, DEPTH), inner, :], in_sem.at[part]
        )
        for part in range(9)
    ]
    tables = ((buo_hbm, buo, BUO), (lame_hbm, lame, MOD), (shear_hbm, shear, MOD))
    mat_loads = [
        pltpu.make_async_copy(source, target.at[pl.ds(lead, DEPTH)], in_sem.at[9 + k])
        for k, (source, target, lead) in enumerate(tables)
    ]
    for copy in loads + mat_loads:
        copy.start()

    zero = jnp.zeros((PAD, COLS), F32)
    plane = jnp.zeros((ROWS, COLS), F32)

    @pl.loop(0, 9)
    def _(part):
        for z in range(DEPTH + 2 * OWN):
            own[part, z, pl.ds(0, PAD), :] = zero
            own[part, z, pl.ds(PAD + ROWS, PAD), :] = zero
        for z in list(range(OWN)) + list(range(OWN + DEPTH, DEPTH + 2 * OWN)):
            own[part, z, inner, :] = plane

    def clear(base_mat, base_own):
        for _, target, lead in tables:
            for z in range(lead):
                target[z + (lead + DEPTH if base_mat else 0)] = plane

        @pl.loop(0, 9)
        def _(part):
            for z in range(FAR):
                got[part, z + base_own] = jnp.zeros((ROWS, COLS), BF16)

    @pl.when(jnp.logical_not(has_down))
    def _():
        clear(0, 0)

    @pl.when(jnp.logical_not(has_up))
    def _():
        clear(1, FAR + DEPTH)

    for copy in loads:
        copy.wait()

    @pl.loop(0, 9)
    def _(part):
        for z in (0, 1, 2, 5, 6, 7):
            mirror[0, part, z] = own[part, z + OWN, inner, :].astype(BF16)

    mat_layers = ((0, buo, BUO), (BUO, lame, MOD), (BUO + MOD, shear, MOD))
    for copy in mat_loads:
        copy.wait()
    for at, target, lead in mat_layers:
        for z in range(lead):
            mat_out[0, at + z] = target[DEPTH + z].astype(BF16)
            mat_out[1, at + z] = target[lead + z].astype(BF16)

    def place_sources(target, first_z, count, shot, step):
        place = lax.broadcasted_iota(jnp.int32, (ROWS, COLS), 0) * COLS + lanes((ROWS, COLS))

        @pl.loop(0, count)
        def _(i):
            first = (me * DEPTH + first_z + i) * ROWS * COLS
            total = jnp.zeros((ROWS, COLS), F32)
            for j in range(SOURCES):
                total = total + jnp.where(place == cells[shot, j] - first, wavelet[step, shot, j], 0.0)
            target[i] = total

    for step in range(STEPS):
        place_sources(image_own.at[step], 0, DEPTH, peer, step)

    greeted = [flag.astype(jnp.int32) for flag in (has_up, has_down, below_cross, above_cross)]
    pl.semaphore_wait(barrier, 1 + len(near_peers) + len(wide_peers) + sum(greeted))

    def halo_up(step):
        return [
            remote(mirror.at[step, pl.ds(0, 6), pl.ds(7, 1)], low_a.at[step, :, pl.ds(1, 1)],
                   halo_send.at[step, 0, 0], halo_recv.at[step, 0, 0], up),
            remote(mirror.at[step, pl.ds(VZ, 1), pl.ds(6, 1)], low_a.at[step, pl.ds(VZ, 1), pl.ds(0, 1)],
                   halo_send.at[step, 0, 2], halo_recv.at[step, 0, 2], up),
            remote(mirror.at[step, pl.ds(6, 3), pl.ds(5, 3)], low_b.at[step],
                   halo_send.at[step, 0, 1], halo_recv.at[step, 0, 1], up),
        ]

    def halo_down(step):
        return [
            remote(mirror.at[step, pl.ds(0, 6), pl.ds(0, 2)], high_a.at[step],
                   halo_send.at[step, 1, 0], halo_recv.at[step, 1, 0], down),
            remote(mirror.at[step, pl.ds(6, 3), pl.ds(0, 3)], high_b.at[step],
                   halo_send.at[step, 1, 1], halo_recv.at[step, 1, 1], down),
        ]

    def mat_copy(kind, side, device):
        layers = pl.ds(0, BUO) if kind == 0 else pl.ds(BUO, 2 * MOD)
        return remote(mat_out.at[side, layers], mat_in.at[side, layers],
                      mat_send.at[kind, side], mat_recv.at[kind, side], device)

    def each(flag, copies, act):
        @pl.when(flag)
        def _():
            for copy in copies():
                act(copy)

    begin, sent = (lambda copy: copy.start()), (lambda copy: copy.wait_send())

    def send_mats(kind):
        each(has_up, lambda: [mat_copy(kind, 0, up)], begin)
        each(has_down, lambda: [mat_copy(kind, 1, down)], begin)

    def take_mats(kind):
        for side, flag, device in ((0, has_down, up), (1, has_up, down)):
            @pl.when(flag)
            def _(side=side, device=device):
                mat_copy(kind, side, device).wait_recv()
                for at, target, lead in mat_layers[:1] if kind == 0 else mat_layers[1:]:
                    for z in range(lead):
                        target[z + (lead + DEPTH if side else 0)] = mat_in[side, at + z].astype(F32)

    def send_halos(step):
        @pl.when(has_up)
        def _():
            for copy in halo_up(step):
                copy.start()

        @pl.when(has_down)
        def _():
            for copy in halo_down(step):
                copy.start()

    send_mats(0)
    send_halos(0)

    band = extra[0] if MATMUL_X else None
    if MATMUL_X:
        row = lax.broadcasted_iota(jnp.int32, (2 * COLS, COLS), 0)
        offset = lax.rem(row, COLS) - lanes((2 * COLS, COLS))
        for k, sign in ((0, -1), (1, 1)):
            weight = jnp.where(offset == 0, -27.0 * sign, 0.0)
            weight = jnp.where(offset == sign, 27.0 * sign, weight)
            weight = jnp.where(offset == -sign, 1.0 * sign, weight)
            weight = jnp.where(offset == 2 * sign, -1.0 * sign, weight)
            band[k] = weight.astype(BF16)

    row_parts = list(zip(ROW_CUTS[:-1], ROW_CUTS[1:]))

    def across(index):
        if index == 0:
            layer, count, lo, hi = 3, 2, 0, ROWS
        else:
            lo, hi = row_parts[(index - 1) // 2]
            layer, count = (0, 3) if index % 2 else (5, 3)
        return remote(
            mirror.at[1, :, pl.ds(layer, count), pl.ds(lo, hi - lo)],
            got.at[:, pl.ds(FAR + layer, count), pl.ds(lo, hi - lo)],
            x_send.at[index], x_recv.at[index], partner,
        )

    across_count = 1 + 2 * len(row_parts)

    def forward(index, source, lead, upward, device):
        side, base = (0, 0) if upward else (1, FAR + DEPTH)
        if index == 0:
            return [
                remote(source.at[:, pl.ds(lead + 3, 2)], got.at[:, pl.ds(base + (1 if upward else 3), 2)],
                       fwd_send.at[0, side, 0], fwd_recv.at[0, side, 0], device)
            ]
        lo, hi = row_parts[index - 1]
        rows, deep = pl.ds(lo, hi - lo), pl.ds(6, 3)
        first, single = (5, 2) if upward else (0, 5)
        return [
            remote(source.at[:, pl.ds(lead + first, 3), rows],
                   got.at[:, pl.ds(base + (3 if upward else 0), 3), rows],
                   fwd_send.at[index, side, 0], fwd_recv.at[index, side, 0], device),
            remote(source.at[deep, pl.ds(lead + single, 1), rows],
                   got.at[deep, pl.ds(base + (0 if upward else 5), 1), rows],
                   fwd_send.at[index, side, 1], fwd_recv.at[index, side, 1], device),
        ]

    def forward_up(index):
        return forward(index, got, FAR, True, up)

    def forward_down(index):
        return forward(index, got, FAR, False, down)

    def straight_up(index):
        return forward(index, mirror.at[1], 0, True, cross_up)

    def straight_down(index):
        return forward(index, mirror.at[1], 0, False, cross_down)

    held = (me == half - 2) | (me == half + 1)
    passes_up = has_up & jnp.logical_not(below_cross)
    passes_down = has_down & jnp.logical_not(above_cross)

    def pass_on(index):
        if index == 0:
            across(0).wait_recv()
        else:
            across(2 * index - 1).wait_recv()
            across(2 * index).wait_recv()
        each(passes_up, lambda: forward_up(index), begin)
        each(passes_down, lambda: forward_down(index), begin)

    def send_across(index):
        if index == 0:
            across(0).start()
        else:
            across(2 * index - 1).start()
            across(2 * index).start()
        each(below_cross, lambda: straight_up(index), begin)
        each(above_cross, lambda: straight_down(index), begin)

    def send_rest():
        for index in range(2, len(row_parts) + 1):
            send_across(index)

    def prepare():
        spread = (
            lax.broadcasted_iota(jnp.int32, (COLS // BLOCK, COLS), 0)
            == lanes((COLS // BLOCK, COLS)) // BLOCK
        ).astype(F32)
        exp_rows[...] = jnp.dot(
            exps[...].astype(F32), spread, preferred_element_type=F32, precision=lax.Precision.HIGHEST
        )

        @pl.loop(0, 9 * ROWS // BLOCK)
        def _(i):
            level = jnp.broadcast_to(exp_rows[pl.ds(i, 1), :], (BLOCK, COLS))
            upscale = jnp.ones((BLOCK, COLS), F32)
            downscale = upscale
            for exponent in (-2, -1, 1, 2):
                chosen = jnp.abs(level - exponent) < 0.5
                upscale = jnp.where(chosen, 2.0**exponent, upscale)
                downscale = jnp.where(chosen, 2.0**-exponent, downscale)
            up_rows[pl.ds(pl.multiple_of(i * BLOCK, BLOCK), BLOCK), :] = upscale
            down_rows[pl.ds(pl.multiple_of(i * BLOCK, BLOCK), BLOCK), :] = downscale

        @pl.loop(0, 9)
        def _(part):
            for z in range(DEPTH + 2 * FAR):
                other[part, z, pl.ds(0, PAD), :] = zero
                other[part, z, pl.ds(PAD + ROWS, PAD), :] = zero
        place_sources(image_far.at[pl.ds(0, DEPTH + 2 * MOD)], -MOD, DEPTH + 2 * MOD, 1 - peer, 1)
        place_sources(image_far.at[pl.ds(DEPTH + 2 * MOD, DEPTH)], 0, DEPTH, 1 - peer, 2)

    mine = Slab(own, OWN, buo, lame, shear, band).rows((0, ROWS))

    def copy_rounded(step, zs):
        @pl.loop(0, 9)
        def _(part):
            for z in zs:
                mirror[step + 1, part, z] = mine.at(part, z).astype(BF16)

    def tally(step):
        def body(k, carry):
            part = k // (DEPTH // 2)
            down_scale = down_rows[pl.ds(pl.multiple_of(part * ROWS, ROWS), ROWS), :]
            up_scale = up_rows[pl.ds(pl.multiple_of(part * ROWS, ROWS), ROWS), :]
            sizes, misfits, squares = carry
            for side in range(2):
                z = lax.rem(k, DEPTH // 2) * 2 + side
                value = mine.at(part, z)
                rounded = mirror[step + 1, part, z].astype(F32)
                level = jnp.clip(rounded * down_scale, -clip_level, clip_level)
                misfit = value - level * up_scale
                for y in range(0, ROWS, YB):
                    at = slice(y, y + YB)
                    sizes = sizes + jnp.abs(level[at])
                    misfits = misfits + misfit[at] * misfit[at]
                    squares = squares + value[at] * value[at]
            return sizes, misfits, squares

        zeros = jnp.zeros((YB, COLS), F32)
        for k, total in enumerate(lax.fori_loop(0, 9 * (DEPTH // 2), body, (zeros,) * 3)):
            sums[step, k] = total

    edges = lambda first, gap: (lambda i: first + i + (i // 3) * gap)

    theirs = Slab(other, FAR, buo, lame, shear, band)

    def widen(rows):
        lo, hi = rows

        def move(part, z):
            other[part, z, pl.ds(PAD + lo, hi - lo), :] = got[part, z, pl.ds(lo, hi - lo), :].astype(F32)

        @pl.loop(0, 9)
        def _(part):
            for z in range(1, DEPTH + 2 * FAR - 1):
                move(part, z)

        for part in range(6, 9):
            for z in (0, DEPTH + 2 * FAR - 1):
                move(part, z)

    def compress(step, rows):
        lo, hi = rows

        @pl.loop(0, 9)
        def _(part):
            for y in range(lo // YB * YB, hi, YB):
                row = lax.broadcasted_iota(jnp.int32, (YB, COLS), 0) + y
                down = down_rows[pl.ds(pl.multiple_of(part * ROWS + y, YB), YB), :]
                for z in range(DEPTH):
                    value = other[part, z + FAR, pl.ds(PAD + y, YB), :]
                    level = jnp.clip(value * down, -clip_level, clip_level)
                    if lo > y or hi < y + YB:
                        before = packed[step, part, z, pl.ds(y, YB), :].astype(F32)
                        level = jnp.where((row >= lo) & (row < hi), level, before)
                    packed[step, part, z, pl.ds(y, YB), :] = level.astype(BF16)

    def payload_copy(step, index, rows):
        lo, hi = (bound // YB * YB for bound in rows)
        if lo == hi:
            return []
        return [
            pltpu.make_async_copy(
                packed.at[step, :, :, pl.ds(lo, hi - lo)],
                stored_hbm.at[0, step, :, :, pl.ds(lo, hi - lo)],
                out_sem.at[1 + step * len(row_parts) + index],
            )
        ]

    def store_payload(step, index, rows):
        for copy in payload_copy(step, index, rows):
            copy.start()

    last = len(row_parts) - 1

    def ends_of(index):
        if index < 0:
            return [0] * 4
        return [ROWS if index == last else row_parts[index][1] - 2 * (k + 1) for k in range(4)]

    def recompute(index):
        lo, hi = row_parts[index]

        @pl.when(has_down)
        def _():
            for copy in (forward_up(0) if index == 0 else []) + forward_up(index + 1):
                copy.wait_recv()

        @pl.when(has_up)
        def _():
            for copy in (forward_down(0) if index == 0 else []) + forward_down(index + 1):
                copy.wait_recv()

        if index == 0:
            take_mats(1)
        widen((lo, hi))
        compress(0, (lo, hi))
        store_payload(0, index, (lo, hi))
        span = list(zip(ends_of(index - 1), ends_of(index)))
        wide_group = GROUP * (1 if hi - lo > 32 else 2)
        theirs.rows(span[0])
        over(17, lambda i: i - 4, wide_group, theirs.velocity)
        theirs.rows(span[1])
        image = lambda z, y, n: image_far[z + MOD, pl.ds(y, n), :]
        over(14, lambda i: i - 3, wide_group, lambda zs: theirs.stress(zs, image))
        compress(1, span[1])
        store_payload(1, index, span[1])
        theirs.rows(span[2])
        over(11, lambda i: i - 1, wide_group, theirs.velocity)
        theirs.rows(span[3])
        image = lambda z, y, n: image_far[z + DEPTH + 2 * MOD, pl.ds(y, n), :]
        over(DEPTH, lambda i: i, wide_group, lambda zs: theirs.stress(zs, image))
        compress(2, span[3])
        store_payload(2, index, span[3])

    @pl.loop(0, STEPS)
    def _(step):
        @pl.when(step == 2)
        def _():
            pass_on(0)

        def image(z, y, n):
            return image_own[step, z, pl.ds(y, n), :]

        over(5, lambda i: i + 2, GROUP, mine.velocity)
        middle = (2, lambda i: i + 3)
        over(*middle, GROUP, lambda zs: mine.stress(zs, image))
        copy_rounded(step, (3, 4))

        @pl.when(step == 0)
        def _():
            send_across(0)
            prepare()
            take_mats(0)

        @pl.when(step == 2)
        def _():
            pass_on(1)

        @pl.when(has_down)
        def _():
            for copy in halo_up(step):
                copy.wait_recv()

            @pl.loop(0, 6)
            def _(part):
                own[part, OWN - 1, inner, :] = low_a[step, part, 1].astype(F32)

            own[VZ, OWN - 2, inner, :] = low_a[step, VZ, 0].astype(F32)

            @pl.loop(0, 3)
            def _(part):
                for z in range(3):
                    own[part + 6, OWN - 3 + z, inner, :] = low_b[step, part, z].astype(F32)

        @pl.when(has_up)
        def _():
            for copy in halo_down(step):
                copy.wait_recv()

            @pl.loop(0, 6)
            def _(part):
                for z in range(2):
                    own[part, OWN + DEPTH + z, inner, :] = high_a[step, part, z].astype(F32)

            @pl.loop(0, 3)
            def _(part):
                for z in range(3):
                    own[part + 6, OWN + DEPTH + z, inner, :] = high_b[step, part, z].astype(F32)

        @pl.when((step == 2) & held)
        def _():
            send_rest()

        over(6, edges(-1, 5), GROUP, mine.velocity)
        outer = (6, edges(0, 2))
        over(*outer, GROUP, lambda zs: mine.stress(zs, image))
        copy_rounded(step, (0, 1, 2, 5, 6, 7))

        @pl.when(step < STEPS - 1)
        def _():
            send_halos(step + 1)

        @pl.when(step == 0)
        def _():
            send_mats(1)
            send_across(1)

        @pl.when((step == 1) & jnp.logical_not(held))
        def _():
            send_rest()

        tally(step)

    store_final = pltpu.make_async_copy(
        own.at[:, pl.ds(OWN, DEPTH), inner, :], final_hbm.at[0], out_sem.at[0]
    )
    store_final.start()

    row8 = lax.broadcasted_iota(jnp.int32, (8, COLS), 0)
    lane8 = lanes((8, COLS))
    tile = jnp.zeros((8, COLS), F32)
    for step in range(STEPS):
        for k in range(3):
            tile = tile + jnp.where((row8 == k) & (lane8 == step), jnp.sum(sums[step, k]), 0.0)

    def spread_sums(phase, peers, mine_at, tile):
        stat_src[phase] = tile
        stat_rx[phase, mine_at] = tile
        copies = [
            remote(stat_src.at[phase], stat_rx.at[phase, mine_at],
                   stat_send.at[phase, k], stat_recv.at[phase, k], device)
            for k, device in enumerate(peers)
        ]
        for copy in copies:
            copy.start()
        return copies

    def collect_sums(phase, copies, size):
        for copy in copies:
            copy.wait()
        total = stat_rx[phase, 0]
        for k in range(1, size):
            total = total + stat_rx[phase, k]
        return total

    sum_copies = spread_sums(0, near_peers, lane_of, tile)

    for index in range(len(row_parts)):
        if index < last:
            pass_on(index + 2)
        else:
            tile = collect_sums(0, sum_copies, LOW)
            sum_copies = spread_sums(1, wide_peers, block, tile)
        recompute(index)

    tile = collect_sums(1, sum_copies, groups)
    scaled = tile * (1.0 / (9 * slabs * DEPTH * ROWS * COLS))
    ratio = scaled[1:2] / (scaled[2:3] + energy_floor)
    stats_out[0:1, :] = scaled[0:1, :STEPS]
    stats_out[1:2, :] = jnp.sqrt(ratio)[:, :STEPS]

    for index in range(across_count):
        across(index).wait_send()

    @pl.when(has_up)
    def _():
        for kind in range(2):
            mat_copy(kind, 0, up).wait_send()
        for step in range(STEPS):
            for copy in halo_up(step):
                copy.wait_send()

    @pl.when(has_down)
    def _():
        for kind in range(2):
            mat_copy(kind, 1, down).wait_send()
        for step in range(STEPS):
            for copy in halo_down(step):
                copy.wait_send()

    for index in range(len(row_parts) + 1):
        each(passes_up, lambda: forward_up(index), sent)
        each(passes_down, lambda: forward_down(index), sent)
        each(below_cross, lambda: straight_up(index), sent)
        each(above_cross, lambda: straight_down(index), sent)

    store_final.wait()
    for index, part_rows in enumerate(row_parts):
        span = list(zip(ends_of(index - 1), ends_of(index)))
        for step, rows in enumerate((part_rows, span[1], span[3])):
            for copy in payload_copy(step, index, rows):
                copy.wait()


def per_device(slabs, wavefield, buoyancy, lame_lambda, shear_modulus, scale_exponents, source_cells, wavelet):
    hbm = pl.BlockSpec(memory_space=pl.ANY)
    vmem = pl.BlockSpec(memory_space=pltpu.VMEM)
    smem = pl.BlockSpec(memory_space=pltpu.SMEM)
    parts = len(ROW_CUTS) - 1
    dma = pltpu.SemaphoreType.DMA
    final, stored, statistics = pl.pallas_call(
        functools.partial(kernel, slabs),
        out_shape=(
            jax.ShapeDtypeStruct(wavefield.shape, F32),
            jax.ShapeDtypeStruct((1, STEPS, 9, DEPTH, ROWS, COLS), BF16),
            jax.ShapeDtypeStruct((2, STEPS), F32),
        ),
        in_specs=[hbm, hbm, hbm, hbm, vmem, smem, smem],
        out_specs=(hbm, hbm, vmem),
        scratch_shapes=[
            pltpu.VMEM((9, DEPTH + 2 * OWN, ROWS + 2 * PAD, COLS), F32),
            pltpu.VMEM((9, DEPTH + 2 * FAR, ROWS + 2 * PAD, COLS), F32),
            pltpu.VMEM((STEPS + 1, 9, DEPTH, ROWS, COLS), BF16),
            pltpu.VMEM((STEPS, 6, 2, ROWS, COLS), BF16),
            pltpu.VMEM((STEPS, 3, 3, ROWS, COLS), BF16),
            pltpu.VMEM((STEPS, 6, 2, ROWS, COLS), BF16),
            pltpu.VMEM((STEPS, 3, 3, ROWS, COLS), BF16),
            pltpu.VMEM((DEPTH + 2 * BUO, ROWS, COLS), F32),
            pltpu.VMEM((DEPTH + 2 * MOD, ROWS, COLS), F32),
            pltpu.VMEM((DEPTH + 2 * MOD, ROWS, COLS), F32),
            pltpu.VMEM((2, BUO + 2 * MOD, ROWS, COLS), BF16),
            pltpu.VMEM((2, BUO + 2 * MOD, ROWS, COLS), BF16),
            pltpu.VMEM((9, DEPTH + 2 * FAR, ROWS, COLS), BF16),
            pltpu.VMEM((STEPS, 9, DEPTH, ROWS, COLS), BF16),
            pltpu.VMEM((9 * ROWS, COLS), F32),
            pltpu.VMEM((9 * ROWS, COLS), F32),
            pltpu.VMEM((9 * ROWS // BLOCK, COLS), F32),
            pltpu.VMEM((STEPS, 3, YB, COLS), F32),
            pltpu.VMEM((2, 8, COLS), F32),
            pltpu.VMEM((2, max(LOW, slabs // LOW), 8, COLS), F32),
            pltpu.VMEM((STEPS, DEPTH, ROWS, COLS), F32),
            pltpu.VMEM((2 * DEPTH + 2 * MOD, ROWS, COLS), F32),
            dma((12,)),
            dma((1 + STEPS * parts,)),
            dma((STEPS, 2, 3)),
            dma((STEPS, 2, 3)),
            dma((2, 2)),
            dma((2, 2)),
            dma((1 + 2 * parts,)),
            dma((1 + 2 * parts,)),
            dma((1 + parts, 2, 2)),
            dma((1 + parts, 2, 2)),
            dma((2, max(LOW, slabs // LOW))),
            dma((2, max(LOW, slabs // LOW))),
        ]
        + ([pltpu.VMEM((2, 2 * COLS, COLS), BF16)] if MATMUL_X else []),
        compiler_params=pltpu.CompilerParams(
            collective_id=0, has_side_effects=True, vmem_limit_bytes=60 * 1024 * 1024
        ),
        name="elastic_steps",
    )(
        wavefield, buoyancy, lame_lambda, shear_modulus,
        scale_exponents.reshape(9 * ROWS // BLOCK, COLS // BLOCK), source_cells,
        wavelet.transpose(1, 0, 2),
    )
    return final, stored, statistics.T[None]


def solution(mesh):
    return jax.shard_map(
        functools.partial(per_device, mesh.shape["space"]),
        mesh=mesh,
        in_specs=(
            P("peer", None, "space", None, None),
            P("space", None, None),
            P("space", None, None),
            P("space", None, None),
            P(None, "space", None, None),
            P(),
            P(),
        ),
        out_specs=(
            P("peer", None, "space", None, None),
            P("peer", None, None, "space", None, None),
            P("peer", None, None),
        ),
        check_vma=False,
    )
```

```python
import functools

import jax
import jax.numpy as jnp
from jax import lax
from jax.experimental import pallas as pl
from jax.experimental.pallas import tpu as pltpu
from jax.sharding import PartitionSpec as P

MESH = pl.DeviceIdType.MESH
F32 = jnp.float32
BF16 = jnp.bfloat16

BLOCK = 8
STEPS = 3
SOURCES = 8
DEPTH, ROWS, COLS = 8, 64, 128
PAD = 8
YB = 16
GROUP = 2
MATMUL_X = False
OWN = 3
FAR = 6
BUO, MOD = 5, 3
LOW = 8
ROW_CUTS = (0, 32, 48, 64)
VX, VY, VZ, SXX, SYY, SXY, SZZ, SXZ, SYZ = range(9)
clip_level = 4.0
energy_floor = 1e-06


def lanes(shape):
    return lax.broadcasted_iota(jnp.int32, shape, 1)


class Slab:
    def __init__(self, ref, lead, buoyancy, lame, shear, band):
        self.ref, self.lead = ref, lead
        self.buoyancy, self.lame, self.shear, self.band = buoyancy, lame, shear, band

    def rows(self, rows):
        self.lo, self.hi = rows
        self.y = self.lo // BLOCK * BLOCK
        self.n = -(-self.hi // BLOCK) * BLOCK - self.y
        return self

    def at(self, part, z):
        return self.ref[part, z + self.lead, pl.ds(self.y + PAD, self.n), :]

    def put(self, part, z, value):
        ref, n = self.ref, self.n
        head = BLOCK if self.lo % BLOCK else 0
        tail = BLOCK if self.hi % BLOCK else 0
        row = lax.broadcasted_iota(jnp.int32, (BLOCK, COLS), 0)
        if head:
            at = pl.ds(self.y + PAD, BLOCK)
            keep = row >= self.lo % BLOCK
            if n == BLOCK and tail:
                keep = keep & (row < self.hi % BLOCK)
                tail = 0
            ref[part, z + self.lead, at, :] = jnp.where(keep, value[:BLOCK], ref[part, z + self.lead, at, :])
        if tail:
            at = pl.ds(self.y + PAD + n - BLOCK, BLOCK)
            keep = row < self.hi % BLOCK
            ref[part, z + self.lead, at, :] = jnp.where(
                keep, value[n - BLOCK :], ref[part, z + self.lead, at, :]
            )
        if n - head - tail:
            ref[part, z + self.lead, pl.ds(self.y + PAD + head, n - head - tail), :] = value[head : n - tail]


    def dx(self, part, z, forward):
        f = self.at(part, z)
        if self.band is not None:
            top = f.astype(BF16)
            rest = (f - top.astype(F32)).astype(BF16)
            return jnp.dot(
                jnp.concatenate([top, rest], axis=1), self.band[int(forward)], preferred_element_type=F32
            )
        lane = lanes((1, COLS))
        after = jnp.where(lane < COLS - 1, pltpu.roll(f, COLS - 1, 1), 0.0)
        before = jnp.where(lane >= 1, pltpu.roll(f, 1, 1), 0.0)
        if forward:
            far = jnp.where(lane < COLS - 2, pltpu.roll(f, COLS - 2, 1), 0.0)
            return 27.0 * (after - f) - (far - before)
        far = jnp.where(lane >= 2, pltpu.roll(f, 2, 1), 0.0)
        return 27.0 * (f - before) - (after - far)

    def dy(self, part, z, forward):
        get = lambda shift: self.ref[part, z + self.lead, pl.ds(self.y + PAD + shift, self.n), :]
        if forward:
            return get(1) - get(0), get(2) - get(-1)
        return get(0) - get(-1), get(1) - get(-2)

    def dz(self, part, z, forward):
        get = lambda shift: self.at(part, z + shift)
        if forward:
            return get(1) - get(0), get(2) - get(-1)
        return get(0) - get(-1), get(1) - get(-2)

    def mat(self, table, lead, z, factor):
        return table[z + lead, pl.ds(self.y, self.n), :] * factor

    def velocity(self, zs):
        results = []
        for z in zs:
            for part, along_x, along_y, along_z, at in (
                (VX, (SXX, True), (SXY, False), (SXZ, False), z),
                (VY, (SXY, False), (SYY, True), (SYZ, False), z),
                (VZ, (SXZ, False), (SYZ, False), (SZZ, True), z - 1),
            ):
                x = self.dx(along_x[0], at, along_x[1])
                y = self.dy(along_y[0], at, along_y[1])
                d = self.dz(along_z[0], at, along_z[1])
                change = 27.0 * (y[0] + d[0]) - (y[1] + d[1]) + x
                value = self.at(part, at) + self.mat(self.buoyancy, BUO, at, 1.0 / 24.0) * change
                results.append((part, at, value))
        for part, at, value in results:
            self.put(part, at, value)

    def stress(self, zs, image, plane_shear=True):
        results = []
        for z in zs:
            join = lambda pair: 27.0 * pair[0] - pair[1]
            strain = (
                self.dx(VX, z, False), join(self.dy(VY, z, False)), join(self.dz(VZ, z, False)),
            )
            shear = self.mat(self.shear, MOD, z, 1.0 / 24.0)
            pressure = self.mat(self.lame, MOD, z, 1.0 / 24.0) * (
                strain[0] + strain[1] + strain[2]
            ) + image(z, self.y, self.n)
            double = shear + shear
            for part, value in zip((SXX, SYY, SZZ), strain):
                results.append((part, z, self.at(part, z) + (pressure + double * value)))
            if plane_shear:
                change = join(self.dy(VX, z, True)) + self.dx(VY, z, True)
                results.append((SXY, z, self.at(SXY, z) + shear * change))
            change = join(self.dz(VX, z, True)) + self.dx(VZ, z, True)
            results.append((SXZ, z, self.at(SXZ, z) + shear * change))
            y, d = self.dy(VZ, z, True), self.dz(VY, z, True)
            change = 27.0 * (y[0] + d[0]) - (y[1] + d[1])
            results.append((SYZ, z, self.at(SYZ, z) + shear * change))
        for part, at, value in results:
            self.put(part, at, value)


def over(count, place, group, body):
    @pl.loop(0, count // group)
    def _(i):
        body([place(i * group + k) for k in range(group)])

    if count % group:
        body([place(i) for i in range(count // group * group, count)])


def kernel(
    slabs,
    wave_hbm, buo_hbm, lame_hbm, shear_hbm, exps, cells, wavelet,
    own, packed, stats_out,
    other, mirror, low_a, low_b, high_a, high_b, buo, lame, shear, mat_out, mat_in, got,
    up_rows, down_rows, exp_rows, sums, stat_src, stat_rx, image_own, image_far,
    in_sem, halo_send, halo_recv, mat_send, mat_recv,
    x_send, x_recv, fwd_send, fwd_recv, stat_send, stat_recv, *extra,
):
    me, peer = lax.axis_index("space"), lax.axis_index("peer")
    has_down, has_up = me > 0, me < slabs - 1
    up, down = (me + 1, peer), (me - 1, peer)
    partner = (me, 1 - peer)
    half = slabs // 2
    below_cross, above_cross = me == half - 1, me == half
    cross_up, cross_down = (me + 1, 1 - peer), (me - 1, 1 - peer)
    groups = slabs // LOW
    block, lane_of = me // LOW, lax.rem(me, LOW)
    near_peers = [(block * LOW + lax.rem(lane_of + k, LOW), peer) for k in range(1, LOW)]
    wide_peers = [(lax.rem(block + k, groups) * LOW + lane_of, peer) for k in range(1, groups)]

    barrier = pltpu.get_barrier_semaphore()
    for device in [partner] + near_peers + wide_peers:
        pl.semaphore_signal(barrier, inc=1, device_id=device, device_id_type=MESH)

    @pl.when(has_up)
    def _():
        pl.semaphore_signal(barrier, inc=1, device_id=up, device_id_type=MESH)

    @pl.when(has_down)
    def _():
        pl.semaphore_signal(barrier, inc=1, device_id=down, device_id_type=MESH)

    @pl.when(below_cross)
    def _():
        pl.semaphore_signal(barrier, inc=1, device_id=cross_up, device_id_type=MESH)

    @pl.when(above_cross)
    def _():
        pl.semaphore_signal(barrier, inc=1, device_id=cross_down, device_id_type=MESH)

    def remote(source, target, send, recv, device):
        return pltpu.make_async_remote_copy(
            src_ref=source, dst_ref=target, send_sem=send, recv_sem=recv,
            device_id=device, device_id_type=MESH,
        )

    inner = pl.ds(PAD, ROWS)
    loads = [
        pltpu.make_async_copy(
            wave_hbm.at[0, part], own.at[part, pl.ds(OWN, DEPTH), inner, :], in_sem.at[part]
        )
        for part in range(9)
    ]
    tables = ((buo_hbm, buo, BUO), (lame_hbm, lame, MOD), (shear_hbm, shear, MOD))
    mat_loads = [
        pltpu.make_async_copy(source, target.at[pl.ds(lead, DEPTH)], in_sem.at[9 + k])
        for k, (source, target, lead) in enumerate(tables)
    ]
    for copy in loads + mat_loads:
        copy.start()

    zero = jnp.zeros((PAD, COLS), F32)
    plane = jnp.zeros((ROWS, COLS), F32)

    @pl.loop(0, 9)
    def _(part):
        for z in range(DEPTH + 2 * OWN):
            own[part, z, pl.ds(0, PAD), :] = zero
            own[part, z, pl.ds(PAD + ROWS, PAD), :] = zero
        for z in list(range(OWN)) + list(range(OWN + DEPTH, DEPTH + 2 * OWN)):
            own[part, z, inner, :] = plane

    def clear(base_mat, base_own):
        for _, target, lead in tables:
            for z in range(lead):
                target[z + (lead + DEPTH if base_mat else 0)] = plane

        @pl.loop(0, 9)
        def _(part):
            for z in range(FAR):
                got[part, z + base_own] = jnp.zeros((ROWS, COLS), BF16)

    @pl.when(jnp.logical_not(has_down))
    def _():
        clear(0, 0)

    @pl.when(jnp.logical_not(has_up))
    def _():
        clear(1, FAR + DEPTH)

    for copy in loads:
        copy.wait()

    @pl.loop(0, 9)
    def _(part):
        for z in (0, 1, 2, 5, 6, 7):
            mirror[0, part, z] = own[part, z + OWN, inner, :].astype(BF16)

    mat_layers = ((0, buo, BUO), (BUO, lame, MOD), (BUO + MOD, shear, MOD))
    for copy in mat_loads:
        copy.wait()
    for at, target, lead in mat_layers:
        for z in range(lead):
            mat_out[0, at + z] = target[DEPTH + z].astype(BF16)
            mat_out[1, at + z] = target[lead + z].astype(BF16)

    def place_sources(target, first_z, count, shot, step):
        place = lax.broadcasted_iota(jnp.int32, (ROWS, COLS), 0) * COLS + lanes((ROWS, COLS))

        @pl.loop(0, count)
        def _(i):
            first = (me * DEPTH + first_z + i) * ROWS * COLS
            total = jnp.zeros((ROWS, COLS), F32)
            for j in range(SOURCES):
                total = total + jnp.where(place == cells[shot, j] - first, wavelet[step, shot, j], 0.0)
            target[i] = total

    for step in range(STEPS):
        place_sources(image_own.at[step], 0, DEPTH, peer, step)

    greeted = [flag.astype(jnp.int32) for flag in (has_up, has_down, below_cross, above_cross)]
    pl.semaphore_wait(barrier, 1 + len(near_peers) + len(wide_peers) + sum(greeted))

    def halo_up(step):
        return [
            remote(mirror.at[step, pl.ds(0, 6), pl.ds(7, 1)], low_a.at[step, :, pl.ds(1, 1)],
                   halo_send.at[step, 0, 0], halo_recv.at[step, 0, 0], up),
            remote(mirror.at[step, pl.ds(VZ, 1), pl.ds(6, 1)], low_a.at[step, pl.ds(VZ, 1), pl.ds(0, 1)],
                   halo_send.at[step, 0, 2], halo_recv.at[step, 0, 2], up),
            remote(mirror.at[step, pl.ds(6, 3), pl.ds(5, 3)], low_b.at[step],
                   halo_send.at[step, 0, 1], halo_recv.at[step, 0, 1], up),
        ]

    def halo_down(step):
        return [
            remote(mirror.at[step, pl.ds(0, 6), pl.ds(0, 2)], high_a.at[step],
                   halo_send.at[step, 1, 0], halo_recv.at[step, 1, 0], down),
            remote(mirror.at[step, pl.ds(6, 3), pl.ds(0, 3)], high_b.at[step],
                   halo_send.at[step, 1, 1], halo_recv.at[step, 1, 1], down),
        ]

    def mat_copy(kind, side, device):
        layers = pl.ds(0, BUO) if kind == 0 else pl.ds(BUO, 2 * MOD)
        return remote(mat_out.at[side, layers], mat_in.at[side, layers],
                      mat_send.at[kind, side], mat_recv.at[kind, side], device)

    def each(flag, copies, act):
        @pl.when(flag)
        def _():
            for copy in copies():
                act(copy)

    begin, sent = (lambda copy: copy.start()), (lambda copy: copy.wait_send())

    def send_mats(kind):
        each(has_up, lambda: [mat_copy(kind, 0, up)], begin)
        each(has_down, lambda: [mat_copy(kind, 1, down)], begin)

    def take_mats(kind):
        for side, flag, device in ((0, has_down, up), (1, has_up, down)):
            @pl.when(flag)
            def _(side=side, device=device):
                mat_copy(kind, side, device).wait_recv()
                for at, target, lead in mat_layers[:1] if kind == 0 else mat_layers[1:]:
                    for z in range(lead):
                        target[z + (lead + DEPTH if side else 0)] = mat_in[side, at + z].astype(F32)

    def send_halos(step):
        @pl.when(has_up)
        def _():
            for copy in halo_up(step):
                copy.start()

        @pl.when(has_down)
        def _():
            for copy in halo_down(step):
                copy.start()

    send_mats(0)
    send_halos(0)

    band = extra[0] if MATMUL_X else None
    if MATMUL_X:
        row = lax.broadcasted_iota(jnp.int32, (2 * COLS, COLS), 0)
        offset = lax.rem(row, COLS) - lanes((2 * COLS, COLS))
        for k, sign in ((0, -1), (1, 1)):
            weight = jnp.where(offset == 0, -27.0 * sign, 0.0)
            weight = jnp.where(offset == sign, 27.0 * sign, weight)
            weight = jnp.where(offset == -sign, 1.0 * sign, weight)
            weight = jnp.where(offset == 2 * sign, -1.0 * sign, weight)
            band[k] = weight.astype(BF16)

    row_parts = list(zip(ROW_CUTS[:-1], ROW_CUTS[1:]))

    def across(index):
        if index == 0:
            layer, count, lo, hi = 3, 2, 0, ROWS
        else:
            lo, hi = row_parts[(index - 1) // 2]
            layer, count = (0, 3) if index % 2 else (5, 3)
        return remote(
            mirror.at[1, :, pl.ds(layer, count), pl.ds(lo, hi - lo)],
            got.at[:, pl.ds(FAR + layer, count), pl.ds(lo, hi - lo)],
            x_send.at[index], x_recv.at[index], partner,
        )

    across_count = 1 + 2 * len(row_parts)

    def forward(index, source, lead, upward, device):
        side, base = (0, 0) if upward else (1, FAR + DEPTH)
        if index == 0:
            return [
                remote(source.at[:, pl.ds(lead + 3, 2)], got.at[:, pl.ds(base + (1 if upward else 3), 2)],
                       fwd_send.at[0, side, 0], fwd_recv.at[0, side, 0], device)
            ]
        lo, hi = row_parts[index - 1]
        rows, deep = pl.ds(lo, hi - lo), pl.ds(6, 3)
        first, single = (5, 2) if upward else (0, 5)
        return [
            remote(source.at[:, pl.ds(lead + first, 3), rows],
                   got.at[:, pl.ds(base + (3 if upward else 0), 3), rows],
                   fwd_send.at[index, side, 0], fwd_recv.at[index, side, 0], device),
            remote(source.at[deep, pl.ds(lead + single, 1), rows],
                   got.at[deep, pl.ds(base + (0 if upward else 5), 1), rows],
                   fwd_send.at[index, side, 1], fwd_recv.at[index, side, 1], device),
        ]

    def forward_up(index):
        return forward(index, got, FAR, True, up)

    def forward_down(index):
        return forward(index, got, FAR, False, down)

    def straight_up(index):
        return forward(index, mirror.at[1], 0, True, cross_up)

    def straight_down(index):
        return forward(index, mirror.at[1], 0, False, cross_down)

    held = (me == half - 2) | (me == half + 1)
    passes_up = has_up & jnp.logical_not(below_cross)
    passes_down = has_down & jnp.logical_not(above_cross)

    def pass_on(index):
        if index == 0:
            across(0).wait_recv()
        else:
            across(2 * index - 1).wait_recv()
            across(2 * index).wait_recv()
        each(passes_up, lambda: forward_up(index), begin)
        each(passes_down, lambda: forward_down(index), begin)

    def send_across(index):
        if index == 0:
            across(0).start()
        else:
            across(2 * index - 1).start()
            across(2 * index).start()
        each(below_cross, lambda: straight_up(index), begin)
        each(above_cross, lambda: straight_down(index), begin)

    def send_rest():
        for index in range(2, len(row_parts) + 1):
            send_across(index)

    def prepare():
        spread = (
            lax.broadcasted_iota(jnp.int32, (COLS // BLOCK, COLS), 0)
            == lanes((COLS // BLOCK, COLS)) // BLOCK
        ).astype(F32)
        exp_rows[...] = jnp.dot(
            exps[...].astype(F32), spread, preferred_element_type=F32, precision=lax.Precision.HIGHEST
        )

        @pl.loop(0, 9 * ROWS // BLOCK)
        def _(i):
            level = jnp.broadcast_to(exp_rows[pl.ds(i, 1), :], (BLOCK, COLS))
            upscale = jnp.ones((BLOCK, COLS), F32)
            downscale = upscale
            for exponent in (-2, -1, 1, 2):
                chosen = jnp.abs(level - exponent) < 0.5
                upscale = jnp.where(chosen, 2.0**exponent, upscale)
                downscale = jnp.where(chosen, 2.0**-exponent, downscale)
            up_rows[pl.ds(pl.multiple_of(i * BLOCK, BLOCK), BLOCK), :] = upscale
            down_rows[pl.ds(pl.multiple_of(i * BLOCK, BLOCK), BLOCK), :] = downscale

        @pl.loop(0, 9)
        def _(part):
            for z in range(DEPTH + 2 * FAR):
                other[part, z, pl.ds(0, PAD), :] = zero
                other[part, z, pl.ds(PAD + ROWS, PAD), :] = zero
        place_sources(image_far.at[pl.ds(0, DEPTH + 2 * MOD)], -MOD, DEPTH + 2 * MOD, 1 - peer, 1)
        place_sources(image_far.at[pl.ds(DEPTH + 2 * MOD, DEPTH)], 0, DEPTH, 1 - peer, 2)

    mine = Slab(own, OWN, buo, lame, shear, band).rows((0, ROWS))

    def copy_rounded(step, zs):
        @pl.loop(0, 9)
        def _(part):
            for z in zs:
                mirror[step + 1, part, z] = mine.at(part, z).astype(BF16)

    def tally(step):
        def body(k, carry):
            part = k // (DEPTH // 2)
            down_scale = down_rows[pl.ds(pl.multiple_of(part * ROWS, ROWS), ROWS), :]
            up_scale = up_rows[pl.ds(pl.multiple_of(part * ROWS, ROWS), ROWS), :]
            sizes, misfits, squares = carry
            for side in range(2):
                z = lax.rem(k, DEPTH // 2) * 2 + side
                value = mine.at(part, z)
                rounded = mirror[step + 1, part, z].astype(F32)
                level = jnp.clip(rounded * down_scale, -clip_level, clip_level)
                misfit = value - level * up_scale
                for y in range(0, ROWS, YB):
                    at = slice(y, y + YB)
                    sizes = sizes + jnp.abs(level[at])
                    misfits = misfits + misfit[at] * misfit[at]
                    squares = squares + value[at] * value[at]
            return sizes, misfits, squares

        zeros = jnp.zeros((YB, COLS), F32)
        for k, total in enumerate(lax.fori_loop(0, 9 * (DEPTH // 2), body, (zeros,) * 3)):
            sums[step, k] = total

    edges = lambda first, gap: (lambda i: first + i + (i // 3) * gap)

    theirs = Slab(other, FAR, buo, lame, shear, band)

    def widen(rows):
        lo, hi = rows

        def move(part, z):
            other[part, z, pl.ds(PAD + lo, hi - lo), :] = got[part, z, pl.ds(lo, hi - lo), :].astype(F32)

        @pl.loop(0, 9)
        def _(part):
            for z in range(1, DEPTH + 2 * FAR - 1):
                move(part, z)

        for part in range(6, 9):
            for z in (0, DEPTH + 2 * FAR - 1):
                move(part, z)

    def compress(step, rows):
        lo, hi = rows

        @pl.loop(0, 9)
        def _(part):
            for y in range(lo // YB * YB, hi, YB):
                row = lax.broadcasted_iota(jnp.int32, (YB, COLS), 0) + y
                down = down_rows[pl.ds(pl.multiple_of(part * ROWS + y, YB), YB), :]
                for z in range(DEPTH):
                    value = other[part, z + FAR, pl.ds(PAD + y, YB), :]
                    level = jnp.clip(value * down, -clip_level, clip_level)
                    if lo > y or hi < y + YB:
                        before = packed[step, part, z, pl.ds(y, YB), :].astype(F32)
                        level = jnp.where((row >= lo) & (row < hi), level, before)
                    packed[step, part, z, pl.ds(y, YB), :] = level.astype(BF16)

    last = len(row_parts) - 1

    def ends_of(index):
        if index < 0:
            return [0] * 4
        return [ROWS if index == last else row_parts[index][1] - 2 * (k + 1) for k in range(4)]

    def recompute(index):
        lo, hi = row_parts[index]

        @pl.when(has_down)
        def _():
            for copy in (forward_up(0) if index == 0 else []) + forward_up(index + 1):
                copy.wait_recv()

        @pl.when(has_up)
        def _():
            for copy in (forward_down(0) if index == 0 else []) + forward_down(index + 1):
                copy.wait_recv()

        if index == 0:
            take_mats(1)
        widen((lo, hi))
        compress(0, (lo, hi))
        span = list(zip(ends_of(index - 1), ends_of(index)))
        wide_group = GROUP * (1 if hi - lo > 32 else 2)
        theirs.rows(span[0])
        over(17, lambda i: i - 4, wide_group, theirs.velocity)
        theirs.rows(span[1])
        image = lambda z, y, n: image_far[z + MOD, pl.ds(y, n), :]
        over(14, lambda i: i - 3, wide_group, lambda zs: theirs.stress(zs, image))
        compress(1, span[1])
        theirs.rows(span[2])
        over(11, lambda i: i - 1, wide_group, theirs.velocity)
        theirs.rows(span[3])
        image = lambda z, y, n: image_far[z + DEPTH + 2 * MOD, pl.ds(y, n), :]
        over(DEPTH, lambda i: i, wide_group, lambda zs: theirs.stress(zs, image))
        compress(2, span[3])

    @pl.loop(0, STEPS)
    def _(step):
        @pl.when(step == 2)
        def _():
            pass_on(0)

        def image(z, y, n):
            return image_own[step, z, pl.ds(y, n), :]

        over(5, lambda i: i + 2, GROUP, mine.velocity)
        middle = (2, lambda i: i + 3)
        over(*middle, GROUP, lambda zs: mine.stress(zs, image))
        copy_rounded(step, (3, 4))

        @pl.when(step == 0)
        def _():
            send_across(0)
            prepare()
            take_mats(0)

        @pl.when(step == 2)
        def _():
            pass_on(1)

        @pl.when(has_down)
        def _():
            for copy in halo_up(step):
                copy.wait_recv()

            @pl.loop(0, 6)
            def _(part):
                own[part, OWN - 1, inner, :] = low_a[step, part, 1].astype(F32)

            own[VZ, OWN - 2, inner, :] = low_a[step, VZ, 0].astype(F32)

            @pl.loop(0, 3)
            def _(part):
                for z in range(3):
                    own[part + 6, OWN - 3 + z, inner, :] = low_b[step, part, z].astype(F32)

        @pl.when(has_up)
        def _():
            for copy in halo_down(step):
                copy.wait_recv()

            @pl.loop(0, 6)
            def _(part):
                for z in range(2):
                    own[part, OWN + DEPTH + z, inner, :] = high_a[step, part, z].astype(F32)

            @pl.loop(0, 3)
            def _(part):
                for z in range(3):
                    own[part + 6, OWN + DEPTH + z, inner, :] = high_b[step, part, z].astype(F32)

        @pl.when((step == 2) & held)
        def _():
            send_rest()

        over(6, edges(-1, 5), GROUP, mine.velocity)
        outer = (6, edges(0, 2))
        over(*outer, GROUP, lambda zs: mine.stress(zs, image))
        copy_rounded(step, (0, 1, 2, 5, 6, 7))

        @pl.when(step < STEPS - 1)
        def _():
            send_halos(step + 1)

        @pl.when(step == 0)
        def _():
            send_mats(1)
            send_across(1)

        @pl.when((step == 1) & jnp.logical_not(held))
        def _():
            send_rest()

        tally(step)

    row8 = lax.broadcasted_iota(jnp.int32, (8, COLS), 0)
    lane8 = lanes((8, COLS))
    tile = jnp.zeros((8, COLS), F32)
    for step in range(STEPS):
        for k in range(3):
            tile = tile + jnp.where((row8 == k) & (lane8 == step), jnp.sum(sums[step, k]), 0.0)

    def spread_sums(phase, peers, mine_at, tile):
        stat_src[phase] = tile
        stat_rx[phase, mine_at] = tile
        copies = [
            remote(stat_src.at[phase], stat_rx.at[phase, mine_at],
                   stat_send.at[phase, k], stat_recv.at[phase, k], device)
            for k, device in enumerate(peers)
        ]
        for copy in copies:
            copy.start()
        return copies

    def collect_sums(phase, copies, size):
        for copy in copies:
            copy.wait()
        total = stat_rx[phase, 0]
        for k in range(1, size):
            total = total + stat_rx[phase, k]
        return total

    sum_copies = spread_sums(0, near_peers, lane_of, tile)

    for index in range(len(row_parts)):
        if index < last:
            pass_on(index + 2)
        else:
            tile = collect_sums(0, sum_copies, LOW)
            sum_copies = spread_sums(1, wide_peers, block, tile)
        recompute(index)

    tile = collect_sums(1, sum_copies, groups)
    scaled = tile * (1.0 / (9 * slabs * DEPTH * ROWS * COLS))
    ratio = scaled[1:2] / (scaled[2:3] + energy_floor)
    stats_out[0:1, :] = scaled[0:1, :STEPS]
    stats_out[1:2, :] = jnp.sqrt(ratio)[:, :STEPS]

    for index in range(across_count):
        across(index).wait_send()

    @pl.when(has_up)
    def _():
        for kind in range(2):
            mat_copy(kind, 0, up).wait_send()
        for step in range(STEPS):
            for copy in halo_up(step):
                copy.wait_send()

    @pl.when(has_down)
    def _():
        for kind in range(2):
            mat_copy(kind, 1, down).wait_send()
        for step in range(STEPS):
            for copy in halo_down(step):
                copy.wait_send()

    for index in range(len(row_parts) + 1):
        each(passes_up, lambda: forward_up(index), sent)
        each(passes_down, lambda: forward_down(index), sent)
        each(below_cross, lambda: straight_up(index), sent)
        each(above_cross, lambda: straight_down(index), sent)


def write_out(own, packed, sums, final_hbm, stored_hbm, stats_out, sem):
    copies = [
        pltpu.make_async_copy(packed.at[step], stored_hbm.at[0, step], sem.at[step]) for step in range(STEPS)
    ]
    copies.append(
        pltpu.make_async_copy(
            own.at[:, pl.ds(OWN, DEPTH), pl.ds(PAD, ROWS), :], final_hbm.at[0], sem.at[STEPS]
        )
    )
    for copy in copies:
        copy.start()
    stats_out[...] = sums[...]
    for copy in copies:
        copy.wait()


def per_device(slabs, wavefield, buoyancy, lame_lambda, shear_modulus, scale_exponents, source_cells, wavelet):
    hbm = pl.BlockSpec(memory_space=pl.ANY)
    vmem = pl.BlockSpec(memory_space=pltpu.VMEM)
    smem = pl.BlockSpec(memory_space=pltpu.SMEM)
    parts = len(ROW_CUTS) - 1
    dma = pltpu.SemaphoreType.DMA
    own, packed, statistics = pl.pallas_call(
        functools.partial(kernel, slabs),
        out_shape=(
            pltpu.VMEM((9, DEPTH + 2 * OWN, ROWS + 2 * PAD, COLS), F32),
            pltpu.VMEM((STEPS, 9, DEPTH, ROWS, COLS), BF16),
            pltpu.VMEM((2, STEPS), F32),
        ),
        in_specs=[hbm, hbm, hbm, hbm, vmem, smem, smem],
        out_specs=(vmem, vmem, vmem),
        scratch_shapes=[
            pltpu.VMEM((9, DEPTH + 2 * FAR, ROWS + 2 * PAD, COLS), F32),
            pltpu.VMEM((STEPS + 1, 9, DEPTH, ROWS, COLS), BF16),
            pltpu.VMEM((STEPS, 6, 2, ROWS, COLS), BF16),
            pltpu.VMEM((STEPS, 3, 3, ROWS, COLS), BF16),
            pltpu.VMEM((STEPS, 6, 2, ROWS, COLS), BF16),
            pltpu.VMEM((STEPS, 3, 3, ROWS, COLS), BF16),
            pltpu.VMEM((DEPTH + 2 * BUO, ROWS, COLS), F32),
            pltpu.VMEM((DEPTH + 2 * MOD, ROWS, COLS), F32),
            pltpu.VMEM((DEPTH + 2 * MOD, ROWS, COLS), F32),
            pltpu.VMEM((2, BUO + 2 * MOD, ROWS, COLS), BF16),
            pltpu.VMEM((2, BUO + 2 * MOD, ROWS, COLS), BF16),
            pltpu.VMEM((9, DEPTH + 2 * FAR, ROWS, COLS), BF16),
            pltpu.VMEM((9 * ROWS, COLS), F32),
            pltpu.VMEM((9 * ROWS, COLS), F32),
            pltpu.VMEM((9 * ROWS // BLOCK, COLS), F32),
            pltpu.VMEM((STEPS, 3, YB, COLS), F32),
            pltpu.VMEM((2, 8, COLS), F32),
            pltpu.VMEM((2, max(LOW, slabs // LOW), 8, COLS), F32),
            pltpu.VMEM((STEPS, DEPTH, ROWS, COLS), F32),
            pltpu.VMEM((2 * DEPTH + 2 * MOD, ROWS, COLS), F32),
            dma((12,)),
            dma((STEPS, 2, 3)),
            dma((STEPS, 2, 3)),
            dma((2, 2)),
            dma((2, 2)),
            dma((1 + 2 * parts,)),
            dma((1 + 2 * parts,)),
            dma((1 + parts, 2, 2)),
            dma((1 + parts, 2, 2)),
            dma((2, max(LOW, slabs // LOW))),
            dma((2, max(LOW, slabs // LOW))),
        ]
        + ([pltpu.VMEM((2, 2 * COLS, COLS), BF16)] if MATMUL_X else []),
        compiler_params=pltpu.CompilerParams(
            collective_id=0, has_side_effects=True, vmem_limit_bytes=55 * 1024 * 1024
        ),
        name="elastic_steps",
    )(
        wavefield, buoyancy, lame_lambda, shear_modulus,
        scale_exponents.reshape(9 * ROWS // BLOCK, COLS // BLOCK), source_cells,
        wavelet.transpose(1, 0, 2),
    )
    final, stored, statistics = pl.pallas_call(
        write_out,
        out_shape=(
            jax.ShapeDtypeStruct(wavefield.shape, F32),
            jax.ShapeDtypeStruct((1, STEPS, 9, DEPTH, ROWS, COLS), BF16),
            jax.ShapeDtypeStruct((2, STEPS), F32),
        ),
        in_specs=[vmem, vmem, vmem],
        out_specs=(hbm, hbm, vmem),
        scratch_shapes=[dma((STEPS + 1,))],
        compiler_params=pltpu.CompilerParams(vmem_limit_bytes=8 * 1024 * 1024),
        name="write_out",
    )(own, packed, statistics)
    return final, stored, statistics.T[None]


def solution(mesh):
    return jax.shard_map(
        functools.partial(per_device, mesh.shape["space"]),
        mesh=mesh,
        in_specs=(
            P("peer", None, "space", None, None),
            P("space", None, None),
            P("space", None, None),
            P("space", None, None),
            P(None, "space", None, None),
            P(),
            P(),
        ),
        out_specs=(
            P("peer", None, "space", None, None),
            P("peer", None, None, "space", None, None),
            P("peer", None, None),
        ),
        check_vma=False,
    )
```

```python
import functools

import jax
import jax.numpy as jnp
from jax import lax
from jax.experimental import pallas as pl
from jax.experimental.pallas import tpu as pltpu
from jax.sharding import PartitionSpec as P

MESH = pl.DeviceIdType.MESH
F32 = jnp.float32
BF16 = jnp.bfloat16

BLOCK = 8
STEPS = 3
SOURCES = 8
DEPTH, ROWS, COLS = 8, 64, 128
PAD = 8
YB = 16
GROUP = 2
WIDE_GROUP = 4
MATMUL_X = False
OWN = 3
FAR = 6
BUO, MOD = 5, 3
LOW = 8
ROW_CUTS = (0, 32, 48, 64)
GROUPS = ((0,), (1, 2))
VX, VY, VZ, SXX, SYY, SXY, SZZ, SXZ, SYZ = range(9)
clip_level = 4.0
energy_floor = 1e-06


def lanes(shape):
    return lax.broadcasted_iota(jnp.int32, shape, 1)


class Slab:
    def __init__(self, ref, lead, buoyancy, lame, shear, band):
        self.ref, self.lead = ref, lead
        self.buoyancy, self.lame, self.shear, self.band = buoyancy, lame, shear, band

    def rows(self, rows):
        self.lo, self.hi = rows
        self.y = self.lo // BLOCK * BLOCK
        self.n = -(-self.hi // BLOCK) * BLOCK - self.y
        return self

    def at(self, part, z):
        return self.ref[part, z + self.lead, pl.ds(self.y + PAD, self.n), :]

    def put(self, part, z, value):
        ref, n = self.ref, self.n
        head = BLOCK if self.lo % BLOCK else 0
        tail = BLOCK if self.hi % BLOCK else 0
        row = lax.broadcasted_iota(jnp.int32, (BLOCK, COLS), 0)
        if head:
            at = pl.ds(self.y + PAD, BLOCK)
            keep = row >= self.lo % BLOCK
            if n == BLOCK and tail:
                keep = keep & (row < self.hi % BLOCK)
                tail = 0
            ref[part, z + self.lead, at, :] = jnp.where(keep, value[:BLOCK], ref[part, z + self.lead, at, :])
        if tail:
            at = pl.ds(self.y + PAD + n - BLOCK, BLOCK)
            keep = row < self.hi % BLOCK
            ref[part, z + self.lead, at, :] = jnp.where(
                keep, value[n - BLOCK :], ref[part, z + self.lead, at, :]
            )
        if n - head - tail:
            ref[part, z + self.lead, pl.ds(self.y + PAD + head, n - head - tail), :] = value[head : n - tail]


    def dx(self, part, z, forward):
        f = self.at(part, z)
        if self.band is not None:
            top = f.astype(BF16)
            rest = (f - top.astype(F32)).astype(BF16)
            return jnp.dot(
                jnp.concatenate([top, rest], axis=1), self.band[int(forward)], preferred_element_type=F32
            )
        lane = lanes((1, COLS))
        after = jnp.where(lane < COLS - 1, pltpu.roll(f, COLS - 1, 1), 0.0)
        before = jnp.where(lane >= 1, pltpu.roll(f, 1, 1), 0.0)
        if forward:
            far = jnp.where(lane < COLS - 2, pltpu.roll(f, COLS - 2, 1), 0.0)
            return 27.0 * (after - f) - (far - before)
        far = jnp.where(lane >= 2, pltpu.roll(f, 2, 1), 0.0)
        return 27.0 * (f - before) - (after - far)

    def dy(self, part, z, forward):
        get = lambda shift: self.ref[part, z + self.lead, pl.ds(self.y + PAD + shift, self.n), :]
        if forward:
            return get(1) - get(0), get(2) - get(-1)
        return get(0) - get(-1), get(1) - get(-2)

    def dz(self, part, z, forward):
        get = lambda shift: self.at(part, z + shift)
        if forward:
            return get(1) - get(0), get(2) - get(-1)
        return get(0) - get(-1), get(1) - get(-2)

    def mat(self, table, lead, z, factor):
        return table[z + lead, pl.ds(self.y, self.n), :] * factor

    def velocity(self, zs):
        results = []
        for z in zs:
            for part, along_x, along_y, along_z, at in (
                (VX, (SXX, True), (SXY, False), (SXZ, False), z),
                (VY, (SXY, False), (SYY, True), (SYZ, False), z),
                (VZ, (SXZ, False), (SYZ, False), (SZZ, True), z - 1),
            ):
                x = self.dx(along_x[0], at, along_x[1])
                y = self.dy(along_y[0], at, along_y[1])
                d = self.dz(along_z[0], at, along_z[1])
                change = 27.0 * (y[0] + d[0]) - (y[1] + d[1]) + x
                value = self.at(part, at) + self.mat(self.buoyancy, BUO, at, 1.0 / 24.0) * change
                results.append((part, at, value))
        for part, at, value in results:
            self.put(part, at, value)

    def stress(self, zs, image, plane_shear=True):
        results = []
        for z in zs:
            join = lambda pair: 27.0 * pair[0] - pair[1]
            strain = (
                self.dx(VX, z, False), join(self.dy(VY, z, False)), join(self.dz(VZ, z, False)),
            )
            shear = self.mat(self.shear, MOD, z, 1.0 / 24.0)
            pressure = self.mat(self.lame, MOD, z, 1.0 / 24.0) * (
                strain[0] + strain[1] + strain[2]
            ) + image(z, self.y, self.n)
            double = shear + shear
            for part, value in zip((SXX, SYY, SZZ), strain):
                results.append((part, z, self.at(part, z) + (pressure + double * value)))
            if plane_shear:
                change = join(self.dy(VX, z, True)) + self.dx(VY, z, True)
                results.append((SXY, z, self.at(SXY, z) + shear * change))
            change = join(self.dz(VX, z, True)) + self.dx(VZ, z, True)
            results.append((SXZ, z, self.at(SXZ, z) + shear * change))
            y, d = self.dy(VZ, z, True), self.dz(VY, z, True)
            change = 27.0 * (y[0] + d[0]) - (y[1] + d[1])
            results.append((SYZ, z, self.at(SYZ, z) + shear * change))
        for part, at, value in results:
            self.put(part, at, value)


def over(count, place, group, body):
    @pl.loop(0, count // group)
    def _(i):
        body([place(i * group + k) for k in range(group)])

    if count % group:
        body([place(i) for i in range(count // group * group, count)])


def kernel(
    slabs,
    wave_hbm, buo_hbm, lame_hbm, shear_hbm, exps, cells, wavelet,
    own, packed, stats_out,
    other, mirror, low_a, low_b, high_a, high_b, buo, lame, shear, mat_out, mat_in, got,
    up_rows, down_rows, exp_rows, sums, stat_src, stat_rx, image_own, image_far, held_over,
    in_sem, halo_send, halo_recv, mat_send, mat_recv,
    x_send, x_recv, help_send, help_recv, fwd_send, fwd_recv, stat_send, stat_recv, *extra,
):
    me, peer = lax.axis_index("space"), lax.axis_index("peer")
    has_down, has_up = me > 0, me < slabs - 1
    up, down = (me + 1, peer), (me - 1, peer)
    partner = (me, 1 - peer)
    half = slabs // 2
    below_cross, above_cross = me == half - 1, me == half
    cross_up, cross_down = (me + 1, 1 - peer), (me - 1, 1 - peer)
    detours = ((half - 2, -2), (half - 1, -LOW), (half, LOW), (half + 1, 2))
    flag = lambda condition: condition.astype(jnp.int32)
    hands_over = (me >= half - 2) & (me <= half + 1)
    helper = me + sum(flag(me == slab) * offset for slab, offset in detours)
    helped = sum(flag(me == slab + offset) * slab for slab, offset in detours)
    helps = helped > 0
    groups = slabs // LOW
    block, lane_of = me // LOW, lax.rem(me, LOW)
    near_peers = [(block * LOW + lax.rem(lane_of + k, LOW), peer) for k in range(1, LOW)]
    wide_peers = [(lax.rem(block + k, groups) * LOW + lane_of, peer) for k in range(1, groups)]

    barrier = pltpu.get_barrier_semaphore()
    for device in [partner] + near_peers + wide_peers:
        pl.semaphore_signal(barrier, inc=1, device_id=device, device_id_type=MESH)

    @pl.when(has_up)
    def _():
        pl.semaphore_signal(barrier, inc=1, device_id=up, device_id_type=MESH)

    @pl.when(has_down)
    def _():
        pl.semaphore_signal(barrier, inc=1, device_id=down, device_id_type=MESH)

    @pl.when(hands_over)
    def _():
        pl.semaphore_signal(barrier, inc=1, device_id=(helper, 1 - peer), device_id_type=MESH)

    @pl.when(helps)
    def _():
        pl.semaphore_signal(barrier, inc=1, device_id=(helped, peer), device_id_type=MESH)

    @pl.when(below_cross)
    def _():
        pl.semaphore_signal(barrier, inc=1, device_id=cross_up, device_id_type=MESH)

    @pl.when(above_cross)
    def _():
        pl.semaphore_signal(barrier, inc=1, device_id=cross_down, device_id_type=MESH)

    def remote(source, target, send, recv, device):
        return pltpu.make_async_remote_copy(
            src_ref=source, dst_ref=target, send_sem=send, recv_sem=recv,
            device_id=device, device_id_type=MESH,
        )

    inner = pl.ds(PAD, ROWS)
    loads = [
        pltpu.make_async_copy(
            wave_hbm.at[0, part], own.at[part, pl.ds(OWN, DEPTH), inner, :], in_sem.at[part]
        )
        for part in range(9)
    ]
    tables = ((buo_hbm, buo, BUO), (lame_hbm, lame, MOD), (shear_hbm, shear, MOD))
    mat_loads = [
        pltpu.make_async_copy(source, target.at[pl.ds(lead, DEPTH)], in_sem.at[9 + k])
        for k, (source, target, lead) in enumerate(tables)
    ]
    for copy in loads + mat_loads:
        copy.start()

    zero = jnp.zeros((PAD, COLS), F32)
    plane = jnp.zeros((ROWS, COLS), F32)

    @pl.loop(0, 9)
    def _(part):
        for z in range(DEPTH + 2 * OWN):
            own[part, z, pl.ds(0, PAD), :] = zero
            own[part, z, pl.ds(PAD + ROWS, PAD), :] = zero
        for z in list(range(OWN)) + list(range(OWN + DEPTH, DEPTH + 2 * OWN)):
            own[part, z, inner, :] = plane

    def clear(base_mat, base_own):
        for _, target, lead in tables:
            for z in range(lead):
                target[z + (lead + DEPTH if base_mat else 0)] = plane

        @pl.loop(0, 9)
        def _(part):
            for z in range(FAR):
                got[part, z + base_own] = jnp.zeros((ROWS, COLS), BF16)

    @pl.when(jnp.logical_not(has_down))
    def _():
        clear(0, 0)

    @pl.when(jnp.logical_not(has_up))
    def _():
        clear(1, FAR + DEPTH)

    for part, copy in enumerate(loads):
        copy.wait()
        for z in (0, 1, 6, 7) if part < 6 else (0, 1, 2, 5, 6, 7):
            mirror[0, part, z] = own[part, z + OWN, inner, :].astype(BF16)

    def place_sources(target, first_z, count, shot, step):
        place = lax.broadcasted_iota(jnp.int32, (ROWS, COLS), 0) * COLS + lanes((ROWS, COLS))

        @pl.loop(0, count)
        def _(i):
            first = (me * DEPTH + first_z + i) * ROWS * COLS
            total = jnp.zeros((ROWS, COLS), F32)
            for j in range(SOURCES):
                total = total + jnp.where(place == cells[shot, j] - first, wavelet[step, shot, j], 0.0)
            target[i] = total

    mat_layers = ((0, buo, BUO), (BUO, lame, MOD), (BUO + MOD, shear, MOD))

    def round_mats(layers_of):
        for at, target, lead in layers_of:
            for z in range(lead):
                mat_out[0, at + z] = target[DEPTH + z].astype(BF16)
                mat_out[1, at + z] = target[lead + z].astype(BF16)

    for copy in mat_loads:
        copy.wait()
    round_mats(mat_layers[:1])

    greeted = [flag(yes) for yes in (has_up, has_down, below_cross, above_cross, hands_over, helps)]
    pl.semaphore_wait(barrier, 1 + len(near_peers) + len(wide_peers) + sum(greeted))

    def halo_up(step):
        return [
            remote(mirror.at[step, pl.ds(0, 6), pl.ds(7, 1)], low_a.at[step, :, pl.ds(1, 1)],
                   halo_send.at[step, 0, 0], halo_recv.at[step, 0, 0], up),
            remote(mirror.at[step, pl.ds(VZ, 1), pl.ds(6, 1)], low_a.at[step, pl.ds(VZ, 1), pl.ds(0, 1)],
                   halo_send.at[step, 0, 2], halo_recv.at[step, 0, 2], up),
            remote(mirror.at[step, pl.ds(6, 3), pl.ds(5, 3)], low_b.at[step],
                   halo_send.at[step, 0, 1], halo_recv.at[step, 0, 1], up),
        ]

    def halo_down(step):
        return [
            remote(mirror.at[step, pl.ds(0, 6), pl.ds(0, 2)], high_a.at[step],
                   halo_send.at[step, 1, 0], halo_recv.at[step, 1, 0], down),
            remote(mirror.at[step, pl.ds(6, 3), pl.ds(0, 3)], high_b.at[step],
                   halo_send.at[step, 1, 1], halo_recv.at[step, 1, 1], down),
        ]

    def mat_copy(kind, side, device):
        layers = pl.ds(0, BUO) if kind == 0 else pl.ds(BUO, 2 * MOD)
        return remote(mat_out.at[side, layers], mat_in.at[side, layers],
                      mat_send.at[kind, side], mat_recv.at[kind, side], device)

    def each(flag, copies, act):
        @pl.when(flag)
        def _():
            for copy in copies():
                act(copy)

    begin, sent = (lambda copy: copy.start()), (lambda copy: copy.wait_send())

    def send_mats(kind):
        each(has_up, lambda: [mat_copy(kind, 0, up)], begin)
        each(has_down, lambda: [mat_copy(kind, 1, down)], begin)

    def take_mats(kind):
        for side, flag, device in ((0, has_down, up), (1, has_up, down)):
            @pl.when(flag)
            def _(side=side, device=device):
                mat_copy(kind, side, device).wait_recv()
                for at, target, lead in mat_layers[:1] if kind == 0 else mat_layers[1:]:
                    for z in range(lead):
                        target[z + (lead + DEPTH if side else 0)] = mat_in[side, at + z].astype(F32)

    def send_halos(step):
        @pl.when(has_up)
        def _():
            for copy in halo_up(step):
                copy.start()

        @pl.when(has_down)
        def _():
            for copy in halo_down(step):
                copy.start()

    send_mats(0)
    send_halos(0)
    place_sources(image_own.at[0], 0, DEPTH, peer, 0)

    band = extra[0] if MATMUL_X else None
    if MATMUL_X:
        row = lax.broadcasted_iota(jnp.int32, (2 * COLS, COLS), 0)
        offset = lax.rem(row, COLS) - lanes((2 * COLS, COLS))
        for k, sign in ((0, -1), (1, 1)):
            weight = jnp.where(offset == 0, -27.0 * sign, 0.0)
            weight = jnp.where(offset == sign, 27.0 * sign, weight)
            weight = jnp.where(offset == -sign, 1.0 * sign, weight)
            weight = jnp.where(offset == 2 * sign, -1.0 * sign, weight)
            band[k] = weight.astype(BF16)

    row_parts = list(zip(ROW_CUTS[:-1], ROW_CUTS[1:]))

    def across(index):
        if index == 0:
            layer, count, lo, hi = 3, 2, 0, ROWS
        else:
            lo, hi = row_parts[(index - 1) // 2]
            layer, count = (0, 3) if index % 2 else (5, 3)
        return remote(
            mirror.at[1, :, pl.ds(layer, count), pl.ds(lo, hi - lo)],
            got.at[:, pl.ds(FAR + layer, count), pl.ds(lo, hi - lo)],
            x_send.at[index], x_recv.at[index], partner,
        )

    across_count = 1 + 2 * len(row_parts)

    def forward(index, source, lead, upward, device):
        side, base = (0, 0) if upward else (1, FAR + DEPTH)
        if index == 0:
            return [
                remote(source.at[:, pl.ds(lead + 3, 2)], got.at[:, pl.ds(base + (1 if upward else 3), 2)],
                       fwd_send.at[0, side, 0], fwd_recv.at[0, side, 0], device)
            ]
        lo, hi = row_parts[index - 1]
        rows, deep = pl.ds(lo, hi - lo), pl.ds(6, 3)
        first, single = (5, 2) if upward else (0, 5)
        return [
            remote(source.at[:, pl.ds(lead + first, 3), rows],
                   got.at[:, pl.ds(base + (3 if upward else 0), 3), rows],
                   fwd_send.at[index, side, 0], fwd_recv.at[index, side, 0], device),
            remote(source.at[deep, pl.ds(lead + single, 1), rows],
                   got.at[deep, pl.ds(base + (0 if upward else 5), 1), rows],
                   fwd_send.at[index, side, 1], fwd_recv.at[index, side, 1], device),
        ]

    def forward_up(index):
        return forward(index, got, FAR, True, up)

    def forward_down(index):
        return forward(index, got, FAR, False, down)

    def straight_up(index):
        return forward(index, mirror.at[1], 0, True, cross_up)

    def straight_down(index):
        return forward(index, mirror.at[1], 0, False, cross_down)

    held = (me < 2) | (me >= slabs - 2)
    passes_up = has_up & jnp.logical_not(below_cross)
    passes_down = has_down & jnp.logical_not(above_cross)

    def pass_on(index):
        if index == 0:
            across(0).wait_recv()
        else:
            across(2 * index - 1).wait_recv()
            across(2 * index).wait_recv()
        each(passes_up, lambda: forward_up(index), begin)
        each(passes_down, lambda: forward_down(index), begin)

    own_way = jnp.logical_not(hands_over)

    def across_copies(index):
        return [across(0)] if index == 0 else [across(2 * index - 1), across(2 * index)]

    def send_across(index):
        if index < 2:
            for copy in across_copies(index):
                copy.start()
        else:
            each(own_way, lambda: across_copies(index), begin)
        each(below_cross, lambda: straight_up(index), begin)
        each(above_cross, lambda: straight_down(index), begin)

    late = pl.ds(ROW_CUTS[1], ROWS - ROW_CUTS[1])

    def hand_over():
        return [
            remote(mirror.at[1, :, pl.ds(first, 3), late], held_over.at[:, pl.ds(3 * k, 3)],
                   help_send.at[k], help_recv.at[k], (helper, peer))
            for k, first in enumerate((0, 5))
        ]

    def help_across():
        return [
            remote(held_over.at[:, pl.ds(3 * k, 3), pl.ds(lo - ROW_CUTS[1], hi - lo)],
                   got.at[:, pl.ds(FAR + first, 3), pl.ds(lo, hi - lo)],
                   help_send.at[2 * i + k], x_recv.at[2 * i - 1 + k], (helped, 1 - peer))
            for i, (lo, hi) in enumerate(row_parts, 1) if i > 1
            for k, first in enumerate((0, 5))
        ]

    def send_rest():
        for index in range(2, len(row_parts) + 1):
            send_across(index)

    def prepare():
        spread = (
            lax.broadcasted_iota(jnp.int32, (COLS // BLOCK, COLS), 0)
            == lanes((COLS // BLOCK, COLS)) // BLOCK
        ).astype(F32)
        exp_rows[...] = jnp.dot(
            exps[...].astype(F32), spread, preferred_element_type=F32, precision=lax.Precision.HIGHEST
        )

        @pl.loop(0, 9 * ROWS // BLOCK)
        def _(i):
            level = jnp.broadcast_to(exp_rows[pl.ds(i, 1), :], (BLOCK, COLS))
            upscale = jnp.ones((BLOCK, COLS), F32)
            downscale = upscale
            for exponent in (-2, -1, 1, 2):
                chosen = jnp.abs(level - exponent) < 0.5
                upscale = jnp.where(chosen, 2.0**exponent, upscale)
                downscale = jnp.where(chosen, 2.0**-exponent, downscale)
            up_rows[pl.ds(pl.multiple_of(i * BLOCK, BLOCK), BLOCK), :] = upscale
            down_rows[pl.ds(pl.multiple_of(i * BLOCK, BLOCK), BLOCK), :] = downscale

        @pl.loop(0, 9)
        def _(part):
            for z in range(DEPTH + 2 * FAR):
                other[part, z, pl.ds(0, PAD), :] = zero
                other[part, z, pl.ds(PAD + ROWS, PAD), :] = zero
        round_mats(mat_layers[1:])
        for step in (1, 2):
            place_sources(image_own.at[step], 0, DEPTH, peer, step)
        place_sources(image_far.at[pl.ds(0, DEPTH + 2 * MOD)], -MOD, DEPTH + 2 * MOD, 1 - peer, 1)
        place_sources(image_far.at[pl.ds(DEPTH + 2 * MOD, DEPTH)], 0, DEPTH, 1 - peer, 2)

    mine = Slab(own, OWN, buo, lame, shear, band).rows((0, ROWS))

    def copy_rounded(step, zs):
        @pl.loop(0, 9)
        def _(part):
            for z in zs:
                mirror[step + 1, part, z] = mine.at(part, z).astype(BF16)

    def tally(step):
        def body(k, carry):
            part = k // (DEPTH // 2)
            down_scale = down_rows[pl.ds(pl.multiple_of(part * ROWS, ROWS), ROWS), :]
            up_scale = up_rows[pl.ds(pl.multiple_of(part * ROWS, ROWS), ROWS), :]
            sizes, misfits, squares = carry
            for side in range(2):
                z = lax.rem(k, DEPTH // 2) * 2 + side
                value = mine.at(part, z)
                rounded = mirror[step + 1, part, z].astype(F32)
                level = jnp.clip(rounded * down_scale, -clip_level, clip_level)
                misfit = value - level * up_scale
                for y in range(0, ROWS, YB):
                    at = slice(y, y + YB)
                    sizes = sizes + jnp.abs(level[at])
                    misfits = misfits + misfit[at] * misfit[at]
                    squares = squares + value[at] * value[at]
            return sizes, misfits, squares

        zeros = jnp.zeros((YB, COLS), F32)
        for k, total in enumerate(lax.fori_loop(0, 9 * (DEPTH // 2), body, (zeros,) * 3)):
            sums[step, k] = total

    edges = lambda first, gap: (lambda i: first + i + (i // 3) * gap)

    theirs = Slab(other, FAR, buo, lame, shear, band)

    def widen(rows):
        lo, hi = rows

        def move(part, z):
            other[part, z, pl.ds(PAD + lo, hi - lo), :] = got[part, z, pl.ds(lo, hi - lo), :].astype(F32)

        @pl.loop(0, 9)
        def _(part):
            for z in range(1, DEPTH + 2 * FAR - 1):
                move(part, z)

        for part in range(6, 9):
            for z in (0, DEPTH + 2 * FAR - 1):
                move(part, z)

    def compress(step, rows):
        lo, hi = rows

        @pl.loop(0, 9)
        def _(part):
            for y in range(lo // YB * YB, hi, YB):
                row = lax.broadcasted_iota(jnp.int32, (YB, COLS), 0) + y
                down = down_rows[pl.ds(pl.multiple_of(part * ROWS + y, YB), YB), :]
                for z in range(DEPTH):
                    value = other[part, z + FAR, pl.ds(PAD + y, YB), :]
                    level = jnp.clip(value * down, -clip_level, clip_level)
                    if lo > y or hi < y + YB:
                        before = packed[step, part, z, pl.ds(y, YB), :].astype(F32)
                        level = jnp.where((row >= lo) & (row < hi), level, before)
                    packed[step, part, z, pl.ds(y, YB), :] = level.astype(BF16)


    def ends_of(index):
        if index < 0:
            return [0] * 4
        end = row_parts[GROUPS[index][-1]][1]
        return [end if end == ROWS else end - 2 * (k + 1) for k in range(4)]

    def recompute(index, between):
        lo, hi = row_parts[GROUPS[index][0]][0], row_parts[GROUPS[index][-1]][1]
        arriving = ([0] if index == 0 else []) + [part + 1 for part in GROUPS[index]]

        @pl.when(has_down)
        def _():
            for part in arriving:
                for copy in forward_up(part):
                    copy.wait_recv()

        @pl.when(has_up)
        def _():
            for part in arriving:
                for copy in forward_down(part):
                    copy.wait_recv()

        if index == 0:
            take_mats(1)
        widen((lo, hi))
        compress(0, (lo, hi))
        span = list(zip(ends_of(index - 1), ends_of(index)))
        wide_group = WIDE_GROUP
        theirs.rows(span[0])
        over(17, lambda i: i - 4, wide_group, theirs.velocity)
        theirs.rows(span[1])
        image = lambda z, y, n: image_far[z + MOD, pl.ds(y, n), :]
        over(14, lambda i: i - 3, wide_group, lambda zs: theirs.stress(zs, image))
        compress(1, span[1])
        between()
        theirs.rows(span[2])
        over(11, lambda i: i - 1, wide_group, theirs.velocity)
        theirs.rows(span[3])
        image = lambda z, y, n: image_far[z + DEPTH + 2 * MOD, pl.ds(y, n), :]
        over(DEPTH, lambda i: i, wide_group, lambda zs: theirs.stress(zs, image))
        compress(2, span[3])

    @pl.loop(0, STEPS)
    def _(step):
        @pl.when(step == 2)
        def _():
            pass_on(0)

        def image(z, y, n):
            return image_own[step, z, pl.ds(y, n), :]

        over(5, lambda i: i + 2, GROUP, mine.velocity)
        middle = (2, lambda i: i + 3)
        over(*middle, GROUP, lambda zs: mine.stress(zs, image))
        copy_rounded(step, (3, 4))

        @pl.when(step == 0)
        def _():
            send_across(0)
            prepare()
            take_mats(0)

        @pl.when((step == 2) & own_way)
        def _():
            pass_on(1)

        @pl.when(has_down)
        def _():
            for copy in halo_up(step):
                copy.wait_recv()

            @pl.loop(0, 6)
            def _(part):
                own[part, OWN - 1, inner, :] = low_a[step, part, 1].astype(F32)

            own[VZ, OWN - 2, inner, :] = low_a[step, VZ, 0].astype(F32)

            @pl.loop(0, 3)
            def _(part):
                for z in range(3):
                    own[part + 6, OWN - 3 + z, inner, :] = low_b[step, part, z].astype(F32)

        @pl.when(has_up)
        def _():
            for copy in halo_down(step):
                copy.wait_recv()

            @pl.loop(0, 6)
            def _(part):
                for z in range(2):
                    own[part, OWN + DEPTH + z, inner, :] = high_a[step, part, z].astype(F32)

            @pl.loop(0, 3)
            def _(part):
                for z in range(3):
                    own[part + 6, OWN + DEPTH + z, inner, :] = high_b[step, part, z].astype(F32)

        @pl.when((step == 2) & held)
        def _():
            send_rest()

        over(6, edges(-1, 5), GROUP, mine.velocity)
        outer = (6, edges(0, 2))
        over(*outer, GROUP, lambda zs: mine.stress(zs, image))
        copy_rounded(step, (0, 1, 2, 5, 6, 7))

        @pl.when(step < STEPS - 1)
        def _():
            send_halos(step + 1)

        @pl.when(step == 0)
        def _():
            send_mats(1)
            each(hands_over, hand_over, begin)
            pl.when(own_way)(lambda: send_across(1))

        @pl.when((step == 1) & jnp.logical_not(held))
        def _():
            pl.when(hands_over)(lambda: send_across(1))
            send_rest()

        tally(step)

    pl.when(hands_over)(lambda: pass_on(1))

    @pl.when(helps)
    def _():
        for copy in hand_over():
            copy.wait_recv()
        for copy in help_across():
            copy.start()

    row8 = lax.broadcasted_iota(jnp.int32, (8, COLS), 0)
    lane8 = lanes((8, COLS))
    tile = jnp.zeros((8, COLS), F32)
    for step in range(STEPS):
        for k in range(3):
            tile = tile + jnp.where((row8 == k) & (lane8 == step), jnp.sum(sums[step, k]), 0.0)

    def sum_copies(phase):
        peers, slot = ((near_peers, lane_of), (wide_peers, block))[phase]
        return [
            remote(stat_src.at[phase], stat_rx.at[phase, slot],
                   stat_send.at[phase, k], stat_recv.at[phase, k], device)
            for k, device in enumerate(peers)
        ]

    def spread_sums(phase, tile):
        stat_src[phase] = tile
        stat_rx[phase, (lane_of, block)[phase]] = tile
        for copy in sum_copies(phase):
            copy.start()

    def collect_sums(phase):
        for copy in sum_copies(phase):
            copy.wait()
        total = stat_rx[phase, 0]
        for k in range(1, (LOW, groups)[phase]):
            total = total + stat_rx[phase, k]
        return total

    spread_sums(0, tile)
    late_sums = below_cross | above_cross

    def second_phase():
        spread_sums(1, collect_sums(0))

    pass_on(2)
    pl.when(late_sums)(second_phase)
    recompute(0, lambda: pass_on(3))
    pl.when(jnp.logical_not(late_sums))(second_phase)
    recompute(1, lambda: None)

    tile = collect_sums(1)
    scaled = tile * (1.0 / (9 * slabs * DEPTH * ROWS * COLS))
    ratio = scaled[1:2] / (scaled[2:3] + energy_floor)
    stats_out[0:1, :] = scaled[0:1, :STEPS]
    stats_out[1:2, :] = jnp.sqrt(ratio)[:, :STEPS]

    for index in range(2):
        for copy in across_copies(index):
            copy.wait_send()
    for index in range(2, len(row_parts) + 1):
        each(own_way, lambda: across_copies(index), sent)
    each(hands_over, hand_over, sent)
    each(helps, help_across, sent)

    @pl.when(has_up)
    def _():
        for kind in range(2):
            mat_copy(kind, 0, up).wait_send()
        for step in range(STEPS):
            for copy in halo_up(step):
                copy.wait_send()

    @pl.when(has_down)
    def _():
        for kind in range(2):
            mat_copy(kind, 1, down).wait_send()
        for step in range(STEPS):
            for copy in halo_down(step):
                copy.wait_send()

    for index in range(len(row_parts) + 1):
        each(passes_up, lambda: forward_up(index), sent)
        each(passes_down, lambda: forward_down(index), sent)
        each(below_cross, lambda: straight_up(index), sent)
        each(above_cross, lambda: straight_down(index), sent)


def write_out(own, packed, sums, final_hbm, stored_hbm, stats_out, sem):
    copies = []
    for part in range(0, 9, 3):
        parts = pl.ds(part, 3)
        for step in range(STEPS):
            copies.append((packed.at[step, parts], stored_hbm.at[0, step, parts]))
        copies.append((own.at[parts, pl.ds(OWN, DEPTH), pl.ds(PAD, ROWS), :], final_hbm.at[0, parts]))
    copies = [pltpu.make_async_copy(source, target, sem.at[k]) for k, (source, target) in enumerate(copies)]
    for copy in copies:
        copy.start()
    stats_out[...] = sums[...]
    for copy in copies:
        copy.wait()


def per_device(slabs, wavefield, buoyancy, lame_lambda, shear_modulus, scale_exponents, source_cells, wavelet):
    hbm = pl.BlockSpec(memory_space=pl.ANY)
    vmem = pl.BlockSpec(memory_space=pltpu.VMEM)
    smem = pl.BlockSpec(memory_space=pltpu.SMEM)
    parts = len(ROW_CUTS) - 1
    dma = pltpu.SemaphoreType.DMA
    own, packed, statistics = pl.pallas_call(
        functools.partial(kernel, slabs),
        out_shape=(
            pltpu.VMEM((9, DEPTH + 2 * OWN, ROWS + 2 * PAD, COLS), F32),
            pltpu.VMEM((STEPS, 9, DEPTH, ROWS, COLS), BF16),
            pltpu.VMEM((2, STEPS), F32),
        ),
        in_specs=[hbm, hbm, hbm, hbm, vmem, smem, smem],
        out_specs=(vmem, vmem, vmem),
        scratch_shapes=[
            pltpu.VMEM((9, DEPTH + 2 * FAR, ROWS + 2 * PAD, COLS), F32),
            pltpu.VMEM((STEPS + 1, 9, DEPTH, ROWS, COLS), BF16),
            pltpu.VMEM((STEPS, 6, 2, ROWS, COLS), BF16),
            pltpu.VMEM((STEPS, 3, 3, ROWS, COLS), BF16),
            pltpu.VMEM((STEPS, 6, 2, ROWS, COLS), BF16),
            pltpu.VMEM((STEPS, 3, 3, ROWS, COLS), BF16),
            pltpu.VMEM((DEPTH + 2 * BUO, ROWS, COLS), F32),
            pltpu.VMEM((DEPTH + 2 * MOD, ROWS, COLS), F32),
            pltpu.VMEM((DEPTH + 2 * MOD, ROWS, COLS), F32),
            pltpu.VMEM((2, BUO + 2 * MOD, ROWS, COLS), BF16),
            pltpu.VMEM((2, BUO + 2 * MOD, ROWS, COLS), BF16),
            pltpu.VMEM((9, DEPTH + 2 * FAR, ROWS, COLS), BF16),
            pltpu.VMEM((9 * ROWS, COLS), F32),
            pltpu.VMEM((9 * ROWS, COLS), F32),
            pltpu.VMEM((9 * ROWS // BLOCK, COLS), F32),
            pltpu.VMEM((STEPS, 3, YB, COLS), F32),
            pltpu.VMEM((2, 8, COLS), F32),
            pltpu.VMEM((2, max(LOW, slabs // LOW), 8, COLS), F32),
            pltpu.VMEM((STEPS, DEPTH, ROWS, COLS), F32),
            pltpu.VMEM((2 * DEPTH + 2 * MOD, ROWS, COLS), F32),
            pltpu.VMEM((9, 6, ROWS - ROW_CUTS[1], COLS), BF16),
            dma((12,)),
            dma((STEPS, 2, 3)),
            dma((STEPS, 2, 3)),
            dma((2, 2)),
            dma((2, 2)),
            dma((1 + 2 * parts,)),
            dma((1 + 2 * parts,)),
            dma((2 + 2 * parts,)),
            dma((2,)),
            dma((1 + parts, 2, 2)),
            dma((1 + parts, 2, 2)),
            dma((2, max(LOW, slabs // LOW))),
            dma((2, max(LOW, slabs // LOW))),
        ]
        + ([pltpu.VMEM((2, 2 * COLS, COLS), BF16)] if MATMUL_X else []),
        compiler_params=pltpu.CompilerParams(
            collective_id=0, has_side_effects=True, vmem_limit_bytes=55 * 1024 * 1024
        ),
        name="elastic_steps",
    )(
        wavefield, buoyancy, lame_lambda, shear_modulus,
        scale_exponents.reshape(9 * ROWS // BLOCK, COLS // BLOCK), source_cells,
        wavelet.transpose(1, 0, 2),
    )
    final, stored, statistics = pl.pallas_call(
        write_out,
        out_shape=(
            jax.ShapeDtypeStruct(wavefield.shape, F32),
            jax.ShapeDtypeStruct((1, STEPS, 9, DEPTH, ROWS, COLS), BF16),
            jax.ShapeDtypeStruct((2, STEPS), F32),
        ),
        in_specs=[vmem, vmem, vmem],
        out_specs=(hbm, hbm, vmem),
        scratch_shapes=[dma((12,))],
        compiler_params=pltpu.CompilerParams(vmem_limit_bytes=8 * 1024 * 1024),
        name="write_out",
    )(own, packed, statistics)
    return final, stored, statistics.T[None]


def solution(mesh):
    return jax.shard_map(
        functools.partial(per_device, mesh.shape["space"]),
        mesh=mesh,
        in_specs=(
            P("peer", None, "space", None, None),
            P("space", None, None),
            P("space", None, None),
            P("space", None, None),
            P(None, "space", None, None),
            P(),
            P(),
        ),
        out_specs=(
            P("peer", None, "space", None, None),
            P("peer", None, None, "space", None, None),
            P("peer", None, None),
        ),
        check_vma=False,
    )
```

```python
import functools

import jax
import jax.numpy as jnp
from jax import lax
from jax.experimental import pallas as pl
from jax.experimental.pallas import tpu as pltpu
from jax.sharding import PartitionSpec as P

MESH = pl.DeviceIdType.MESH
F32 = jnp.float32
BF16 = jnp.bfloat16

BLOCK = 8
STEPS = 3
SOURCES = 8
DEPTH, ROWS, COLS = 8, 64, 128
PAD = 8
YB = 16
GROUP = 2
WIDE_GROUP = 9
MATMUL_X = False
OWN = 3
FAR = 6
BUO, MOD = 5, 3
LOW = 8
ROW_CUTS = (0, 32, 48, 64)
GROUPS = ((0,), (1, 2))
VX, VY, VZ, SXX, SYY, SXY, SZZ, SXZ, SYZ = range(9)
clip_level = 4.0
energy_floor = 1e-06


def lanes(shape):
    return lax.broadcasted_iota(jnp.int32, shape, 1)


class Slab:
    def __init__(self, ref, lead, buoyancy, lame, shear, band):
        self.ref, self.lead = ref, lead
        self.buoyancy, self.lame, self.shear, self.band = buoyancy, lame, shear, band

    def rows(self, rows):
        self.lo, self.hi = rows
        self.y = self.lo // BLOCK * BLOCK
        self.n = -(-self.hi // BLOCK) * BLOCK - self.y
        return self

    def at(self, part, z):
        return self.ref[part, z + self.lead, pl.ds(self.y + PAD, self.n), :]

    def put(self, part, z, value):
        ref, n = self.ref, self.n
        head = BLOCK if self.lo % BLOCK else 0
        tail = BLOCK if self.hi % BLOCK else 0
        row = lax.broadcasted_iota(jnp.int32, (BLOCK, COLS), 0)
        if head:
            at = pl.ds(self.y + PAD, BLOCK)
            keep = row >= self.lo % BLOCK
            if n == BLOCK and tail:
                keep = keep & (row < self.hi % BLOCK)
                tail = 0
            ref[part, z + self.lead, at, :] = jnp.where(keep, value[:BLOCK], ref[part, z + self.lead, at, :])
        if tail:
            at = pl.ds(self.y + PAD + n - BLOCK, BLOCK)
            keep = row < self.hi % BLOCK
            ref[part, z + self.lead, at, :] = jnp.where(
                keep, value[n - BLOCK :], ref[part, z + self.lead, at, :]
            )
        if n - head - tail:
            ref[part, z + self.lead, pl.ds(self.y + PAD + head, n - head - tail), :] = value[head : n - tail]


    def dx(self, part, z, forward):
        f = self.at(part, z)
        if self.band is not None:
            top = f.astype(BF16)
            rest = (f - top.astype(F32)).astype(BF16)
            return jnp.dot(
                jnp.concatenate([top, rest], axis=1), self.band[int(forward)], preferred_element_type=F32
            )
        lane = lanes((1, COLS))
        after = jnp.where(lane < COLS - 1, pltpu.roll(f, COLS - 1, 1), 0.0)
        before = jnp.where(lane >= 1, pltpu.roll(f, 1, 1), 0.0)
        if forward:
            far = jnp.where(lane < COLS - 2, pltpu.roll(f, COLS - 2, 1), 0.0)
            return 27.0 * (after - f) - (far - before)
        far = jnp.where(lane >= 2, pltpu.roll(f, 2, 1), 0.0)
        return 27.0 * (f - before) - (after - far)

    def dy(self, part, z, forward):
        get = lambda shift: self.ref[part, z + self.lead, pl.ds(self.y + PAD + shift, self.n), :]
        if forward:
            return get(1) - get(0), get(2) - get(-1)
        return get(0) - get(-1), get(1) - get(-2)

    def dz(self, part, z, forward):
        get = lambda shift: self.at(part, z + shift)
        if forward:
            return get(1) - get(0), get(2) - get(-1)
        return get(0) - get(-1), get(1) - get(-2)

    def mat(self, table, lead, z, factor):
        return table[z + lead, pl.ds(self.y, self.n), :] * factor

    def velocity(self, zs):
        results = []
        for z in zs:
            for part, along_x, along_y, along_z, at in (
                (VX, (SXX, True), (SXY, False), (SXZ, False), z),
                (VY, (SXY, False), (SYY, True), (SYZ, False), z),
                (VZ, (SXZ, False), (SYZ, False), (SZZ, True), z - 1),
            ):
                x = self.dx(along_x[0], at, along_x[1])
                y = self.dy(along_y[0], at, along_y[1])
                d = self.dz(along_z[0], at, along_z[1])
                change = 27.0 * (y[0] + d[0]) - (y[1] + d[1]) + x
                value = self.at(part, at) + self.mat(self.buoyancy, BUO, at, 1.0 / 24.0) * change
                results.append((part, at, value))
        for part, at, value in results:
            self.put(part, at, value)

    def stress(self, zs, image, plane_shear=True):
        results = []
        for z in zs:
            join = lambda pair: 27.0 * pair[0] - pair[1]
            strain = (
                self.dx(VX, z, False), join(self.dy(VY, z, False)), join(self.dz(VZ, z, False)),
            )
            shear = self.mat(self.shear, MOD, z, 1.0 / 24.0)
            pressure = self.mat(self.lame, MOD, z, 1.0 / 24.0) * (
                strain[0] + strain[1] + strain[2]
            ) + image(z, self.y, self.n)
            double = shear + shear
            for part, value in zip((SXX, SYY, SZZ), strain):
                results.append((part, z, self.at(part, z) + (pressure + double * value)))
            if plane_shear:
                change = join(self.dy(VX, z, True)) + self.dx(VY, z, True)
                results.append((SXY, z, self.at(SXY, z) + shear * change))
            change = join(self.dz(VX, z, True)) + self.dx(VZ, z, True)
            results.append((SXZ, z, self.at(SXZ, z) + shear * change))
            y, d = self.dy(VZ, z, True), self.dz(VY, z, True)
            change = 27.0 * (y[0] + d[0]) - (y[1] + d[1])
            results.append((SYZ, z, self.at(SYZ, z) + shear * change))
        for part, at, value in results:
            self.put(part, at, value)


def over(count, place, group, body):
    @pl.loop(0, count // group)
    def _(i):
        body([place(i * group + k) for k in range(group)])

    if count % group:
        body([place(i) for i in range(count // group * group, count)])


def kernel(
    slabs,
    wave_hbm, buo_hbm, lame_hbm, shear_hbm, exps, cells, wavelet,
    own, packed, stats_out,
    other, mirror, low_a, low_b, high_a, high_b, buo, lame, shear, mat_out, mat_in, got,
    up_rows, down_rows, exp_rows, sums, stat_src, stat_rx, image_own, image_far, held_over,
    in_sem, halo_send, halo_recv, mat_send, mat_recv,
    x_send, x_recv, help_send, help_recv, fwd_send, fwd_recv, stat_send, stat_recv, *extra,
):
    me, peer = lax.axis_index("space"), lax.axis_index("peer")
    has_down, has_up = me > 0, me < slabs - 1
    up, down = (me + 1, peer), (me - 1, peer)
    partner = (me, 1 - peer)
    half = slabs // 2
    below_cross, above_cross = me == half - 1, me == half
    cross_up, cross_down = (me + 1, 1 - peer), (me - 1, 1 - peer)
    detours = ((half - 2, -2), (half - 1, -LOW), (half, LOW), (half + 1, 2))
    flag = lambda condition: condition.astype(jnp.int32)
    hands_over = (me >= half - 2) & (me <= half + 1)
    helper = me + sum(flag(me == slab) * offset for slab, offset in detours)
    helped = sum(flag(me == slab + offset) * slab for slab, offset in detours)
    helps = helped > 0
    groups = slabs // LOW
    block, lane_of = me // LOW, lax.rem(me, LOW)
    near_peers = [(block * LOW + lax.rem(lane_of + k, LOW), peer) for k in range(1, LOW)]
    wide_peers = [(lax.rem(block + k, groups) * LOW + lane_of, peer) for k in range(1, groups)]

    barrier = pltpu.get_barrier_semaphore()
    for device in [partner] + near_peers + wide_peers:
        pl.semaphore_signal(barrier, inc=1, device_id=device, device_id_type=MESH)

    @pl.when(has_up)
    def _():
        pl.semaphore_signal(barrier, inc=1, device_id=up, device_id_type=MESH)

    @pl.when(has_down)
    def _():
        pl.semaphore_signal(barrier, inc=1, device_id=down, device_id_type=MESH)

    @pl.when(hands_over)
    def _():
        pl.semaphore_signal(barrier, inc=1, device_id=(helper, 1 - peer), device_id_type=MESH)

    @pl.when(helps)
    def _():
        pl.semaphore_signal(barrier, inc=1, device_id=(helped, peer), device_id_type=MESH)

    @pl.when(below_cross)
    def _():
        pl.semaphore_signal(barrier, inc=1, device_id=cross_up, device_id_type=MESH)

    @pl.when(above_cross)
    def _():
        pl.semaphore_signal(barrier, inc=1, device_id=cross_down, device_id_type=MESH)

    def remote(source, target, send, recv, device):
        return pltpu.make_async_remote_copy(
            src_ref=source, dst_ref=target, send_sem=send, recv_sem=recv,
            device_id=device, device_id_type=MESH,
        )

    inner = pl.ds(PAD, ROWS)
    loads = [
        pltpu.make_async_copy(
            wave_hbm.at[0, part], own.at[part, pl.ds(OWN, DEPTH), inner, :], in_sem.at[part]
        )
        for part in range(9)
    ]
    tables = ((buo_hbm, buo, BUO), (lame_hbm, lame, MOD), (shear_hbm, shear, MOD))
    mat_loads = [
        pltpu.make_async_copy(source, target.at[pl.ds(lead, DEPTH)], in_sem.at[9 + k])
        for k, (source, target, lead) in enumerate(tables)
    ]
    for copy in loads + mat_loads:
        copy.start()

    zero = jnp.zeros((PAD, COLS), F32)
    plane = jnp.zeros((ROWS, COLS), F32)

    @pl.loop(0, 9)
    def _(part):
        for z in range(DEPTH + 2 * OWN):
            own[part, z, pl.ds(0, PAD), :] = zero
            own[part, z, pl.ds(PAD + ROWS, PAD), :] = zero
        for z in list(range(OWN)) + list(range(OWN + DEPTH, DEPTH + 2 * OWN)):
            own[part, z, inner, :] = plane

    def clear(base_mat, base_own):
        for _, target, lead in tables:
            for z in range(lead):
                target[z + (lead + DEPTH if base_mat else 0)] = plane

        @pl.loop(0, 9)
        def _(part):
            for z in range(FAR):
                got[part, z + base_own] = jnp.zeros((ROWS, COLS), BF16)

    @pl.when(jnp.logical_not(has_down))
    def _():
        clear(0, 0)

    @pl.when(jnp.logical_not(has_up))
    def _():
        clear(1, FAR + DEPTH)

    for part, copy in enumerate(loads):
        copy.wait()
        for z in (0, 1, 6, 7) if part < 6 else (0, 1, 2, 5, 6, 7):
            mirror[0, part, z] = own[part, z + OWN, inner, :].astype(BF16)

    def place_sources(target, first_z, count, shot, step):
        place = lax.broadcasted_iota(jnp.int32, (ROWS, COLS), 0) * COLS + lanes((ROWS, COLS))

        @pl.loop(0, count)
        def _(i):
            first = (me * DEPTH + first_z + i) * ROWS * COLS
            total = jnp.zeros((ROWS, COLS), F32)
            for j in range(SOURCES):
                total = total + jnp.where(place == cells[shot, j] - first, wavelet[step, shot, j], 0.0)
            target[i] = total

    mat_layers = ((0, buo, BUO), (BUO, lame, MOD), (BUO + MOD, shear, MOD))

    def round_mats(layers_of):
        for at, target, lead in layers_of:
            for z in range(lead):
                mat_out[0, at + z] = target[DEPTH + z].astype(BF16)
                mat_out[1, at + z] = target[lead + z].astype(BF16)

    for copy in mat_loads:
        copy.wait()
    round_mats(mat_layers[:1])

    greeted = [flag(yes) for yes in (has_up, has_down, below_cross, above_cross, hands_over, helps)]
    pl.semaphore_wait(barrier, 1 + len(near_peers) + len(wide_peers) + sum(greeted))

    def halo_up(step):
        return [
            remote(mirror.at[step, pl.ds(0, 6), pl.ds(7, 1)], low_a.at[step, :, pl.ds(1, 1)],
                   halo_send.at[step, 0, 0], halo_recv.at[step, 0, 0], up),
            remote(mirror.at[step, pl.ds(VZ, 1), pl.ds(6, 1)], low_a.at[step, pl.ds(VZ, 1), pl.ds(0, 1)],
                   halo_send.at[step, 0, 2], halo_recv.at[step, 0, 2], up),
            remote(mirror.at[step, pl.ds(6, 3), pl.ds(5, 3)], low_b.at[step],
                   halo_send.at[step, 0, 1], halo_recv.at[step, 0, 1], up),
        ]

    def halo_down(step):
        return [
            remote(mirror.at[step, pl.ds(0, 6), pl.ds(0, 2)], high_a.at[step],
                   halo_send.at[step, 1, 0], halo_recv.at[step, 1, 0], down),
            remote(mirror.at[step, pl.ds(6, 3), pl.ds(0, 3)], high_b.at[step],
                   halo_send.at[step, 1, 1], halo_recv.at[step, 1, 1], down),
        ]

    def mat_copy(kind, side, device):
        layers = pl.ds(0, BUO) if kind == 0 else pl.ds(BUO, 2 * MOD)
        return remote(mat_out.at[side, layers], mat_in.at[side, layers],
                      mat_send.at[kind, side], mat_recv.at[kind, side], device)

    def each(flag, copies, act):
        @pl.when(flag)
        def _():
            for copy in copies():
                act(copy)

    begin, sent = (lambda copy: copy.start()), (lambda copy: copy.wait_send())

    def send_mats(kind):
        each(has_up, lambda: [mat_copy(kind, 0, up)], begin)
        each(has_down, lambda: [mat_copy(kind, 1, down)], begin)

    def take_mats(kind):
        for side, flag, device in ((0, has_down, up), (1, has_up, down)):
            @pl.when(flag)
            def _(side=side, device=device):
                mat_copy(kind, side, device).wait_recv()
                for at, target, lead in mat_layers[:1] if kind == 0 else mat_layers[1:]:
                    for z in range(lead):
                        target[z + (lead + DEPTH if side else 0)] = mat_in[side, at + z].astype(F32)

    def send_halos(step):
        @pl.when(has_up)
        def _():
            for copy in halo_up(step):
                copy.start()

        @pl.when(has_down)
        def _():
            for copy in halo_down(step):
                copy.start()

    send_mats(0)
    send_halos(0)
    place_sources(image_own.at[0], 0, DEPTH, peer, 0)

    band = extra[0] if MATMUL_X else None
    if MATMUL_X:
        row = lax.broadcasted_iota(jnp.int32, (2 * COLS, COLS), 0)
        offset = lax.rem(row, COLS) - lanes((2 * COLS, COLS))
        for k, sign in ((0, -1), (1, 1)):
            weight = jnp.where(offset == 0, -27.0 * sign, 0.0)
            weight = jnp.where(offset == sign, 27.0 * sign, weight)
            weight = jnp.where(offset == -sign, 1.0 * sign, weight)
            weight = jnp.where(offset == 2 * sign, -1.0 * sign, weight)
            band[k] = weight.astype(BF16)

    row_parts = list(zip(ROW_CUTS[:-1], ROW_CUTS[1:]))

    def across(index):
        if index == 0:
            layer, count, lo, hi = 3, 2, 0, ROWS
        else:
            lo, hi = row_parts[(index - 1) // 2]
            layer, count = (0, 3) if index % 2 else (5, 3)
        return remote(
            mirror.at[1, :, pl.ds(layer, count), pl.ds(lo, hi - lo)],
            got.at[:, pl.ds(FAR + layer, count), pl.ds(lo, hi - lo)],
            x_send.at[index], x_recv.at[index], partner,
        )

    across_count = 1 + 2 * len(row_parts)

    def forward(index, source, lead, upward, device):
        side, base = (0, 0) if upward else (1, FAR + DEPTH)
        if index == 0:
            return [
                remote(source.at[:, pl.ds(lead + 3, 2)], got.at[:, pl.ds(base + (1 if upward else 3), 2)],
                       fwd_send.at[0, side, 0], fwd_recv.at[0, side, 0], device)
            ]
        lo, hi = row_parts[index - 1]
        rows, deep = pl.ds(lo, hi - lo), pl.ds(6, 3)
        first, single = (5, 2) if upward else (0, 5)
        return [
            remote(source.at[:, pl.ds(lead + first, 3), rows],
                   got.at[:, pl.ds(base + (3 if upward else 0), 3), rows],
                   fwd_send.at[index, side, 0], fwd_recv.at[index, side, 0], device),
            remote(source.at[deep, pl.ds(lead + single, 1), rows],
                   got.at[deep, pl.ds(base + (0 if upward else 5), 1), rows],
                   fwd_send.at[index, side, 1], fwd_recv.at[index, side, 1], device),
        ]

    def forward_up(index):
        return forward(index, got, FAR, True, up)

    def forward_down(index):
        return forward(index, got, FAR, False, down)

    def straight_up(index):
        return forward(index, mirror.at[1], 0, True, cross_up)

    def straight_down(index):
        return forward(index, mirror.at[1], 0, False, cross_down)

    held = (me < 2) | (me >= slabs - 2)
    passes_up = has_up & jnp.logical_not(below_cross)
    passes_down = has_down & jnp.logical_not(above_cross)

    def pass_on(index):
        if index == 0:
            across(0).wait_recv()
        else:
            across(2 * index - 1).wait_recv()
            across(2 * index).wait_recv()
        each(passes_up, lambda: forward_up(index), begin)
        each(passes_down, lambda: forward_down(index), begin)

    own_way = jnp.logical_not(hands_over)

    def across_copies(index):
        return [across(0)] if index == 0 else [across(2 * index - 1), across(2 * index)]

    def send_across(index):
        if index < 2:
            for copy in across_copies(index):
                copy.start()
        else:
            each(own_way, lambda: across_copies(index), begin)
        each(below_cross, lambda: straight_up(index), begin)
        each(above_cross, lambda: straight_down(index), begin)

    late = pl.ds(ROW_CUTS[1], ROWS - ROW_CUTS[1])

    def hand_over():
        return [
            remote(mirror.at[1, :, pl.ds(first, 3), late], held_over.at[:, pl.ds(3 * k, 3)],
                   help_send.at[k], help_recv.at[k], (helper, peer))
            for k, first in enumerate((0, 5))
        ]

    def help_across():
        return [
            remote(held_over.at[:, pl.ds(3 * k, 3), pl.ds(lo - ROW_CUTS[1], hi - lo)],
                   got.at[:, pl.ds(FAR + first, 3), pl.ds(lo, hi - lo)],
                   help_send.at[2 * i + k], x_recv.at[2 * i - 1 + k], (helped, 1 - peer))
            for i, (lo, hi) in enumerate(row_parts, 1) if i > 1
            for k, first in enumerate((0, 5))
        ]

    def send_rest():
        for index in range(2, len(row_parts) + 1):
            send_across(index)

    def prepare():
        spread = (
            lax.broadcasted_iota(jnp.int32, (COLS // BLOCK, COLS), 0)
            == lanes((COLS // BLOCK, COLS)) // BLOCK
        ).astype(F32)
        exp_rows[...] = jnp.dot(
            exps[...].astype(F32), spread, preferred_element_type=F32, precision=lax.Precision.HIGHEST
        )

        @pl.loop(0, 9 * ROWS // BLOCK)
        def _(i):
            level = jnp.broadcast_to(exp_rows[pl.ds(i, 1), :], (BLOCK, COLS))
            upscale = jnp.ones((BLOCK, COLS), F32)
            downscale = upscale
            for exponent in (-2, -1, 1, 2):
                chosen = jnp.abs(level - exponent) < 0.5
                upscale = jnp.where(chosen, 2.0**exponent, upscale)
                downscale = jnp.where(chosen, 2.0**-exponent, downscale)
            up_rows[pl.ds(pl.multiple_of(i * BLOCK, BLOCK), BLOCK), :] = upscale
            down_rows[pl.ds(pl.multiple_of(i * BLOCK, BLOCK), BLOCK), :] = downscale

        @pl.loop(0, 9)
        def _(part):
            for z in range(DEPTH + 2 * FAR):
                other[part, z, pl.ds(0, PAD), :] = zero
                other[part, z, pl.ds(PAD + ROWS, PAD), :] = zero
        round_mats(mat_layers[1:])
        for step in (1, 2):
            place_sources(image_own.at[step], 0, DEPTH, peer, step)
        place_sources(image_far.at[pl.ds(0, DEPTH + 2 * MOD)], -MOD, DEPTH + 2 * MOD, 1 - peer, 1)
        place_sources(image_far.at[pl.ds(DEPTH + 2 * MOD, DEPTH)], 0, DEPTH, 1 - peer, 2)

    mine = Slab(own, OWN, buo, lame, shear, band).rows((0, ROWS))

    def copy_rounded(step, zs):
        @pl.loop(0, 9)
        def _(part):
            for z in zs:
                mirror[step + 1, part, z] = mine.at(part, z).astype(BF16)

    def tally(step):
        def body(k, carry):
            part = k // (DEPTH // 2)
            down_scale = down_rows[pl.ds(pl.multiple_of(part * ROWS, ROWS), ROWS), :]
            up_scale = up_rows[pl.ds(pl.multiple_of(part * ROWS, ROWS), ROWS), :]
            sizes, misfits, squares = carry
            for side in range(2):
                z = lax.rem(k, DEPTH // 2) * 2 + side
                value = mine.at(part, z)
                rounded = mirror[step + 1, part, z].astype(F32)
                level = jnp.clip(rounded * down_scale, -clip_level, clip_level)
                misfit = value - level * up_scale
                for y in range(0, ROWS, YB):
                    at = slice(y, y + YB)
                    sizes = sizes + jnp.abs(level[at])
                    misfits = misfits + misfit[at] * misfit[at]
                    squares = squares + value[at] * value[at]
            return sizes, misfits, squares

        zeros = jnp.zeros((YB, COLS), F32)
        for k, total in enumerate(lax.fori_loop(0, 9 * (DEPTH // 2), body, (zeros,) * 3)):
            sums[step, k] = total

    edges = lambda first, gap: (lambda i: first + i + (i // 3) * gap)

    theirs = Slab(other, FAR, buo, lame, shear, band)

    def widen(rows):
        lo, hi = rows

        def move(part, z):
            other[part, z, pl.ds(PAD + lo, hi - lo), :] = got[part, z, pl.ds(lo, hi - lo), :].astype(F32)

        @pl.loop(0, 9)
        def _(part):
            for z in range(1, DEPTH + 2 * FAR - 1):
                move(part, z)

        for part in range(6, 9):
            for z in (0, DEPTH + 2 * FAR - 1):
                move(part, z)

    def compress(step, rows):
        lo, hi = rows

        @pl.loop(0, 9)
        def _(part):
            for y in range(lo // YB * YB, hi, YB):
                row = lax.broadcasted_iota(jnp.int32, (YB, COLS), 0) + y
                down = down_rows[pl.ds(pl.multiple_of(part * ROWS + y, YB), YB), :]
                for z in range(DEPTH):
                    value = other[part, z + FAR, pl.ds(PAD + y, YB), :]
                    level = jnp.clip(value * down, -clip_level, clip_level)
                    if lo > y or hi < y + YB:
                        before = packed[step, part, z, pl.ds(y, YB), :].astype(F32)
                        level = jnp.where((row >= lo) & (row < hi), level, before)
                    packed[step, part, z, pl.ds(y, YB), :] = level.astype(BF16)


    def ends_of(index):
        if index < 0:
            return [0] * 4
        end = row_parts[GROUPS[index][-1]][1]
        return [end if end == ROWS else end - 2 * (k + 1) for k in range(4)]

    def recompute(index, between):
        lo, hi = row_parts[GROUPS[index][0]][0], row_parts[GROUPS[index][-1]][1]
        arriving = ([0] if index == 0 else []) + [part + 1 for part in GROUPS[index]]

        @pl.when(has_down)
        def _():
            for part in arriving:
                for copy in forward_up(part):
                    copy.wait_recv()

        @pl.when(has_up)
        def _():
            for part in arriving:
                for copy in forward_down(part):
                    copy.wait_recv()

        if index == 0:
            take_mats(1)
        widen((lo, hi))
        compress(0, (lo, hi))
        span = list(zip(ends_of(index - 1), ends_of(index)))
        wide_group = WIDE_GROUP
        theirs.rows(span[0])
        over(17, lambda i: i - 4, wide_group, theirs.velocity)
        theirs.rows(span[1])
        image = lambda z, y, n: image_far[z + MOD, pl.ds(y, n), :]
        over(14, lambda i: i - 3, wide_group, lambda zs: theirs.stress(zs, image))
        compress(1, span[1])
        between()
        theirs.rows(span[2])
        over(11, lambda i: i - 1, wide_group, theirs.velocity)
        theirs.rows(span[3])
        image = lambda z, y, n: image_far[z + DEPTH + 2 * MOD, pl.ds(y, n), :]
        over(DEPTH, lambda i: i, wide_group, lambda zs: theirs.stress(zs, image))
        compress(2, span[3])

    @pl.loop(0, STEPS)
    def _(step):
        @pl.when(step == 2)
        def _():
            pass_on(0)

        def image(z, y, n):
            return image_own[step, z, pl.ds(y, n), :]

        over(5, lambda i: i + 2, GROUP, mine.velocity)
        middle = (2, lambda i: i + 3)
        over(*middle, GROUP, lambda zs: mine.stress(zs, image))
        copy_rounded(step, (3, 4))

        @pl.when(step == 0)
        def _():
            send_across(0)
            prepare()
            take_mats(0)

        @pl.when((step == 2) & own_way)
        def _():
            pass_on(1)

        @pl.when(has_down)
        def _():
            for copy in halo_up(step):
                copy.wait_recv()

            @pl.loop(0, 6)
            def _(part):
                own[part, OWN - 1, inner, :] = low_a[step, part, 1].astype(F32)

            own[VZ, OWN - 2, inner, :] = low_a[step, VZ, 0].astype(F32)

            @pl.loop(0, 3)
            def _(part):
                for z in range(3):
                    own[part + 6, OWN - 3 + z, inner, :] = low_b[step, part, z].astype(F32)

        @pl.when(has_up)
        def _():
            for copy in halo_down(step):
                copy.wait_recv()

            @pl.loop(0, 6)
            def _(part):
                for z in range(2):
                    own[part, OWN + DEPTH + z, inner, :] = high_a[step, part, z].astype(F32)

            @pl.loop(0, 3)
            def _(part):
                for z in range(3):
                    own[part + 6, OWN + DEPTH + z, inner, :] = high_b[step, part, z].astype(F32)

        @pl.when((step == 2) & held)
        def _():
            send_rest()

        over(6, edges(-1, 5), GROUP, mine.velocity)
        outer = (6, edges(0, 2))
        over(*outer, GROUP, lambda zs: mine.stress(zs, image))
        copy_rounded(step, (0, 1, 2, 5, 6, 7))

        @pl.when(step < STEPS - 1)
        def _():
            send_halos(step + 1)

        @pl.when(step == 0)
        def _():
            send_mats(1)
            each(hands_over, hand_over, begin)
            pl.when(own_way)(lambda: send_across(1))

        @pl.when((step == 1) & jnp.logical_not(held))
        def _():
            pl.when(hands_over)(lambda: send_across(1))
            send_rest()

        tally(step)

    pl.when(hands_over)(lambda: pass_on(1))

    @pl.when(helps)
    def _():
        for copy in hand_over():
            copy.wait_recv()
        for copy in help_across():
            copy.start()

    row8 = lax.broadcasted_iota(jnp.int32, (8, COLS), 0)
    lane8 = lanes((8, COLS))
    tile = jnp.zeros((8, COLS), F32)
    for step in range(STEPS):
        for k in range(3):
            tile = tile + jnp.where((row8 == k) & (lane8 == step), jnp.sum(sums[step, k]), 0.0)

    def sum_copies(phase):
        peers, slot = ((near_peers, lane_of), (wide_peers, block))[phase]
        return [
            remote(stat_src.at[phase], stat_rx.at[phase, slot],
                   stat_send.at[phase, k], stat_recv.at[phase, k], device)
            for k, device in enumerate(peers)
        ]

    def spread_sums(phase, tile):
        stat_src[phase] = tile
        stat_rx[phase, (lane_of, block)[phase]] = tile
        for copy in sum_copies(phase):
            copy.start()

    def collect_sums(phase):
        for copy in sum_copies(phase):
            copy.wait()
        total = stat_rx[phase, 0]
        for k in range(1, (LOW, groups)[phase]):
            total = total + stat_rx[phase, k]
        return total

    spread_sums(0, tile)
    late_sums = below_cross | above_cross

    def second_phase():
        spread_sums(1, collect_sums(0))

    pass_on(2)
    pl.when(late_sums)(second_phase)
    pl.when(hands_over)(lambda: pass_on(3))
    recompute(0, lambda: pl.when(own_way)(lambda: pass_on(3)))
    pl.when(jnp.logical_not(late_sums))(second_phase)
    recompute(1, lambda: None)

    tile = collect_sums(1)
    scaled = tile * (1.0 / (9 * slabs * DEPTH * ROWS * COLS))
    ratio = scaled[1:2] / (scaled[2:3] + energy_floor)
    stats_out[0:1, :] = scaled[0:1, :STEPS]
    stats_out[1:2, :] = jnp.sqrt(ratio)[:, :STEPS]

    for index in range(2):
        for copy in across_copies(index):
            copy.wait_send()
    for index in range(2, len(row_parts) + 1):
        each(own_way, lambda: across_copies(index), sent)
    each(hands_over, hand_over, sent)
    each(helps, help_across, sent)

    @pl.when(has_up)
    def _():
        for kind in range(2):
            mat_copy(kind, 0, up).wait_send()
        for step in range(STEPS):
            for copy in halo_up(step):
                copy.wait_send()

    @pl.when(has_down)
    def _():
        for kind in range(2):
            mat_copy(kind, 1, down).wait_send()
        for step in range(STEPS):
            for copy in halo_down(step):
                copy.wait_send()

    for index in range(len(row_parts) + 1):
        each(passes_up, lambda: forward_up(index), sent)
        each(passes_down, lambda: forward_down(index), sent)
        each(below_cross, lambda: straight_up(index), sent)
        each(above_cross, lambda: straight_down(index), sent)


def write_out(own, packed, sums, final_hbm, stored_hbm, stats_out, sem):
    copies = []
    for part in range(0, 9, 3):
        parts = pl.ds(part, 3)
        for step in range(STEPS):
            copies.append((packed.at[step, parts], stored_hbm.at[0, step, parts]))
        copies.append((own.at[parts, pl.ds(OWN, DEPTH), pl.ds(PAD, ROWS), :], final_hbm.at[0, parts]))
    copies = [pltpu.make_async_copy(source, target, sem.at[k]) for k, (source, target) in enumerate(copies)]
    for copy in copies:
        copy.start()
    stats_out[...] = sums[...]
    for copy in copies:
        copy.wait()


def per_device(slabs, wavefield, buoyancy, lame_lambda, shear_modulus, scale_exponents, source_cells, wavelet):
    hbm = pl.BlockSpec(memory_space=pl.ANY)
    vmem = pl.BlockSpec(memory_space=pltpu.VMEM)
    smem = pl.BlockSpec(memory_space=pltpu.SMEM)
    parts = len(ROW_CUTS) - 1
    dma = pltpu.SemaphoreType.DMA
    own, packed, statistics = pl.pallas_call(
        functools.partial(kernel, slabs),
        out_shape=(
            pltpu.VMEM((9, DEPTH + 2 * OWN, ROWS + 2 * PAD, COLS), F32),
            pltpu.VMEM((STEPS, 9, DEPTH, ROWS, COLS), BF16),
            pltpu.VMEM((2, STEPS), F32),
        ),
        in_specs=[hbm, hbm, hbm, hbm, vmem, smem, smem],
        out_specs=(vmem, vmem, vmem),
        scratch_shapes=[
            pltpu.VMEM((9, DEPTH + 2 * FAR, ROWS + 2 * PAD, COLS), F32),
            pltpu.VMEM((STEPS + 1, 9, DEPTH, ROWS, COLS), BF16),
            pltpu.VMEM((STEPS, 6, 2, ROWS, COLS), BF16),
            pltpu.VMEM((STEPS, 3, 3, ROWS, COLS), BF16),
            pltpu.VMEM((STEPS, 6, 2, ROWS, COLS), BF16),
            pltpu.VMEM((STEPS, 3, 3, ROWS, COLS), BF16),
            pltpu.VMEM((DEPTH + 2 * BUO, ROWS, COLS), F32),
            pltpu.VMEM((DEPTH + 2 * MOD, ROWS, COLS), F32),
            pltpu.VMEM((DEPTH + 2 * MOD, ROWS, COLS), F32),
            pltpu.VMEM((2, BUO + 2 * MOD, ROWS, COLS), BF16),
            pltpu.VMEM((2, BUO + 2 * MOD, ROWS, COLS), BF16),
            pltpu.VMEM((9, DEPTH + 2 * FAR, ROWS, COLS), BF16),
            pltpu.VMEM((9 * ROWS, COLS), F32),
            pltpu.VMEM((9 * ROWS, COLS), F32),
            pltpu.VMEM((9 * ROWS // BLOCK, COLS), F32),
            pltpu.VMEM((STEPS, 3, YB, COLS), F32),
            pltpu.VMEM((2, 8, COLS), F32),
            pltpu.VMEM((2, max(LOW, slabs // LOW), 8, COLS), F32),
            pltpu.VMEM((STEPS, DEPTH, ROWS, COLS), F32),
            pltpu.VMEM((2 * DEPTH + 2 * MOD, ROWS, COLS), F32),
            pltpu.VMEM((9, 6, ROWS - ROW_CUTS[1], COLS), BF16),
            dma((12,)),
            dma((STEPS, 2, 3)),
            dma((STEPS, 2, 3)),
            dma((2, 2)),
            dma((2, 2)),
            dma((1 + 2 * parts,)),
            dma((1 + 2 * parts,)),
            dma((2 + 2 * parts,)),
            dma((2,)),
            dma((1 + parts, 2, 2)),
            dma((1 + parts, 2, 2)),
            dma((2, max(LOW, slabs // LOW))),
            dma((2, max(LOW, slabs // LOW))),
        ]
        + ([pltpu.VMEM((2, 2 * COLS, COLS), BF16)] if MATMUL_X else []),
        compiler_params=pltpu.CompilerParams(
            collective_id=0, has_side_effects=True, vmem_limit_bytes=55 * 1024 * 1024
        ),
        name="elastic_steps",
    )(
        wavefield, buoyancy, lame_lambda, shear_modulus,
        scale_exponents.reshape(9 * ROWS // BLOCK, COLS // BLOCK), source_cells,
        wavelet.transpose(1, 0, 2),
    )
    final, stored, statistics = pl.pallas_call(
        write_out,
        out_shape=(
            jax.ShapeDtypeStruct(wavefield.shape, F32),
            jax.ShapeDtypeStruct((1, STEPS, 9, DEPTH, ROWS, COLS), BF16),
            jax.ShapeDtypeStruct((2, STEPS), F32),
        ),
        in_specs=[vmem, vmem, vmem],
        out_specs=(hbm, hbm, vmem),
        scratch_shapes=[dma((12,))],
        compiler_params=pltpu.CompilerParams(vmem_limit_bytes=8 * 1024 * 1024),
        name="write_out",
    )(own, packed, statistics)
    return final, stored, statistics.T[None]


def solution(mesh):
    return jax.shard_map(
        functools.partial(per_device, mesh.shape["space"]),
        mesh=mesh,
        in_specs=(
            P("peer", None, "space", None, None),
            P("space", None, None),
            P("space", None, None),
            P("space", None, None),
            P(None, "space", None, None),
            P(),
            P(),
        ),
        out_specs=(
            P("peer", None, "space", None, None),
            P("peer", None, None, "space", None, None),
            P("peer", None, None),
        ),
        check_vma=False,
    )
```

```python
import functools

import jax
import jax.numpy as jnp
from jax import lax
from jax.experimental import pallas as pl
from jax.experimental.pallas import tpu as pltpu
from jax.sharding import PartitionSpec as P

MESH = pl.DeviceIdType.MESH
F32 = jnp.float32
BF16 = jnp.bfloat16

BLOCK = 8
STEPS = 3
SOURCES = 8
DEPTH, ROWS, COLS = 8, 64, 128
PAD = 8
YB = 16
GROUP = 2
WIDE_GROUP = 9
MATMUL_X = False
OWN = 3
FAR = 6
BUO, MOD = 5, 3
LOW = 8
ROW_CUTS = (0, 32, 48, 64)
GROUPS = ((0,), (1, 2))
VX, VY, VZ, SXX, SYY, SXY, SZZ, SXZ, SYZ = range(9)
clip_level = 4.0
energy_floor = 1e-06


def lanes(shape):
    return lax.broadcasted_iota(jnp.int32, shape, 1)


class Slab:
    def __init__(self, ref, lead, buoyancy, lame, shear, band):
        self.ref, self.lead = ref, lead
        self.buoyancy, self.lame, self.shear, self.band = buoyancy, lame, shear, band

    def rows(self, rows):
        self.lo, self.hi = rows
        self.y = self.lo // BLOCK * BLOCK
        self.n = -(-self.hi // BLOCK) * BLOCK - self.y
        return self

    def at(self, part, z):
        return self.ref[part, z + self.lead, pl.ds(self.y + PAD, self.n), :]

    def put(self, part, z, value):
        ref, n = self.ref, self.n
        head = BLOCK if self.lo % BLOCK else 0
        tail = BLOCK if self.hi % BLOCK else 0
        row = lax.broadcasted_iota(jnp.int32, (BLOCK, COLS), 0)
        if head:
            at = pl.ds(self.y + PAD, BLOCK)
            keep = row >= self.lo % BLOCK
            if n == BLOCK and tail:
                keep = keep & (row < self.hi % BLOCK)
                tail = 0
            ref[part, z + self.lead, at, :] = jnp.where(keep, value[:BLOCK], ref[part, z + self.lead, at, :])
        if tail:
            at = pl.ds(self.y + PAD + n - BLOCK, BLOCK)
            keep = row < self.hi % BLOCK
            ref[part, z + self.lead, at, :] = jnp.where(
                keep, value[n - BLOCK :], ref[part, z + self.lead, at, :]
            )
        if n - head - tail:
            ref[part, z + self.lead, pl.ds(self.y + PAD + head, n - head - tail), :] = value[head : n - tail]


    def dx(self, part, z, forward):
        f = self.at(part, z)
        if self.band is not None:
            top = f.astype(BF16)
            rest = (f - top.astype(F32)).astype(BF16)
            return jnp.dot(
                jnp.concatenate([top, rest], axis=1), self.band[int(forward)], preferred_element_type=F32
            )
        lane = lanes((1, COLS))
        after = jnp.where(lane < COLS - 1, pltpu.roll(f, COLS - 1, 1), 0.0)
        before = jnp.where(lane >= 1, pltpu.roll(f, 1, 1), 0.0)
        if forward:
            far = jnp.where(lane < COLS - 2, pltpu.roll(f, COLS - 2, 1), 0.0)
            return 27.0 * (after - f) - (far - before)
        far = jnp.where(lane >= 2, pltpu.roll(f, 2, 1), 0.0)
        return 27.0 * (f - before) - (after - far)

    def dy(self, part, z, forward):
        get = lambda shift: self.ref[part, z + self.lead, pl.ds(self.y + PAD + shift, self.n), :]
        if forward:
            return get(1) - get(0), get(2) - get(-1)
        return get(0) - get(-1), get(1) - get(-2)

    def dz(self, part, z, forward):
        get = lambda shift: self.at(part, z + shift)
        if forward:
            return get(1) - get(0), get(2) - get(-1)
        return get(0) - get(-1), get(1) - get(-2)

    def mat(self, table, lead, z, factor):
        return table[z + lead, pl.ds(self.y, self.n), :] * factor

    def velocity(self, zs):
        results = []
        for z in zs:
            for part, along_x, along_y, along_z, at in (
                (VX, (SXX, True), (SXY, False), (SXZ, False), z),
                (VY, (SXY, False), (SYY, True), (SYZ, False), z),
                (VZ, (SXZ, False), (SYZ, False), (SZZ, True), z - 1),
            ):
                x = self.dx(along_x[0], at, along_x[1])
                y = self.dy(along_y[0], at, along_y[1])
                d = self.dz(along_z[0], at, along_z[1])
                change = 27.0 * (y[0] + d[0]) - (y[1] + d[1]) + x
                value = self.at(part, at) + self.mat(self.buoyancy, BUO, at, 1.0 / 24.0) * change
                results.append((part, at, value))
        for part, at, value in results:
            self.put(part, at, value)

    def stress(self, zs, image, plane_shear=True):
        results = []
        for z in zs:
            join = lambda pair: 27.0 * pair[0] - pair[1]
            strain = (
                self.dx(VX, z, False), join(self.dy(VY, z, False)), join(self.dz(VZ, z, False)),
            )
            shear = self.mat(self.shear, MOD, z, 1.0 / 24.0)
            pressure = self.mat(self.lame, MOD, z, 1.0 / 24.0) * (
                strain[0] + strain[1] + strain[2]
            ) + image(z, self.y, self.n)
            double = shear + shear
            for part, value in zip((SXX, SYY, SZZ), strain):
                results.append((part, z, self.at(part, z) + (pressure + double * value)))
            if plane_shear:
                change = join(self.dy(VX, z, True)) + self.dx(VY, z, True)
                results.append((SXY, z, self.at(SXY, z) + shear * change))
            change = join(self.dz(VX, z, True)) + self.dx(VZ, z, True)
            results.append((SXZ, z, self.at(SXZ, z) + shear * change))
            y, d = self.dy(VZ, z, True), self.dz(VY, z, True)
            change = 27.0 * (y[0] + d[0]) - (y[1] + d[1])
            results.append((SYZ, z, self.at(SYZ, z) + shear * change))
        for part, at, value in results:
            self.put(part, at, value)


def over(count, place, group, body):
    @pl.loop(0, count // group)
    def _(i):
        body([place(i * group + k) for k in range(group)])

    if count % group:
        body([place(i) for i in range(count // group * group, count)])


def kernel(
    slabs,
    wave_hbm, buo_hbm, lame_hbm, shear_hbm, exps, cells, wavelet,
    own, packed, stats_out,
    other, mirror, low_a, low_b, high_a, high_b, buo, lame, shear, mat_out, mat_in, got,
    up_rows, down_rows, exp_rows, sums, stat_src, stat_rx, image_own, image_far, held_over,
    in_sem, halo_send, halo_recv, mat_send, mat_recv,
    x_send, x_recv, help_send, help_recv, fwd_send, fwd_recv, stat_send, stat_recv, *extra,
):
    me, peer = lax.axis_index("space"), lax.axis_index("peer")
    has_down, has_up = me > 0, me < slabs - 1
    up, down = (me + 1, peer), (me - 1, peer)
    partner = (me, 1 - peer)
    half = slabs // 2
    below_cross, above_cross = me == half - 1, me == half
    cross_up, cross_down = (me + 1, 1 - peer), (me - 1, 1 - peer)
    detours = ((half - 2, -2), (half - 1, -LOW), (half, LOW), (half + 1, 2))
    flag = lambda condition: condition.astype(jnp.int32)
    hands_over = (me >= half - 2) & (me <= half + 1)
    helper = me + sum(flag(me == slab) * offset for slab, offset in detours)
    helped = sum(flag(me == slab + offset) * slab for slab, offset in detours)
    helps = helped > 0
    groups = slabs // LOW
    block, lane_of = me // LOW, lax.rem(me, LOW)
    near_peers = [(block * LOW + lax.rem(lane_of + k, LOW), peer) for k in range(1, LOW)]
    wide_peers = [(lax.rem(block + k, groups) * LOW + lane_of, peer) for k in range(1, groups)]

    barrier = pltpu.get_barrier_semaphore()
    for device in [partner] + near_peers + wide_peers:
        pl.semaphore_signal(barrier, inc=1, device_id=device, device_id_type=MESH)

    @pl.when(has_up)
    def _():
        pl.semaphore_signal(barrier, inc=1, device_id=up, device_id_type=MESH)

    @pl.when(has_down)
    def _():
        pl.semaphore_signal(barrier, inc=1, device_id=down, device_id_type=MESH)

    @pl.when(hands_over)
    def _():
        pl.semaphore_signal(barrier, inc=1, device_id=(helper, 1 - peer), device_id_type=MESH)

    @pl.when(helps)
    def _():
        pl.semaphore_signal(barrier, inc=1, device_id=(helped, peer), device_id_type=MESH)

    @pl.when(below_cross)
    def _():
        pl.semaphore_signal(barrier, inc=1, device_id=cross_up, device_id_type=MESH)

    @pl.when(above_cross)
    def _():
        pl.semaphore_signal(barrier, inc=1, device_id=cross_down, device_id_type=MESH)

    def remote(source, target, send, recv, device):
        return pltpu.make_async_remote_copy(
            src_ref=source, dst_ref=target, send_sem=send, recv_sem=recv,
            device_id=device, device_id_type=MESH,
        )

    inner = pl.ds(PAD, ROWS)
    loads = [
        pltpu.make_async_copy(
            wave_hbm.at[0, part], own.at[part, pl.ds(OWN, DEPTH), inner, :], in_sem.at[part]
        )
        for part in range(9)
    ]
    tables = ((buo_hbm, buo, BUO), (lame_hbm, lame, MOD), (shear_hbm, shear, MOD))
    mat_loads = [
        pltpu.make_async_copy(source, target.at[pl.ds(lead, DEPTH)], in_sem.at[9 + k])
        for k, (source, target, lead) in enumerate(tables)
    ]
    for copy in loads + mat_loads:
        copy.start()

    zero = jnp.zeros((PAD, COLS), F32)
    plane = jnp.zeros((ROWS, COLS), F32)

    @pl.loop(0, 9)
    def _(part):
        for z in range(DEPTH + 2 * OWN):
            own[part, z, pl.ds(0, PAD), :] = zero
            own[part, z, pl.ds(PAD + ROWS, PAD), :] = zero
        for z in list(range(OWN)) + list(range(OWN + DEPTH, DEPTH + 2 * OWN)):
            own[part, z, inner, :] = plane

    def clear(base_mat, base_own):
        for _, target, lead in tables:
            for z in range(lead):
                target[z + (lead + DEPTH if base_mat else 0)] = plane

        @pl.loop(0, 9)
        def _(part):
            for z in range(FAR):
                got[part, z + base_own] = jnp.zeros((ROWS, COLS), BF16)

    @pl.when(jnp.logical_not(has_down))
    def _():
        clear(0, 0)

    @pl.when(jnp.logical_not(has_up))
    def _():
        clear(1, FAR + DEPTH)

    for part, copy in enumerate(loads):
        copy.wait()
        for z in (0, 1, 6, 7) if part < 6 else (0, 1, 2, 5, 6, 7):
            mirror[0, part, z] = own[part, z + OWN, inner, :].astype(BF16)

    def place_sources(target, first_z, count, shot, step):
        place = lax.broadcasted_iota(jnp.int32, (ROWS, COLS), 0) * COLS + lanes((ROWS, COLS))

        @pl.loop(0, count)
        def _(i):
            first = (me * DEPTH + first_z + i) * ROWS * COLS
            total = jnp.zeros((ROWS, COLS), F32)
            for j in range(SOURCES):
                total = total + jnp.where(place == cells[shot, j] - first, wavelet[step, shot, j], 0.0)
            target[i] = total

    mat_layers = ((0, buo, BUO), (BUO, lame, MOD), (BUO + MOD, shear, MOD))

    def round_mats(layers_of):
        for at, target, lead in layers_of:
            for z in range(lead):
                mat_out[0, at + z] = target[DEPTH + z].astype(BF16)
                mat_out[1, at + z] = target[lead + z].astype(BF16)

    for copy in mat_loads:
        copy.wait()
    round_mats(mat_layers[:1])

    greeted = [flag(yes) for yes in (has_up, has_down, below_cross, above_cross, hands_over, helps)]
    pl.semaphore_wait(barrier, 1 + len(near_peers) + len(wide_peers) + sum(greeted))

    def halo_up(step):
        return [
            remote(mirror.at[step, pl.ds(0, 6), pl.ds(7, 1)], low_a.at[step, :, pl.ds(1, 1)],
                   halo_send.at[step, 0, 0], halo_recv.at[step, 0, 0], up),
            remote(mirror.at[step, pl.ds(VZ, 1), pl.ds(6, 1)], low_a.at[step, pl.ds(VZ, 1), pl.ds(0, 1)],
                   halo_send.at[step, 0, 2], halo_recv.at[step, 0, 2], up),
            remote(mirror.at[step, pl.ds(6, 3), pl.ds(5, 3)], low_b.at[step],
                   halo_send.at[step, 0, 1], halo_recv.at[step, 0, 1], up),
        ]

    def halo_down(step):
        return [
            remote(mirror.at[step, pl.ds(0, 6), pl.ds(0, 2)], high_a.at[step],
                   halo_send.at[step, 1, 0], halo_recv.at[step, 1, 0], down),
            remote(mirror.at[step, pl.ds(6, 3), pl.ds(0, 3)], high_b.at[step],
                   halo_send.at[step, 1, 1], halo_recv.at[step, 1, 1], down),
        ]

    def mat_copy(kind, side, device):
        layers = pl.ds(0, BUO) if kind == 0 else pl.ds(BUO, 2 * MOD)
        return remote(mat_out.at[side, layers], mat_in.at[side, layers],
                      mat_send.at[kind, side], mat_recv.at[kind, side], device)

    def each(flag, copies, act):
        @pl.when(flag)
        def _():
            for copy in copies():
                act(copy)

    begin, sent = (lambda copy: copy.start()), (lambda copy: copy.wait_send())

    def send_mats(kind):
        each(has_up, lambda: [mat_copy(kind, 0, up)], begin)
        each(has_down, lambda: [mat_copy(kind, 1, down)], begin)

    def take_mats(kind):
        for side, flag, device in ((0, has_down, up), (1, has_up, down)):
            @pl.when(flag)
            def _(side=side, device=device):
                mat_copy(kind, side, device).wait_recv()
                for at, target, lead in mat_layers[:1] if kind == 0 else mat_layers[1:]:
                    for z in range(lead):
                        target[z + (lead + DEPTH if side else 0)] = mat_in[side, at + z].astype(F32)

    def send_halos(step):
        @pl.when(has_up)
        def _():
            for copy in halo_up(step):
                copy.start()

        @pl.when(has_down)
        def _():
            for copy in halo_down(step):
                copy.start()

    send_mats(0)
    send_halos(0)
    place_sources(image_own.at[0], 0, DEPTH, peer, 0)

    band = extra[0] if MATMUL_X else None
    if MATMUL_X:
        row = lax.broadcasted_iota(jnp.int32, (2 * COLS, COLS), 0)
        offset = lax.rem(row, COLS) - lanes((2 * COLS, COLS))
        for k, sign in ((0, -1), (1, 1)):
            weight = jnp.where(offset == 0, -27.0 * sign, 0.0)
            weight = jnp.where(offset == sign, 27.0 * sign, weight)
            weight = jnp.where(offset == -sign, 1.0 * sign, weight)
            weight = jnp.where(offset == 2 * sign, -1.0 * sign, weight)
            band[k] = weight.astype(BF16)

    row_parts = list(zip(ROW_CUTS[:-1], ROW_CUTS[1:]))

    def across(index):
        if index == 0:
            layer, count, lo, hi = 3, 2, 0, ROWS
        else:
            lo, hi = row_parts[(index - 1) // 2]
            layer, count = (0, 3) if index % 2 else (5, 3)
        return remote(
            mirror.at[1, :, pl.ds(layer, count), pl.ds(lo, hi - lo)],
            got.at[:, pl.ds(FAR + layer, count), pl.ds(lo, hi - lo)],
            x_send.at[index], x_recv.at[index], partner,
        )

    across_count = 1 + 2 * len(row_parts)

    def forward(index, source, lead, upward, device):
        side, base = (0, 0) if upward else (1, FAR + DEPTH)
        if index == 0:
            return [
                remote(source.at[:, pl.ds(lead + 3, 2)], got.at[:, pl.ds(base + (1 if upward else 3), 2)],
                       fwd_send.at[0, side, 0], fwd_recv.at[0, side, 0], device)
            ]
        lo, hi = row_parts[index - 1]
        rows, deep = pl.ds(lo, hi - lo), pl.ds(6, 3)
        first, single = (5, 2) if upward else (0, 5)
        return [
            remote(source.at[:, pl.ds(lead + first, 3), rows],
                   got.at[:, pl.ds(base + (3 if upward else 0), 3), rows],
                   fwd_send.at[index, side, 0], fwd_recv.at[index, side, 0], device),
            remote(source.at[deep, pl.ds(lead + single, 1), rows],
                   got.at[deep, pl.ds(base + (0 if upward else 5), 1), rows],
                   fwd_send.at[index, side, 1], fwd_recv.at[index, side, 1], device),
        ]

    def forward_up(index):
        return forward(index, got, FAR, True, up)

    def forward_down(index):
        return forward(index, got, FAR, False, down)

    def straight_up(index):
        return forward(index, mirror.at[1], 0, True, cross_up)

    def straight_down(index):
        return forward(index, mirror.at[1], 0, False, cross_down)

    held = (me < 2) | (me >= slabs - 2)
    passes_up = has_up & jnp.logical_not(below_cross)
    passes_down = has_down & jnp.logical_not(above_cross)

    def pass_on(index):
        if index == 0:
            across(0).wait_recv()
        else:
            across(2 * index - 1).wait_recv()
            across(2 * index).wait_recv()
        each(passes_up, lambda: forward_up(index), begin)
        each(passes_down, lambda: forward_down(index), begin)

    own_way = jnp.logical_not(hands_over)

    at_face = below_cross | above_cross
    helps_face = (me == half - 1 - LOW) | (me == half + LOW)
    hand_both, help_both = hands_over & jnp.logical_not(at_face), helps & jnp.logical_not(helps_face)

    def goes(index):
        return own_way | at_face if index == 3 else own_way

    def across_copies(index):
        return [across(0)] if index == 0 else [across(2 * index - 1), across(2 * index)]

    def send_across(index):
        if index < 2:
            for copy in across_copies(index):
                copy.start()
        else:
            each(goes(index), lambda: across_copies(index), begin)
        if index == 0:
            each(below_cross, lambda: straight_up(index), begin)
            each(above_cross, lambda: straight_down(index), begin)

    def hand_over(parts):
        begin_row, count = ROW_CUTS[1], ROW_CUTS[1 + parts] - ROW_CUTS[1]
        return [
            remote(mirror.at[1, :, pl.ds(first, 3), pl.ds(begin_row, count)],
                   held_over.at[:, pl.ds(3 * k, 3), pl.ds(0, count)],
                   help_send.at[k], help_recv.at[k], (helper, peer))
            for k, first in enumerate((0, 5))
        ]

    def help_across(parts):
        return [
            remote(held_over.at[:, pl.ds(3 * k, 3), pl.ds(lo - ROW_CUTS[1], hi - lo)],
                   got.at[:, pl.ds(FAR + first, 3), pl.ds(lo, hi - lo)],
                   help_send.at[2 * i + k], x_recv.at[2 * i - 1 + k], (helped, 1 - peer))
            for i, (lo, hi) in enumerate(row_parts, 1) if 1 < i <= 1 + parts
            for k, first in enumerate((0, 5))
        ]

    def help_out(flagged, parts_given):
        each(flagged, lambda: hand_over(parts_given), lambda copy: copy.wait_recv())
        each(flagged, lambda: help_across(parts_given), begin)

    def send_rest():
        for index in range(2, len(row_parts) + 1):
            send_across(index)

    def prepare():
        spread = (
            lax.broadcasted_iota(jnp.int32, (COLS // BLOCK, COLS), 0)
            == lanes((COLS // BLOCK, COLS)) // BLOCK
        ).astype(F32)
        exp_rows[...] = jnp.dot(
            exps[...].astype(F32), spread, preferred_element_type=F32, precision=lax.Precision.HIGHEST
        )

        @pl.loop(0, 9 * ROWS // BLOCK)
        def _(i):
            level = jnp.broadcast_to(exp_rows[pl.ds(i, 1), :], (BLOCK, COLS))
            upscale = jnp.ones((BLOCK, COLS), F32)
            downscale = upscale
            for exponent in (-2, -1, 1, 2):
                chosen = jnp.abs(level - exponent) < 0.5
                upscale = jnp.where(chosen, 2.0**exponent, upscale)
                downscale = jnp.where(chosen, 2.0**-exponent, downscale)
            up_rows[pl.ds(pl.multiple_of(i * BLOCK, BLOCK), BLOCK), :] = upscale
            down_rows[pl.ds(pl.multiple_of(i * BLOCK, BLOCK), BLOCK), :] = downscale

        @pl.loop(0, 9)
        def _(part):
            for z in range(DEPTH + 2 * FAR):
                other[part, z, pl.ds(0, PAD), :] = zero
                other[part, z, pl.ds(PAD + ROWS, PAD), :] = zero
        round_mats(mat_layers[1:])
        for step in (1, 2):
            place_sources(image_own.at[step], 0, DEPTH, peer, step)
        place_sources(image_far.at[pl.ds(0, DEPTH + 2 * MOD)], -MOD, DEPTH + 2 * MOD, 1 - peer, 1)
        place_sources(image_far.at[pl.ds(DEPTH + 2 * MOD, DEPTH)], 0, DEPTH, 1 - peer, 2)

    mine = Slab(own, OWN, buo, lame, shear, band).rows((0, ROWS))

    def copy_rounded(step, zs):
        @pl.loop(0, 9)
        def _(part):
            for z in zs:
                mirror[step + 1, part, z] = mine.at(part, z).astype(BF16)

    def tally(step):
        def body(k, carry):
            part = k // (DEPTH // 2)
            down_scale = down_rows[pl.ds(pl.multiple_of(part * ROWS, ROWS), ROWS), :]
            up_scale = up_rows[pl.ds(pl.multiple_of(part * ROWS, ROWS), ROWS), :]
            sizes, misfits, squares = carry
            for side in range(2):
                z = lax.rem(k, DEPTH // 2) * 2 + side
                value = mine.at(part, z)
                rounded = mirror[step + 1, part, z].astype(F32)
                level = jnp.clip(rounded * down_scale, -clip_level, clip_level)
                misfit = value - level * up_scale
                for y in range(0, ROWS, YB):
                    at = slice(y, y + YB)
                    sizes = sizes + jnp.abs(level[at])
                    misfits = misfits + misfit[at] * misfit[at]
                    squares = squares + value[at] * value[at]
            return sizes, misfits, squares

        zeros = jnp.zeros((YB, COLS), F32)
        for k, total in enumerate(lax.fori_loop(0, 9 * (DEPTH // 2), body, (zeros,) * 3)):
            sums[step, k] = total

    edges = lambda first, gap: (lambda i: first + i + (i // 3) * gap)

    theirs = Slab(other, FAR, buo, lame, shear, band)

    def widen(rows):
        lo, hi = rows

        def move(part, z):
            other[part, z, pl.ds(PAD + lo, hi - lo), :] = got[part, z, pl.ds(lo, hi - lo), :].astype(F32)

        @pl.loop(0, 9)
        def _(part):
            for z in range(1, DEPTH + 2 * FAR - 1):
                move(part, z)

        for part in range(6, 9):
            for z in (0, DEPTH + 2 * FAR - 1):
                move(part, z)

    def compress(step, rows):
        lo, hi = rows

        @pl.loop(0, 9)
        def _(part):
            for y in range(lo // YB * YB, hi, YB):
                row = lax.broadcasted_iota(jnp.int32, (YB, COLS), 0) + y
                down = down_rows[pl.ds(pl.multiple_of(part * ROWS + y, YB), YB), :]
                for z in range(DEPTH):
                    value = other[part, z + FAR, pl.ds(PAD + y, YB), :]
                    level = jnp.clip(value * down, -clip_level, clip_level)
                    if lo > y or hi < y + YB:
                        before = packed[step, part, z, pl.ds(y, YB), :].astype(F32)
                        level = jnp.where((row >= lo) & (row < hi), level, before)
                    packed[step, part, z, pl.ds(y, YB), :] = level.astype(BF16)


    def ends_of(index):
        if index < 0:
            return [0] * 4
        end = row_parts[GROUPS[index][-1]][1]
        return [end if end == ROWS else end - 2 * (k + 1) for k in range(4)]

    def recompute(index, between):
        lo, hi = row_parts[GROUPS[index][0]][0], row_parts[GROUPS[index][-1]][1]
        arriving = ([0] if index == 0 else []) + [part + 1 for part in GROUPS[index]]

        @pl.when(has_down)
        def _():
            for part in arriving:
                for copy in forward_up(part):
                    copy.wait_recv()

        @pl.when(has_up)
        def _():
            for part in arriving:
                for copy in forward_down(part):
                    copy.wait_recv()

        if index == 0:
            take_mats(1)
        widen((lo, hi))
        compress(0, (lo, hi))
        span = list(zip(ends_of(index - 1), ends_of(index)))
        wide_group = WIDE_GROUP
        theirs.rows(span[0])
        over(17, lambda i: i - 4, wide_group, theirs.velocity)
        theirs.rows(span[1])
        image = lambda z, y, n: image_far[z + MOD, pl.ds(y, n), :]
        over(14, lambda i: i - 3, wide_group, lambda zs: theirs.stress(zs, image))
        compress(1, span[1])
        between()
        theirs.rows(span[2])
        over(11, lambda i: i - 1, wide_group, theirs.velocity)
        theirs.rows(span[3])
        image = lambda z, y, n: image_far[z + DEPTH + 2 * MOD, pl.ds(y, n), :]
        over(DEPTH, lambda i: i, wide_group, lambda zs: theirs.stress(zs, image))
        compress(2, span[3])

    @pl.loop(0, STEPS)
    def _(step):
        @pl.when(step == 2)
        def _():
            pass_on(0)

        def image(z, y, n):
            return image_own[step, z, pl.ds(y, n), :]

        over(5, lambda i: i + 2, GROUP, mine.velocity)
        middle = (2, lambda i: i + 3)
        over(*middle, GROUP, lambda zs: mine.stress(zs, image))
        copy_rounded(step, (3, 4))

        @pl.when(step == 0)
        def _():
            send_across(0)
            prepare()
            take_mats(0)

        @pl.when((step == 2) & own_way)
        def _():
            pass_on(1)

        @pl.when(has_down)
        def _():
            for copy in halo_up(step):
                copy.wait_recv()

            @pl.loop(0, 6)
            def _(part):
                own[part, OWN - 1, inner, :] = low_a[step, part, 1].astype(F32)

            own[VZ, OWN - 2, inner, :] = low_a[step, VZ, 0].astype(F32)

            @pl.loop(0, 3)
            def _(part):
                for z in range(3):
                    own[part + 6, OWN - 3 + z, inner, :] = low_b[step, part, z].astype(F32)

        @pl.when(has_up)
        def _():
            for copy in halo_down(step):
                copy.wait_recv()

            @pl.loop(0, 6)
            def _(part):
                for z in range(2):
                    own[part, OWN + DEPTH + z, inner, :] = high_a[step, part, z].astype(F32)

            @pl.loop(0, 3)
            def _(part):
                for z in range(3):
                    own[part + 6, OWN + DEPTH + z, inner, :] = high_b[step, part, z].astype(F32)

        pl.when((step == 1) & hand_both)(lambda: send_across(1))

        @pl.when((step == 2) & held)
        def _():
            send_rest()

        over(6, edges(-1, 5), GROUP, mine.velocity)
        outer = (6, edges(0, 2))
        over(*outer, GROUP, lambda zs: mine.stress(zs, image))
        copy_rounded(step, (0, 1, 2, 5, 6, 7))

        @pl.when(step < STEPS - 1)
        def _():
            send_halos(step + 1)

        @pl.when(step == 0)
        def _():
            send_mats(1)
            each(hand_both, lambda: hand_over(2), begin)
            each(at_face, lambda: hand_over(1), begin)
            pl.when(own_way)(lambda: send_across(1))
            for index in (1, 2, 3):
                each(below_cross, lambda: straight_up(index), begin)
                each(above_cross, lambda: straight_down(index), begin)

        @pl.when((step == 1) & jnp.logical_not(held))
        def _():
            pl.when(at_face)(lambda: send_across(1))
            help_out(help_both, 2)
            send_rest()

        pl.when((step == 2) & hands_over)(lambda: pass_on(1))
        tally(step)

    help_out(helps_face, 1)

    row8 = lax.broadcasted_iota(jnp.int32, (8, COLS), 0)
    lane8 = lanes((8, COLS))
    tile = jnp.zeros((8, COLS), F32)
    for step in range(STEPS):
        for k in range(3):
            tile = tile + jnp.where((row8 == k) & (lane8 == step), jnp.sum(sums[step, k]), 0.0)

    def sum_copies(phase):
        peers, slot = ((near_peers, lane_of), (wide_peers, block))[phase]
        return [
            remote(stat_src.at[phase], stat_rx.at[phase, slot],
                   stat_send.at[phase, k], stat_recv.at[phase, k], device)
            for k, device in enumerate(peers)
        ]

    def spread_sums(phase, tile):
        stat_src[phase] = tile
        stat_rx[phase, (lane_of, block)[phase]] = tile
        for copy in sum_copies(phase):
            copy.start()

    def collect_sums(phase):
        for copy in sum_copies(phase):
            copy.wait()
        total = stat_rx[phase, 0]
        for k in range(1, (LOW, groups)[phase]):
            total = total + stat_rx[phase, k]
        return total

    spread_sums(0, tile)
    late_sums = below_cross | above_cross

    def second_phase():
        spread_sums(1, collect_sums(0))

    pass_on(2)
    pl.when(late_sums)(second_phase)
    pl.when(hands_over)(lambda: pass_on(3))
    recompute(0, lambda: pl.when(own_way)(lambda: pass_on(3)))
    pl.when(jnp.logical_not(late_sums))(second_phase)
    recompute(1, lambda: None)

    tile = collect_sums(1)
    scaled = tile * (1.0 / (9 * slabs * DEPTH * ROWS * COLS))
    ratio = scaled[1:2] / (scaled[2:3] + energy_floor)
    stats_out[0:1, :] = scaled[0:1, :STEPS]
    stats_out[1:2, :] = jnp.sqrt(ratio)[:, :STEPS]

    for index in range(2):
        for copy in across_copies(index):
            copy.wait_send()
    for index in range(2, len(row_parts) + 1):
        each(goes(index), lambda: across_copies(index), sent)
    each(hand_both, lambda: hand_over(2), sent)
    each(at_face, lambda: hand_over(1), sent)
    each(help_both, lambda: help_across(2), sent)
    each(helps_face, lambda: help_across(1), sent)

    @pl.when(has_up)
    def _():
        for kind in range(2):
            mat_copy(kind, 0, up).wait_send()
        for step in range(STEPS):
            for copy in halo_up(step):
                copy.wait_send()

    @pl.when(has_down)
    def _():
        for kind in range(2):
            mat_copy(kind, 1, down).wait_send()
        for step in range(STEPS):
            for copy in halo_down(step):
                copy.wait_send()

    for index in range(len(row_parts) + 1):
        each(passes_up, lambda: forward_up(index), sent)
        each(passes_down, lambda: forward_down(index), sent)
        each(below_cross, lambda: straight_up(index), sent)
        each(above_cross, lambda: straight_down(index), sent)


def write_out(own, packed, sums, final_hbm, stored_hbm, stats_out, sem):
    copies = []
    for part in range(0, 9, 3):
        parts = pl.ds(part, 3)
        for step in range(STEPS):
            copies.append((packed.at[step, parts], stored_hbm.at[0, step, parts]))
        copies.append((own.at[parts, pl.ds(OWN, DEPTH), pl.ds(PAD, ROWS), :], final_hbm.at[0, parts]))
    copies = [pltpu.make_async_copy(source, target, sem.at[k]) for k, (source, target) in enumerate(copies)]
    for copy in copies:
        copy.start()
    stats_out[...] = sums[...]
    for copy in copies:
        copy.wait()


def per_device(slabs, wavefield, buoyancy, lame_lambda, shear_modulus, scale_exponents, source_cells, wavelet):
    hbm = pl.BlockSpec(memory_space=pl.ANY)
    vmem = pl.BlockSpec(memory_space=pltpu.VMEM)
    smem = pl.BlockSpec(memory_space=pltpu.SMEM)
    parts = len(ROW_CUTS) - 1
    dma = pltpu.SemaphoreType.DMA
    own, packed, statistics = pl.pallas_call(
        functools.partial(kernel, slabs),
        out_shape=(
            pltpu.VMEM((9, DEPTH + 2 * OWN, ROWS + 2 * PAD, COLS), F32),
            pltpu.VMEM((STEPS, 9, DEPTH, ROWS, COLS), BF16),
            pltpu.VMEM((2, STEPS), F32),
        ),
        in_specs=[hbm, hbm, hbm, hbm, vmem, smem, smem],
        out_specs=(vmem, vmem, vmem),
        scratch_shapes=[
            pltpu.VMEM((9, DEPTH + 2 * FAR, ROWS + 2 * PAD, COLS), F32),
            pltpu.VMEM((STEPS + 1, 9, DEPTH, ROWS, COLS), BF16),
            pltpu.VMEM((STEPS, 6, 2, ROWS, COLS), BF16),
            pltpu.VMEM((STEPS, 3, 3, ROWS, COLS), BF16),
            pltpu.VMEM((STEPS, 6, 2, ROWS, COLS), BF16),
            pltpu.VMEM((STEPS, 3, 3, ROWS, COLS), BF16),
            pltpu.VMEM((DEPTH + 2 * BUO, ROWS, COLS), F32),
            pltpu.VMEM((DEPTH + 2 * MOD, ROWS, COLS), F32),
            pltpu.VMEM((DEPTH + 2 * MOD, ROWS, COLS), F32),
            pltpu.VMEM((2, BUO + 2 * MOD, ROWS, COLS), BF16),
            pltpu.VMEM((2, BUO + 2 * MOD, ROWS, COLS), BF16),
            pltpu.VMEM((9, DEPTH + 2 * FAR, ROWS, COLS), BF16),
            pltpu.VMEM((9 * ROWS, COLS), F32),
            pltpu.VMEM((9 * ROWS, COLS), F32),
            pltpu.VMEM((9 * ROWS // BLOCK, COLS), F32),
            pltpu.VMEM((STEPS, 3, YB, COLS), F32),
            pltpu.VMEM((2, 8, COLS), F32),
            pltpu.VMEM((2, max(LOW, slabs // LOW), 8, COLS), F32),
            pltpu.VMEM((STEPS, DEPTH, ROWS, COLS), F32),
            pltpu.VMEM((2 * DEPTH + 2 * MOD, ROWS, COLS), F32),
            pltpu.VMEM((9, 6, ROWS - ROW_CUTS[1], COLS), BF16),
            dma((12,)),
            dma((STEPS, 2, 3)),
            dma((STEPS, 2, 3)),
            dma((2, 2)),
            dma((2, 2)),
            dma((1 + 2 * parts,)),
            dma((1 + 2 * parts,)),
            dma((2 + 2 * parts,)),
            dma((2,)),
            dma((1 + parts, 2, 2)),
            dma((1 + parts, 2, 2)),
            dma((2, max(LOW, slabs // LOW))),
            dma((2, max(LOW, slabs // LOW))),
        ]
        + ([pltpu.VMEM((2, 2 * COLS, COLS), BF16)] if MATMUL_X else []),
        compiler_params=pltpu.CompilerParams(
            collective_id=0, has_side_effects=True, vmem_limit_bytes=55 * 1024 * 1024
        ),
        name="elastic_steps",
    )(
        wavefield, buoyancy, lame_lambda, shear_modulus,
        scale_exponents.reshape(9 * ROWS // BLOCK, COLS // BLOCK), source_cells,
        wavelet.transpose(1, 0, 2),
    )
    final, stored, statistics = pl.pallas_call(
        write_out,
        out_shape=(
            jax.ShapeDtypeStruct(wavefield.shape, F32),
            jax.ShapeDtypeStruct((1, STEPS, 9, DEPTH, ROWS, COLS), BF16),
            jax.ShapeDtypeStruct((2, STEPS), F32),
        ),
        in_specs=[vmem, vmem, vmem],
        out_specs=(hbm, hbm, vmem),
        scratch_shapes=[dma((12,))],
        compiler_params=pltpu.CompilerParams(vmem_limit_bytes=8 * 1024 * 1024),
        name="write_out",
    )(own, packed, statistics)
    return final, stored, statistics.T[None]


def solution(mesh):
    return jax.shard_map(
        functools.partial(per_device, mesh.shape["space"]),
        mesh=mesh,
        in_specs=(
            P("peer", None, "space", None, None),
            P("space", None, None),
            P("space", None, None),
            P("space", None, None),
            P(None, "space", None, None),
            P(),
            P(),
        ),
        out_specs=(
            P("peer", None, "space", None, None),
            P("peer", None, None, "space", None, None),
            P("peer", None, None),
        ),
        check_vma=False,
    )
```
